256 devices in a mesh: tm: 2 (over core), space: 128 (over z, y, x).
Axes of the slice: x: 4, y: 4, z: 8, core: 2. Of those that a mesh axis runs over, the one named last changes fastest.
Arguments:
- checkpoints: float32 [2, 5, 16384, 128], P('tm', None, 'space'), may hold values from -6 to 6
- sources: float32 [2, 5, 16384, 128], P(None, None, 'space'), may hold values from -3 to 3
- pitch: float32 [8], replicated, may hold values from -3.140625 to 3.140625
- metric: float32 [16384, 128], P('space'), may hold values from 0.5 to 2
- obj_weight: float32 [5, 16384, 128], P(None, 'space'), may hold values from 0.1 to 0.6
- adjoint_end: float32 [5, 16384, 128], P(None, 'space'), may hold values from -6 to 6
- lift: bfloat16 [5, 128, 128], replicated, may hold values from -0.5 to 0.5
- mixing: float32 [5, 5, 5], replicated, may hold values from -1.25 to 1.25
- faces: int32 [16384, 4], P('space'), may hold values from 0 to 191
- send_idx: int32 [128, 4, 16], P('space'), may hold values from 0 to 127
Outputs:
- adjoint_bounds: float32 [2, 5, 16384, 128], P('tm', None, 'space')
- pitch_grad: float32 [8], replicated
The draws below stay inside these ranges and needn't reach their ends.
Inputs may be any that keep to these rules, and one draw needn't show every extreme that they name: `faces`: values below 128 name the subdomain's own blocks; value 128 + d * 16 + s names slot s of the blocks received from direction d. `send_idx`: entry [p, d, s] is a local block of subdomain p sent to subdomain p + o[d], o = (1, -1, 2, -2); blocks may repeat.
All inputs are finite; a program needn't handle non-finite values.
Results may differ from the reference program's by a relative error of at most 0.0035.
Values may be sent and summed in bfloat16 or wider, within the bound.
A program may use at most 64 MiB of HBM per device.

```python
import math
import jax
import jax.numpy as jnp
from jax import lax

COMPS = 5
NODES = 128
FACES = 4
LEVELS = 8
BLK_DEV = 128
HALO = 16
NBT = 16384
N_TM = 2
N_SPACE = 128


def with_ends(drawn, key, least, high):
    extent = drawn.shape
    spot = [jax.random.randint(jax.random.fold_in(key, axis), (), 0, extent[axis]) for axis in range(len(extent))]
    drawn = drawn.at[tuple(spot)].set(least)
    longest = extent.index(max(extent))
    spot[longest] = (spot[longest] + 1) % extent[longest]
    return drawn.at[tuple(spot)].set(high)


def level_of(rng, extent, cuts, low, largest):
    factor_of, own = 1.0, jax.random.fold_in(rng, 6)
    for position, blocks in cuts:
        steps = jnp.exp(jax.random.uniform(jax.random.fold_in(own, position), (blocks,), jnp.float32, low / len(cuts), largest / len(cuts)))
        factor_of = factor_of * jnp.repeat(steps, extent[position] // blocks).reshape([-1 if axis == position else 1 for axis in range(len(extent))])
    return factor_of


def noise(rng, dims, spread, limit, cuts=(), held_as=jnp.bfloat16):
    entries = jax.random.normal(rng, dims, jnp.float32) * spread
    if len(cuts) > 0:
        entries = level_of(rng, dims, cuts, -0.22, 0.18) * entries
    return jnp.clip(entries, min=-limit, max=limit).astype(held_as)


def setup_inputs(seed: int = 0) -> dict:
    key_of = jax.random.split(jax.random.key(seed), 11)
    return {
        "checkpoints": noise(key_of[0], (2, COMPS, NBT, NODES), 1.0, 6.0, ((0, 2), (2, 128)), jnp.float32),
        "sources": noise(key_of[1], (2, COMPS, NBT, NODES), 0.5, 3.0, ((2, 128),), jnp.float32),
        "pitch": jnp.clip(jax.random.uniform(key_of[2], (LEVELS,), jnp.float32, -3.140625, 3.140625), -3.140625, 3.140625),
        "metric": jnp.clip(jnp.exp(math.log(2.0) - 1.3862944 * jax.random.uniform(key_of[3], (NBT, NODES), jnp.float32) ** level_of(key_of[3], (NBT, NODES), ((0, 128),), -0.2, 0.2)), 0.5, 2.0),
        "obj_weight": jnp.clip(0.1 + 0.5 * jax.random.uniform(key_of[4], (COMPS, NBT, NODES), jnp.float32) ** level_of(key_of[4], (COMPS, NBT, NODES), ((1, 128),), -0.2, 0.2), 0.1, 0.6),
        "adjoint_end": noise(key_of[5], (COMPS, NBT, NODES), 1.0, 6.0, ((1, 128),), jnp.float32),
        "lift": noise(key_of[6], (FACES + 1, NODES, NODES), NODES ** -0.5, 0.5),
        "mixing": noise(key_of[7], (FACES + 1, COMPS, COMPS), (COMPS * (FACES + 1)) ** -0.5, 1.25, (), jnp.float32),
        "faces": with_ends(jax.random.randint(key_of[8], (NBT, FACES), 0, BLK_DEV + 4 * HALO), jax.random.fold_in(key_of[8], 1), 0, (BLK_DEV + 4 * HALO) - 1).astype(jnp.int32),
        "send_idx": with_ends(jax.random.randint(key_of[9], (N_SPACE, 4, HALO), 0, BLK_DEV), jax.random.fold_in(key_of[9], 1), 0, BLK_DEV - 1).astype(jnp.int32),
    }


OFFSETS = (1, -1, 2, -2)
STEP_SIZE = 0.5

def global_faces(faces, send_idx):
    total_blocks = faces.shape[0]
    blk_count = total_blocks // N_SPACE
    slot_count = send_idx.shape[2]
    owner_dev = (jnp.arange(total_blocks, dtype=jnp.int32) // blk_count)[:, None]
    inside = owner_dev * blk_count + faces
    beyond = jnp.maximum(faces - blk_count, 0)
    direction = beyond // slot_count
    slot_pos = beyond % slot_count
    shifts = jnp.array(OFFSETS, dtype=jnp.int32)[direction]
    source_dev = owner_dev - shifts
    is_valid = (source_dev >= 0) & (source_dev < N_SPACE)
    clipped = jnp.clip(source_dev, 0, N_SPACE - 1)
    flat_send = send_idx.reshape(-1)
    picked = flat_send[(clipped * 4 + direction) * slot_count + slot_pos]
    outside = jnp.where(is_valid, clipped * blk_count + picked, total_blocks)
    return jnp.where(faces < blk_count, inside, outside).astype(jnp.int32)

def residual_of(current, global_index, metric, lift_float, mixing):
    squashed = lax.optimization_barrier(jnp.tanh(current).astype(jnp.bfloat16))
    squashed = squashed.astype(jnp.float32)
    padded = jnp.concatenate([squashed, jnp.zeros((COMPS, 1, NODES), jnp.float32)], axis=1)
    totals = jnp.zeros(current.shape, jnp.float32)
    for face_slot in range(global_index.shape[1]):
        picked = padded[:, global_index[:, face_slot], :]
        products = jnp.einsum('cbj,ij->cbi', picked, lift_float[face_slot], precision=lax.Precision.HIGHEST)
        totals = totals + jnp.einsum('ec,cbi->ebi', mixing[face_slot], products, precision=lax.Precision.HIGHEST)
    return metric[None] * totals

def transpose_of(adjoint, current, global_index, metric, lift_float, mixing):
    total_blocks = current.shape[1]
    weighted = metric[None] * adjoint
    totals = jnp.zeros((COMPS, total_blocks + 1, NODES), jnp.float32)
    for face_slot in range(global_index.shape[1]):
        mixed = jnp.einsum('ec,ebi->cbi', mixing[face_slot], weighted, precision=lax.Precision.HIGHEST)
        mixed = lax.optimization_barrier(mixed.astype(jnp.bfloat16)).astype(jnp.float32)
        returned_terms = jnp.einsum('cbi,ij->cbj', mixed, lift_float[face_slot], precision=lax.Precision.HIGHEST)
        totals = totals.at[:, global_index[:, face_slot], :].add(returned_terms)
    derivative = 1.0 - jnp.tanh(current) ** 2
    return totals[:, :total_blocks, :] * derivative

def reference(checkpoints, sources, pitch, metric, obj_weight, adjoint_end, lift, mixing, faces, send_idx):
    total_blocks = faces.shape[0]
    own_index = jnp.arange(total_blocks, dtype=jnp.int32)[:, None]
    global_index = jnp.concatenate([own_index, global_faces(faces, send_idx)], axis=1).astype(jnp.int32)
    half_count = LEVELS // N_TM
    lift_float = lift.astype(jnp.float32)
    states = []
    current = checkpoints[0]
    for segment in range(N_TM):
        current = checkpoints[segment]
        for within in range(half_count):
            level_now = segment * half_count + within
            states.append(current)
            forcing = jnp.cos(pitch[level_now]) * sources[0] + jnp.sin(pitch[level_now]) * sources[1]
            current = current + STEP_SIZE * (forcing - residual_of(current, global_index, metric, lift_float, mixing))
    states.append(current)
    normalizer = math.sqrt(COMPS * NODES * total_blocks)
    adjoint = adjoint_end + obj_weight * states[LEVELS]
    grads = [None] * LEVELS
    bounds = [None, None]
    for level_now in reversed(range(LEVELS)):
        turning = jnp.cos(pitch[level_now]) * sources[1] - jnp.sin(pitch[level_now]) * sources[0]
        grads[level_now] = STEP_SIZE * jnp.sum(adjoint * turning) / normalizer
        adjoint = adjoint - STEP_SIZE * transpose_of(adjoint, states[level_now], global_index, metric, lift_float, mixing)
        if level_now > 0:
            adjoint = adjoint + obj_weight * states[level_now]
        if level_now % half_count == 0:
            bounds[level_now // half_count] = adjoint
    return (jnp.stack(bounds), jnp.stack(grads))
```

```python
import functools
import math

import jax
import jax.numpy as jnp
from jax import lax
from jax.experimental import pallas as pl
from jax.experimental.pallas import tpu as pltpu
from jax.sharding import PartitionSpec as P

OFFSETS = (1, -1, 2, -2)
STEP_SIZE = 0.5
MESH = pl.DeviceIdType.MESH
F32, BF16 = jnp.float32, jnp.bfloat16
CHUNK = 32


def matmul(left, right):
    return jnp.dot(left, right, preferred_element_type=F32)


def sweep(
    n_space,
    plane,
    checkpoint_in,
    sources_in,
    pitch,
    metric_in,
    weight_in,
    end_in,
    lift_in,
    mixing,
    faces,
    send_idx,
    bounds,
    grads,
    states,
    sources,
    metric,
    weight,
    adjoint,
    kept,
    lift,
    lift_t,
    cosines,
    sines,
    pick,
    pick_t,
    near,
    near_t,
    far,
    far_t,
    squashed,
    gathered,
    lifted,
    base,
    slope,
    halo_lifted,
    halo_mixed,
    split,
    pulled,
    halo_pulled,
    mixed,
    far_mixed,
    fwd_out,
    fwd_in,
    rev_out,
    rev_in,
    partial,
    plane_parts,
    plane_sum,
    layer_parts,
    in_sem,
    fwd_send,
    fwd_recv,
    rev_send,
    rev_recv,
    state_send,
    state_recv,
    plane_send,
    plane_recv,
    layer_send,
    layer_recv,
    end_sem,
    out_sem,
):
    comps, blocks, nodes = states.shape[1:]
    slots = lift.shape[0]
    halo = fwd_in.shape[2]
    ghosts = 4 * halo
    levels = pitch.shape[0]
    half = levels // 2
    layers = n_space // plane
    t = lax.axis_index("tm")
    p = lax.axis_index("space")
    spot = lax.rem(p, plane)
    layer = p // plane
    first = t * half

    def exists(q):
        return jnp.logical_and(q >= 0, q < n_space)

    def lane(c):
        return slice(c * nodes, (c + 1) * nodes)

    loads = [
        pltpu.make_async_copy(checkpoint_in.at[0], states.at[first], in_sem.at[0]),
        pltpu.make_async_copy(lift_in, lift, in_sem.at[1]),
        pltpu.make_async_copy(metric_in, metric, in_sem.at[2]),
        pltpu.make_async_copy(sources_in, sources, in_sem.at[3]),
        pltpu.make_async_copy(weight_in, weight, in_sem.at[4]),
        pltpu.make_async_copy(end_in, adjoint, in_sem.at[5]),
    ]
    for load in loads:
        load.start()

    barrier = pltpu.get_barrier_semaphore()

    def greet(device):
        pl.semaphore_signal(barrier, inc=1, device_id=device, device_id_type=MESH)

    for offset in OFFSETS:

        @pl.when(exists(p + offset))
        def _():
            greet((t, p + offset))

    greet((1 - t, p))
    for r in range(1, layers):
        greet((1, lax.rem(layer + r, layers) * plane + spot))

    @pl.when(t == 1)
    def _():
        for r in range(1, plane):
            greet((1, layer * plane + lax.rem(spot + r, plane)))

    lane_of = lax.broadcasted_iota(jnp.int32, (1, blocks), 1)
    for d in range(4):
        for s in range(halo):
            row = d * halo + s
            pick[pl.ds(row, 1), :] = jnp.where(lane_of == send_idx[0, d, s], 1.0, 0.0)

    for d, offset in enumerate(OFFSETS):

        @pl.when(jnp.logical_not(exists(p - offset)))
        def _():
            for i in range(half):
                fwd_in[i, d] = jnp.zeros(fwd_in.shape[2:], BF16)

        @pl.when(jnp.logical_not(exists(p + offset)))
        def _():
            for i in range(levels):
                rev_in[i, d] = jnp.zeros(rev_in.shape[2:], BF16)

    def fwd_copy(i, d, device):
        return pltpu.make_async_remote_copy(
            src_ref=fwd_out.at[i, d],
            dst_ref=fwd_in.at[i, d],
            send_sem=fwd_send.at[i, d],
            recv_sem=fwd_recv.at[i, d],
            device_id=(t, device),
            device_id_type=MESH,
        )

    def rev_copy(i, d, device):
        return pltpu.make_async_remote_copy(
            src_ref=rev_out.at[i, d],
            dst_ref=rev_in.at[i, d],
            send_sem=rev_send.at[i, d],
            recv_sem=rev_recv.at[i, d],
            device_id=(t, device),
            device_id_type=MESH,
        )

    def state_copy(i):
        return pltpu.make_async_remote_copy(
            src_ref=states.at[i],
            dst_ref=states.at[i],
            send_sem=state_send.at[i],
            recv_sem=state_recv.at[i],
            device_id=(1 - t, p),
            device_id_type=MESH,
        )

    def plane_copy(r):
        return pltpu.make_async_remote_copy(
            src_ref=partial,
            dst_ref=plane_parts.at[spot],
            send_sem=plane_send.at[r],
            recv_sem=plane_recv.at[spot],
            device_id=(1, layer * plane + lax.rem(spot + r, plane)),
            device_id_type=MESH,
        )

    def layer_copy(r, core):
        return pltpu.make_async_remote_copy(
            src_ref=plane_sum,
            dst_ref=layer_parts.at[layer],
            send_sem=layer_send.at[core, r],
            recv_sem=layer_recv.at[layer],
            device_id=(core, lax.rem(layer + r, layers) * plane + spot),
            device_id_type=MESH,
        )

    end_copy = pltpu.make_async_remote_copy(
        src_ref=adjoint,
        dst_ref=bounds.at[0],
        send_sem=end_sem.at[0],
        recv_sem=end_sem.at[1],
        device_id=(1 - t, p),
        device_id_type=MESH,
    )
    keep_copy = pltpu.make_async_copy(kept, bounds.at[0], out_sem)

    def squash(state):
        for c in range(comps):
            squashed[:, lane(c)] = jnp.tanh(state(c)).astype(BF16)

    def send_forward(i):
        packets = matmul(pick[...].astype(BF16), squashed[...]).astype(BF16)
        for d, offset in enumerate(OFFSETS):
            fwd_out[i, d] = packets[d * halo : (d + 1) * halo]

            @pl.when(exists(p + offset))
            def _():
                fwd_copy(i, d, p + offset).start()

    def forward_near(i):
        gathered[...] = matmul(near[...], squashed[...]).astype(BF16)
        for k in range(slots):
            rows = squashed if k == 0 else gathered.at[pl.ds((k - 1) * blocks, blocks)]
            left = jnp.concatenate([rows[:, lane(c)] for c in range(comps)], axis=0)
            lifted[k] = matmul(left, lift_t[:, lane(k)])
        cosine = cosines[pl.ds(first + i, 1), :]
        sine = sines[pl.ds(first + i, 1), :]
        for start in range(0, blocks, CHUNK):
            some = slice(start, start + CHUNK)
            totals = [None] * comps
            for k in range(slots):
                for c in range(comps):
                    term = lifted[k, c * blocks + start : c * blocks + start + CHUNK, :]
                    for e in range(comps):
                        more = mixing[k, e, c] * term
                        totals[e] = more if totals[e] is None else totals[e] + more
            for e in range(comps):
                forcing = cosine * sources[0, e, some, :] + sine * sources[1, e, some, :]
                change = forcing - metric[some, :] * totals[e]
                base[e, some, :] = states[first + i, e, some, :] + STEP_SIZE * change

    def forward_far(i):
        for d, offset in enumerate(OFFSETS):

            @pl.when(exists(p - offset))
            def _():
                fwd_copy(i, d, p).wait_recv()

        ghost = jnp.concatenate([fwd_in[i, d] for d in range(4)], axis=0)
        left = jnp.concatenate([ghost[:, lane(c)] for c in range(comps)], axis=0)
        halo_lifted[...] = matmul(left, lift_t[:, nodes:])
        for k in range(1, slots):
            for start in range(0, ghosts, CHUNK):
                totals = [None] * comps
                for c in range(comps):
                    term = halo_lifted[c * ghosts + start : c * ghosts + start + CHUNK, lane(k - 1)]
                    for e in range(comps):
                        more = mixing[k, e, c] * term
                        totals[e] = more if totals[e] is None else totals[e] + more
                row = (k - 1) * ghosts + start
                for e in range(comps):
                    halo_mixed[row : row + CHUNK, lane(e)] = totals[e].astype(BF16)
        scale = STEP_SIZE * metric[...]
        arrived = matmul(far[...], halo_mixed[...])
        for e in range(comps):
            states[first + i + 1, e] = base[e] - scale * arrived[:, lane(e)]

    def send_reverse(j):
        for e in range(comps):
            weighted = metric[...] * adjoint[e]
            high = weighted.astype(BF16)
            split[:blocks, lane(e)] = high
            split[blocks:, lane(e)] = (weighted - high.astype(F32)).astype(BF16)
        halo_pulled[...] = matmul(far_t[...], split[...])
        for k in range(1, slots):
            for start in range(0, ghosts, CHUNK):
                row = (k - 1) * ghosts + start
                totals = [None] * comps
                for e in range(comps):
                    term = halo_pulled[row : row + CHUNK, lane(e)]
                    for c in range(comps):
                        more = mixing[k, e, c] * term
                        totals[c] = more if totals[c] is None else totals[c] + more
                for c in range(comps):
                    far_mixed[c * ghosts + start : c * ghosts + start + CHUNK, lane(k - 1)] = totals[
                        c
                    ].astype(BF16)
        right = jnp.concatenate([lift[k] for k in range(1, slots)], axis=0)
        packets = matmul(far_mixed[...], right).astype(BF16)
        for d, offset in enumerate(OFFSETS):
            for c in range(comps):
                row = c * ghosts + d * halo
                rev_out[j, d, :, lane(c)] = packets[row : row + halo]

            @pl.when(exists(p - offset))
            def _():
                rev_copy(j, d, p - offset).start()

    def reverse_sum(n):
        by_cosine = jnp.zeros((8, nodes), F32)
        by_sine = jnp.zeros((8, nodes), F32)
        for e in range(comps):
            value = adjoint[e]
            by_cosine += jnp.sum((value * sources[1, e]).reshape(blocks // 8, 8, nodes), axis=0)
            by_sine += jnp.sum((value * sources[0, e]).reshape(blocks // 8, 8, nodes), axis=0)
        both = cosines[pl.ds(n, 1), :] * by_cosine - sines[pl.ds(n, 1), :] * by_sine
        partial[pl.ds(n, 1), :] = jnp.sum(both, axis=0, keepdims=True)

    def reverse_near(n):
        pulled[...] = matmul(near_t[...], split[...])
        for k in range(slots):
            for start in range(0, blocks, CHUNK):
                some = slice(start, start + CHUNK)
                totals = [None] * comps
                for e in range(comps):
                    if k == 0:
                        term = metric[some, :] * adjoint[e, some, :]
                    else:
                        row = (k - 1) * blocks + start
                        term = pulled[row : row + CHUNK, lane(e)]
                    for c in range(comps):
                        more = mixing[k, e, c] * term
                        totals[c] = more if totals[c] is None else totals[c] + more
                for c in range(comps):
                    mixed[c * blocks + start : c * blocks + start + CHUNK, lane(k)] = totals[c].astype(
                        BF16
                    )
        right = jnp.concatenate([lift[k] for k in range(slots)], axis=0)
        pushed = matmul(mixed[...], right)
        inner = jnp.where(n > 0, 1.0, 0.0).astype(F32)
        for c in range(comps):
            state = states[n, c]
            bent = jnp.tanh(state)
            fall = STEP_SIZE * (1.0 - bent * bent)
            slope[c] = fall
            grown = adjoint[c] + inner * (weight[c] * state)
            base[c] = grown - fall * pushed[c * blocks : (c + 1) * blocks]

    def reverse_far(j):
        for d, offset in enumerate(OFFSETS):

            @pl.when(exists(p + offset))
            def _():
                rev_copy(j, d, p).wait_recv()

        ghost = jnp.concatenate([rev_in[j, d] for d in range(4)], axis=0)
        arrived = matmul(pick_t[...], ghost)
        for c in range(comps):
            adjoint[c] = base[c] - slope[c] * arrived[:, lane(c)]

    loads[0].wait()
    squash(lambda c: states[first, c])
    near_peers = sum(exists(p + offset).astype(jnp.int32) for offset in OFFSETS)
    far_peers = t * (plane - 1 + 2 * (layers - 1))
    pl.semaphore_wait(barrier, near_peers + 1 + far_peers)
    send_forward(0)

    @pl.when(t == 0)
    def _():
        state_copy(0).start()

    loads[1].wait()
    for k in range(slots):
        lift_t[:, lane(k)] = lift[k].astype(F32).T.astype(BF16)
    pick_t[...] = pick[...].T.astype(BF16)
    row_of = lax.broadcasted_iota(jnp.int32, (levels, nodes), 0)
    angles = jnp.zeros((levels, nodes), F32)
    for n in range(levels):
        angles = jnp.where(row_of == n, pitch[n], angles)
    cosines[...] = jnp.cos(angles)
    sines[...] = jnp.sin(angles)
    column = lax.broadcasted_iota(jnp.int32, (blocks, blocks), 1)
    for k in range(1, slots):
        wanted = faces[:, k - 1 : k]
        chosen = jnp.where(wanted == column, 1.0, 0.0)
        near[(k - 1) * blocks : k * blocks, :] = chosen.astype(BF16)
        turned = chosen.T.astype(BF16)
        near_t[(k - 1) * blocks : k * blocks, :blocks] = turned
        near_t[(k - 1) * blocks : k * blocks, blocks:] = turned
    slot_of = lax.rem(column, ghosts)
    for pair in range(2):
        left = faces[:, 2 * pair : 2 * pair + 1] - blocks
        right = faces[:, 2 * pair + 1 : 2 * pair + 2] - blocks
        wanted = jnp.where(column < ghosts, left, right)
        chosen = jnp.where(wanted == slot_of, 1.0, 0.0)
        far[:, pair * blocks : (pair + 1) * blocks] = chosen.astype(BF16)
        turned = chosen.T.astype(BF16)
        far_t[pair * blocks : (pair + 1) * blocks, :blocks] = turned
        far_t[pair * blocks : (pair + 1) * blocks, blocks:] = turned
    loads[2].wait()
    loads[3].wait()
    last = half - 2 + t

    def forward_level(i, carry):
        forward_near(i)
        forward_far(i)

        @pl.when(i < last)
        def _():
            squash(lambda c: states[first + i + 1, c])
            send_forward(i + 1)

        @pl.when(t == 0)
        def _():
            state_copy(i + 1).start()

        return carry

    lax.fori_loop(0, half - 1 + t, forward_level, 0)

    for load in loads[4:]:
        load.wait()

    @pl.when(t == 1)
    def _():
        for e in range(comps):
            adjoint[e] = adjoint[e] + weight[e] * states[levels, e]

        def reverse_level(j, carry):
            n = levels - 1 - j

            @pl.when(n < half)
            def _():
                state_copy(n).wait_recv()

            send_reverse(j)
            reverse_sum(n)
            reverse_near(n)
            reverse_far(j)

            @pl.when(n == half)
            def _():
                kept[...] = adjoint[...]
                keep_copy.start()

            return carry

        lax.fori_loop(0, levels - 1, reverse_level, 0)
        state_copy(0).wait_recv()
        reverse_sum(0)
        plane_parts[spot] = partial[...]
        for r in range(1, plane):
            plane_copy(r).start()
        send_reverse(levels - 1)
        reverse_near(0)
        reverse_far(levels - 1)
        end_copy.start()
        for r in range(1, plane):
            other = lax.rem(spot + r, plane)
            pltpu.make_async_remote_copy(
                src_ref=partial,
                dst_ref=plane_parts.at[other],
                send_sem=plane_send.at[r],
                recv_sem=plane_recv.at[other],
                device_id=(1, p),
                device_id_type=MESH,
            ).wait_recv()
        total = plane_parts[0]
        for s in range(1, plane):
            total = total + plane_parts[s]
        plane_sum[...] = total
        layer_parts[layer] = total
        for r in range(layers):
            layer_copy(r, 0).start()
            if r > 0:
                layer_copy(r, 1).start()

    def layer_wait(r):
        other = lax.rem(layer + r, layers)
        pltpu.make_async_remote_copy(
            src_ref=plane_sum,
            dst_ref=layer_parts.at[other],
            send_sem=layer_send.at[0, r],
            recv_sem=layer_recv.at[other],
            device_id=(1 - t, p),
            device_id_type=MESH,
        ).wait_recv()

    for r in range(1, layers):
        layer_wait(r)

    @pl.when(t == 0)
    def _():
        layer_wait(0)

    total = layer_parts[0]
    for s in range(1, layers):
        total = total + layer_parts[s]
    norm = math.sqrt(comps * nodes * blocks * n_space)
    for n in range(levels):
        grads[n] = STEP_SIZE * jnp.sum(total[n : n + 1, :]) / norm

    def drain(i, carry):
        for d, offset in enumerate(OFFSETS):

            @pl.when(exists(p + offset))
            def _():
                fwd_copy(i, d, p).wait_send()

        return carry

    lax.fori_loop(0, half - 1 + t, drain, 0)

    @pl.when(t == 0)
    def _():
        end_copy.wait_recv()
        for i in range(half):
            state_copy(i).wait_send()

    @pl.when(t == 1)
    def _():
        def drain_reverse(j, carry):
            for d, offset in enumerate(OFFSETS):

                @pl.when(exists(p - offset))
                def _():
                    rev_copy(j, d, p).wait_send()

            return carry

        lax.fori_loop(0, levels, drain_reverse, 0)
        keep_copy.wait()
        end_copy.wait_send()
        for r in range(1, plane):
            plane_copy(r).wait_send()
        for r in range(layers):
            layer_copy(r, 0).wait_send()
            if r > 0:
                layer_copy(r, 1).wait_send()


def solution(mesh):
    n_space = mesh.shape["space"]
    plane = 16 if n_space % 16 == 0 else 4

    def shards(
        checkpoints, sources, pitch, metric, obj_weight, adjoint_end, lift, mixing, faces, send_idx
    ):
        comps, blocks, nodes = obj_weight.shape
        slots = lift.shape[0]
        levels = pitch.shape[0]
        half = levels // 2
        halo = send_idx.shape[2]
        ghosts = 4 * halo
        wide = comps * nodes
        links = slots - 1
        layers = n_space // plane
        vmem = pltpu.VMEM
        dma = pltpu.SemaphoreType.DMA
        field = (comps, blocks, nodes)
        scratch = [
            vmem((levels + 1, *field), F32),
            vmem((2, *field), F32),
            vmem((blocks, nodes), F32),
            vmem(field, F32),
            vmem(field, F32),
            vmem(field, F32),
            vmem((slots, nodes, nodes), BF16),
            vmem((nodes, slots * nodes), BF16),
            vmem((levels, nodes), F32),
            vmem((levels, nodes), F32),
            vmem((ghosts, blocks), F32),
            vmem((blocks, ghosts), BF16),
            vmem((links * blocks, blocks), BF16),
            vmem((links * blocks, 2 * blocks), BF16),
            vmem((blocks, links * ghosts), BF16),
            vmem((links * ghosts, 2 * blocks), BF16),
            vmem((blocks, wide), BF16),
            vmem((links * blocks, wide), BF16),
            vmem((slots, comps * blocks, nodes), F32),
            vmem(field, F32),
            vmem(field, F32),
            vmem((comps * ghosts, links * nodes), F32),
            vmem((links * ghosts, wide), BF16),
            vmem((2 * blocks, wide), BF16),
            vmem((links * blocks, wide), F32),
            vmem((links * ghosts, wide), F32),
            vmem((comps * blocks, slots * nodes), BF16),
            vmem((comps * ghosts, links * nodes), BF16),
            vmem((half, 4, halo, wide), BF16),
            vmem((half, 4, halo, wide), BF16),
            vmem((levels, 4, halo, wide), BF16),
            vmem((levels, 4, halo, wide), BF16),
            vmem((levels, nodes), F32),
            vmem((plane, levels, nodes), F32),
            vmem((levels, nodes), F32),
            vmem((layers, levels, nodes), F32),
            dma((6,)),
            dma((half, 4)),
            dma((half, 4)),
            dma((levels, 4)),
            dma((levels, 4)),
            dma((half,)),
            dma((half,)),
            dma((plane,)),
            dma((plane,)),
            dma((2, layers)),
            dma((layers,)),
            dma((2,)),
            dma,
        ]
        anywhere = pl.BlockSpec(memory_space=pl.ANY)
        scalars = pl.BlockSpec(memory_space=pltpu.SMEM)
        return pl.pallas_call(
            functools.partial(sweep, n_space, plane),
            out_shape=(
                jax.ShapeDtypeStruct((1, *field), F32),
                jax.ShapeDtypeStruct((levels,), F32),
            ),
            in_specs=[
                anywhere,
                anywhere,
                scalars,
                anywhere,
                anywhere,
                anywhere,
                anywhere,
                scalars,
                pl.BlockSpec(memory_space=pltpu.VMEM),
                scalars,
            ],
            out_specs=(anywhere, scalars),
            scratch_shapes=scratch,
            compiler_params=pltpu.CompilerParams(
                collective_id=0, has_side_effects=True, vmem_limit_bytes=48 * 1024 * 1024
            ),
            name="adjoint_window",
        )(checkpoints, sources, pitch, metric, obj_weight, adjoint_end, lift, mixing, faces, send_idx)

    return jax.shard_map(
        shards,
        mesh=mesh,
        in_specs=(
            P("tm", None, "space", None),
            P(None, None, "space", None),
            P(),
            P("space", None),
            P(None, "space", None),
            P(None, "space", None),
            P(),
            P(),
            P("space", None),
            P("space", None, None),
        ),
        out_specs=(P("tm", None, "space", None), P()),
        check_vma=False,
    )
```

```python
import functools
import math

import jax
import jax.numpy as jnp
from jax import lax
from jax.experimental import pallas as pl
from jax.experimental.pallas import tpu as pltpu
from jax.sharding import PartitionSpec as P

OFFSETS = (1, -1, 2, -2)
FARTHEST_FIRST = (2, 3, 0, 1)
STEP_SIZE = 0.5
MESH = pl.DeviceIdType.MESH
F32, BF16 = jnp.float32, jnp.bfloat16
CHUNK = 32


def matmul(left, right):
    return jnp.dot(left, right, preferred_element_type=F32)


def sweep(
    n_space,
    plane,
    checkpoint_in,
    sources_in,
    pitch,
    metric_in,
    weight_in,
    end_in,
    lift_in,
    mixing,
    faces,
    send_idx,
    bounds,
    grads,
    states,
    sources,
    metric,
    weight,
    adjoint,
    kept,
    lift,
    lift_t,
    cosines,
    sines,
    pick,
    pick_t,
    near,
    near_t,
    far,
    far_t,
    squashed,
    gathered,
    lifted,
    base,
    slope,
    halo_lifted,
    halo_mixed,
    split,
    pulled,
    halo_pulled,
    mixed,
    far_mixed,
    fwd_out,
    fwd_in,
    rev_out,
    rev_in,
    partial,
    plane_parts,
    plane_sum,
    layer_parts,
    in_sem,
    fwd_send,
    fwd_recv,
    rev_send,
    rev_recv,
    state_send,
    state_recv,
    plane_send,
    plane_recv,
    layer_send,
    layer_recv,
    end_sem,
    out_sem,
):
    comps, blocks, nodes = states.shape[1:]
    slots = lift.shape[0]
    halo = fwd_in.shape[2]
    ghosts = 4 * halo
    levels = pitch.shape[0]
    half = levels // 2
    layers = n_space // plane
    t = lax.axis_index("tm")
    p = lax.axis_index("space")
    spot = lax.rem(p, plane)
    layer = p // plane
    first = t * half

    def exists(q):
        return jnp.logical_and(q >= 0, q < n_space)

    def lane(c):
        return slice(c * nodes, (c + 1) * nodes)

    loads = [
        pltpu.make_async_copy(checkpoint_in.at[0], states.at[first], in_sem.at[0]),
        pltpu.make_async_copy(lift_in, lift, in_sem.at[1]),
        pltpu.make_async_copy(metric_in, metric, in_sem.at[2]),
        pltpu.make_async_copy(sources_in, sources, in_sem.at[3]),
        pltpu.make_async_copy(weight_in, weight, in_sem.at[4]),
        pltpu.make_async_copy(end_in, adjoint, in_sem.at[5]),
    ]
    for load in loads:
        load.start()

    barrier = pltpu.get_barrier_semaphore()

    def greet(device):
        pl.semaphore_signal(barrier, inc=1, device_id=device, device_id_type=MESH)

    for offset in OFFSETS:

        @pl.when(exists(p + offset))
        def _():
            greet((t, p + offset))

    greet((1 - t, p))
    for r in range(1, layers):
        greet((1, lax.rem(layer + r, layers) * plane + spot))

    @pl.when(t == 1)
    def _():
        for r in range(1, plane):
            greet((1, layer * plane + lax.rem(spot + r, plane)))

    lane_of = lax.broadcasted_iota(jnp.int32, (1, blocks), 1)
    for d in range(4):
        for s in range(halo):
            row = d * halo + s
            pick[pl.ds(row, 1), :] = jnp.where(lane_of == send_idx[0, d, s], 1.0, 0.0)

    for d, offset in enumerate(OFFSETS):

        @pl.when(jnp.logical_not(exists(p - offset)))
        def _():
            for i in range(half):
                fwd_in[i, d] = jnp.zeros(fwd_in.shape[2:], BF16)

        @pl.when(jnp.logical_not(exists(p + offset)))
        def _():
            for i in range(levels):
                rev_in[i, d] = jnp.zeros(rev_in.shape[2:], BF16)

    def fwd_copy(i, d, device):
        return pltpu.make_async_remote_copy(
            src_ref=fwd_out.at[i, d],
            dst_ref=fwd_in.at[i, d],
            send_sem=fwd_send.at[i, d],
            recv_sem=fwd_recv.at[i, d],
            device_id=(t, device),
            device_id_type=MESH,
        )

    def rev_copy(i, d, device):
        return pltpu.make_async_remote_copy(
            src_ref=rev_out.at[i, d],
            dst_ref=rev_in.at[i, d],
            send_sem=rev_send.at[i, d],
            recv_sem=rev_recv.at[i, d],
            device_id=(t, device),
            device_id_type=MESH,
        )

    def state_copy(i):
        return pltpu.make_async_remote_copy(
            src_ref=states.at[i],
            dst_ref=states.at[i],
            send_sem=state_send.at[i],
            recv_sem=state_recv.at[i],
            device_id=(1 - t, p),
            device_id_type=MESH,
        )

    def plane_copy(r):
        return pltpu.make_async_remote_copy(
            src_ref=partial,
            dst_ref=plane_parts.at[spot],
            send_sem=plane_send.at[r],
            recv_sem=plane_recv.at[spot],
            device_id=(1, layer * plane + lax.rem(spot + r, plane)),
            device_id_type=MESH,
        )

    def layer_copy(r, core):
        return pltpu.make_async_remote_copy(
            src_ref=plane_sum,
            dst_ref=layer_parts.at[layer],
            send_sem=layer_send.at[core, r],
            recv_sem=layer_recv.at[layer],
            device_id=(core, lax.rem(layer + r, layers) * plane + spot),
            device_id_type=MESH,
        )

    end_copy = pltpu.make_async_remote_copy(
        src_ref=adjoint,
        dst_ref=bounds.at[0],
        send_sem=end_sem.at[0],
        recv_sem=end_sem.at[1],
        device_id=(1 - t, p),
        device_id_type=MESH,
    )
    keep_copy = pltpu.make_async_copy(kept, bounds.at[0], out_sem)

    def squash(state):
        for c in range(comps):
            squashed[:, lane(c)] = jnp.tanh(state(c)).astype(BF16)

    def send_forward(i):
        packets = matmul(pick[...].astype(BF16), squashed[...]).astype(BF16)
        for d in FARTHEST_FIRST:
            fwd_out[i, d] = packets[d * halo : (d + 1) * halo]

            @pl.when(exists(p + OFFSETS[d]))
            def _():
                fwd_copy(i, d, p + OFFSETS[d]).start()

    def forward_near(i):
        gathered[...] = matmul(near[...], squashed[...]).astype(BF16)
        for k in range(slots):
            rows = squashed if k == 0 else gathered.at[pl.ds((k - 1) * blocks, blocks)]
            left = jnp.concatenate([rows[:, lane(c)] for c in range(comps)], axis=0)
            lifted[k] = matmul(left, lift_t[:, lane(k)])
        cosine = cosines[pl.ds(first + i, 1), :]
        sine = sines[pl.ds(first + i, 1), :]
        for start in range(0, blocks, CHUNK):
            some = slice(start, start + CHUNK)
            totals = [None] * comps
            for k in range(slots):
                for c in range(comps):
                    term = lifted[k, c * blocks + start : c * blocks + start + CHUNK, :]
                    for e in range(comps):
                        more = mixing[k, e, c] * term
                        totals[e] = more if totals[e] is None else totals[e] + more
            for e in range(comps):
                forcing = cosine * sources[0, e, some, :] + sine * sources[1, e, some, :]
                change = forcing - metric[some, :] * totals[e]
                base[e, some, :] = states[first + i, e, some, :] + STEP_SIZE * change

    def forward_far(i):
        for d, offset in enumerate(OFFSETS):

            @pl.when(exists(p - offset))
            def _():
                fwd_copy(i, d, p).wait_recv()

        ghost = jnp.concatenate([fwd_in[i, d] for d in range(4)], axis=0)
        left = jnp.concatenate([ghost[:, lane(c)] for c in range(comps)], axis=0)
        halo_lifted[...] = matmul(left, lift_t[:, nodes:])
        for k in range(1, slots):
            for start in range(0, ghosts, CHUNK):
                totals = [None] * comps
                for c in range(comps):
                    term = halo_lifted[c * ghosts + start : c * ghosts + start + CHUNK, lane(k - 1)]
                    for e in range(comps):
                        more = mixing[k, e, c] * term
                        totals[e] = more if totals[e] is None else totals[e] + more
                row = (k - 1) * ghosts + start
                for e in range(comps):
                    halo_mixed[row : row + CHUNK, lane(e)] = totals[e].astype(BF16)
        scale = STEP_SIZE * metric[...]
        arrived = matmul(far[...], halo_mixed[...])
        for e in range(comps):
            states[first + i + 1, e] = base[e] - scale * arrived[:, lane(e)]

    def send_reverse(j):
        for e in range(comps):
            weighted = metric[...] * adjoint[e]
            high = weighted.astype(BF16)
            split[:blocks, lane(e)] = high
            split[blocks:, lane(e)] = (weighted - high.astype(F32)).astype(BF16)
        halo_pulled[...] = matmul(far_t[...], split[...])
        for k in range(1, slots):
            for start in range(0, ghosts, CHUNK):
                row = (k - 1) * ghosts + start
                totals = [None] * comps
                for e in range(comps):
                    term = halo_pulled[row : row + CHUNK, lane(e)]
                    for c in range(comps):
                        more = mixing[k, e, c] * term
                        totals[c] = more if totals[c] is None else totals[c] + more
                for c in range(comps):
                    far_mixed[c * ghosts + start : c * ghosts + start + CHUNK, lane(k - 1)] = totals[
                        c
                    ].astype(BF16)
        right = jnp.concatenate([lift[k] for k in range(1, slots)], axis=0)
        packets = matmul(far_mixed[...], right).astype(BF16)
        for d in FARTHEST_FIRST:
            for c in range(comps):
                row = c * ghosts + d * halo
                rev_out[j, d, :, lane(c)] = packets[row : row + halo]

            @pl.when(exists(p - OFFSETS[d]))
            def _():
                rev_copy(j, d, p - OFFSETS[d]).start()

    def reverse_sum(n):
        by_cosine = jnp.zeros((8, nodes), F32)
        by_sine = jnp.zeros((8, nodes), F32)
        for e in range(comps):
            value = adjoint[e]
            by_cosine += jnp.sum((value * sources[1, e]).reshape(blocks // 8, 8, nodes), axis=0)
            by_sine += jnp.sum((value * sources[0, e]).reshape(blocks // 8, 8, nodes), axis=0)
        both = cosines[pl.ds(n, 1), :] * by_cosine - sines[pl.ds(n, 1), :] * by_sine
        partial[pl.ds(n, 1), :] = jnp.sum(both, axis=0, keepdims=True)

    def reverse_near(n):
        pulled[...] = matmul(near_t[...], split[...])
        for k in range(slots):
            for start in range(0, blocks, CHUNK):
                some = slice(start, start + CHUNK)
                totals = [None] * comps
                for e in range(comps):
                    if k == 0:
                        term = metric[some, :] * adjoint[e, some, :]
                    else:
                        row = (k - 1) * blocks + start
                        term = pulled[row : row + CHUNK, lane(e)]
                    for c in range(comps):
                        more = mixing[k, e, c] * term
                        totals[c] = more if totals[c] is None else totals[c] + more
                for c in range(comps):
                    mixed[c * blocks + start : c * blocks + start + CHUNK, lane(k)] = totals[c].astype(
                        BF16
                    )
        right = jnp.concatenate([lift[k] for k in range(slots)], axis=0)
        pushed = matmul(mixed[...], right)
        inner = jnp.where(n > 0, 1.0, 0.0).astype(F32)
        for c in range(comps):
            state = states[n, c]
            bent = jnp.tanh(state)
            fall = STEP_SIZE * (1.0 - bent * bent)
            slope[c] = fall
            grown = adjoint[c] + inner * (weight[c] * state)
            base[c] = grown - fall * pushed[c * blocks : (c + 1) * blocks]

    def reverse_far(j):
        for d, offset in enumerate(OFFSETS):

            @pl.when(exists(p + offset))
            def _():
                rev_copy(j, d, p).wait_recv()

        ghost = jnp.concatenate([rev_in[j, d] for d in range(4)], axis=0)
        arrived = matmul(pick_t[...], ghost)
        for c in range(comps):
            adjoint[c] = base[c] - slope[c] * arrived[:, lane(c)]

    loads[0].wait()
    squash(lambda c: states[first, c])
    near_peers = sum(exists(p + offset).astype(jnp.int32) for offset in OFFSETS)
    far_peers = t * (plane - 1 + 2 * (layers - 1))
    pl.semaphore_wait(barrier, near_peers + 1 + far_peers)
    send_forward(0)

    @pl.when(t == 0)
    def _():
        state_copy(0).start()

    loads[1].wait()
    for k in range(slots):
        lift_t[:, lane(k)] = lift[k].astype(F32).T.astype(BF16)
    pick_t[...] = pick[...].T.astype(BF16)
    row_of = lax.broadcasted_iota(jnp.int32, (levels, nodes), 0)
    angles = jnp.zeros((levels, nodes), F32)
    for n in range(levels):
        angles = jnp.where(row_of == n, pitch[n], angles)
    cosines[...] = jnp.cos(angles)
    sines[...] = jnp.sin(angles)
    row_at = lax.broadcasted_iota(jnp.int32, (blocks, blocks), 0)
    for k in range(1, slots):
        chosen = jnp.where(faces[k - 1 : k, :] == row_at, 1.0, 0.0)
        near[(k - 1) * blocks : k * blocks, :] = chosen.T.astype(BF16)
        turned = chosen.astype(BF16)
        near_t[(k - 1) * blocks : k * blocks, :blocks] = turned
        near_t[(k - 1) * blocks : k * blocks, blocks:] = turned
    slot_at = lax.rem(row_at, ghosts)
    for pair in range(2):
        upper = faces[2 * pair : 2 * pair + 1, :] - blocks
        lower = faces[2 * pair + 1 : 2 * pair + 2, :] - blocks
        wanted = jnp.where(row_at < ghosts, upper, lower)
        chosen = jnp.where(wanted == slot_at, 1.0, 0.0)
        far[:, pair * blocks : (pair + 1) * blocks] = chosen.T.astype(BF16)
        turned = chosen.astype(BF16)
        far_t[pair * blocks : (pair + 1) * blocks, :blocks] = turned
        far_t[pair * blocks : (pair + 1) * blocks, blocks:] = turned
    loads[2].wait()
    loads[3].wait()
    last = half - 2 + t

    def forward_level(i, carry):
        forward_near(i)
        forward_far(i)

        @pl.when(i < last)
        def _():
            squash(lambda c: states[first + i + 1, c])
            send_forward(i + 1)

        @pl.when(t == 0)
        def _():
            state_copy(i + 1).start()

        return carry

    lax.fori_loop(0, half - 1 + t, forward_level, 0)

    for load in loads[4:]:
        load.wait()

    @pl.when(t == 1)
    def _():
        for e in range(comps):
            adjoint[e] = adjoint[e] + weight[e] * states[levels, e]

        def reverse_level(j, carry):
            n = levels - 1 - j

            @pl.when(n < half)
            def _():
                state_copy(n).wait_recv()

            send_reverse(j)
            reverse_sum(n)
            reverse_near(n)
            reverse_far(j)

            @pl.when(n == half)
            def _():
                kept[...] = adjoint[...]
                keep_copy.start()

            return carry

        lax.fori_loop(0, levels - 1, reverse_level, 0)
        state_copy(0).wait_recv()
        reverse_sum(0)
        plane_parts[spot] = partial[...]
        for r in range(1, plane):
            plane_copy(r).start()
        send_reverse(levels - 1)
        reverse_near(0)
        reverse_far(levels - 1)
        end_copy.start()
        for r in range(1, plane):
            other = lax.rem(spot + r, plane)
            pltpu.make_async_remote_copy(
                src_ref=partial,
                dst_ref=plane_parts.at[other],
                send_sem=plane_send.at[r],
                recv_sem=plane_recv.at[other],
                device_id=(1, p),
                device_id_type=MESH,
            ).wait_recv()
        total = plane_parts[0]
        for s in range(1, plane):
            total = total + plane_parts[s]
        plane_sum[...] = total
        layer_parts[layer] = total
        for r in range(layers):
            layer_copy(r, 0).start()
            if r > 0:
                layer_copy(r, 1).start()

    def layer_wait(r):
        other = lax.rem(layer + r, layers)
        pltpu.make_async_remote_copy(
            src_ref=plane_sum,
            dst_ref=layer_parts.at[other],
            send_sem=layer_send.at[0, r],
            recv_sem=layer_recv.at[other],
            device_id=(1 - t, p),
            device_id_type=MESH,
        ).wait_recv()

    for r in range(1, layers):
        layer_wait(r)

    @pl.when(t == 0)
    def _():
        layer_wait(0)

    total = layer_parts[0]
    for s in range(1, layers):
        total = total + layer_parts[s]
    norm = math.sqrt(comps * nodes * blocks * n_space)
    for n in range(levels):
        grads[n] = STEP_SIZE * jnp.sum(total[n : n + 1, :]) / norm

    def drain(i, carry):
        for d, offset in enumerate(OFFSETS):

            @pl.when(exists(p + offset))
            def _():
                fwd_copy(i, d, p).wait_send()

        return carry

    lax.fori_loop(0, half - 1 + t, drain, 0)

    @pl.when(t == 0)
    def _():
        end_copy.wait_recv()
        for i in range(half):
            state_copy(i).wait_send()

    @pl.when(t == 1)
    def _():
        def drain_reverse(j, carry):
            for d, offset in enumerate(OFFSETS):

                @pl.when(exists(p - offset))
                def _():
                    rev_copy(j, d, p).wait_send()

            return carry

        lax.fori_loop(0, levels, drain_reverse, 0)
        keep_copy.wait()
        end_copy.wait_send()
        for r in range(1, plane):
            plane_copy(r).wait_send()
        for r in range(layers):
            layer_copy(r, 0).wait_send()
            if r > 0:
                layer_copy(r, 1).wait_send()


def solution(mesh):
    n_space = mesh.shape["space"]
    plane = 16 if n_space % 16 == 0 else 4

    def shards(
        checkpoints, sources, pitch, metric, obj_weight, adjoint_end, lift, mixing, faces, send_idx
    ):
        comps, blocks, nodes = obj_weight.shape
        slots = lift.shape[0]
        levels = pitch.shape[0]
        half = levels // 2
        halo = send_idx.shape[2]
        ghosts = 4 * halo
        wide = comps * nodes
        links = slots - 1
        layers = n_space // plane
        vmem = pltpu.VMEM
        dma = pltpu.SemaphoreType.DMA
        field = (comps, blocks, nodes)
        scratch = [
            vmem((levels + 1, *field), F32),
            vmem((2, *field), F32),
            vmem((blocks, nodes), F32),
            vmem(field, F32),
            vmem(field, F32),
            vmem(field, F32),
            vmem((slots, nodes, nodes), BF16),
            vmem((nodes, slots * nodes), BF16),
            vmem((levels, nodes), F32),
            vmem((levels, nodes), F32),
            vmem((ghosts, blocks), F32),
            vmem((blocks, ghosts), BF16),
            vmem((links * blocks, blocks), BF16),
            vmem((links * blocks, 2 * blocks), BF16),
            vmem((blocks, links * ghosts), BF16),
            vmem((links * ghosts, 2 * blocks), BF16),
            vmem((blocks, wide), BF16),
            vmem((links * blocks, wide), BF16),
            vmem((slots, comps * blocks, nodes), F32),
            vmem(field, F32),
            vmem(field, F32),
            vmem((comps * ghosts, links * nodes), F32),
            vmem((links * ghosts, wide), BF16),
            vmem((2 * blocks, wide), BF16),
            vmem((links * blocks, wide), F32),
            vmem((links * ghosts, wide), F32),
            vmem((comps * blocks, slots * nodes), BF16),
            vmem((comps * ghosts, links * nodes), BF16),
            vmem((half, 4, halo, wide), BF16),
            vmem((half, 4, halo, wide), BF16),
            vmem((levels, 4, halo, wide), BF16),
            vmem((levels, 4, halo, wide), BF16),
            vmem((levels, nodes), F32),
            vmem((plane, levels, nodes), F32),
            vmem((levels, nodes), F32),
            vmem((layers, levels, nodes), F32),
            dma((6,)),
            dma((half, 4)),
            dma((half, 4)),
            dma((levels, 4)),
            dma((levels, 4)),
            dma((half,)),
            dma((half,)),
            dma((plane,)),
            dma((plane,)),
            dma((2, layers)),
            dma((layers,)),
            dma((2,)),
            dma,
        ]
        anywhere = pl.BlockSpec(memory_space=pl.ANY)
        scalars = pl.BlockSpec(memory_space=pltpu.SMEM)
        return pl.pallas_call(
            functools.partial(sweep, n_space, plane),
            out_shape=(
                jax.ShapeDtypeStruct((1, *field), F32),
                jax.ShapeDtypeStruct((levels,), F32),
            ),
            in_specs=[
                anywhere,
                anywhere,
                scalars,
                anywhere,
                anywhere,
                anywhere,
                anywhere,
                scalars,
                pl.BlockSpec(memory_space=pltpu.VMEM),
                scalars,
            ],
            out_specs=(anywhere, scalars),
            scratch_shapes=scratch,
            compiler_params=pltpu.CompilerParams(
                collective_id=0, has_side_effects=True, vmem_limit_bytes=67043328
            ),
            name="adjoint_window",
        )(checkpoints, sources, pitch, metric, obj_weight, adjoint_end, lift, mixing, faces.T, send_idx)

    return jax.shard_map(
        shards,
        mesh=mesh,
        in_specs=(
            P("tm", None, "space", None),
            P(None, None, "space", None),
            P(),
            P("space", None),
            P(None, "space", None),
            P(None, "space", None),
            P(),
            P(),
            P("space", None),
            P("space", None, None),
        ),
        out_specs=(P("tm", None, "space", None), P()),
        check_vma=False,
    )
```

```python
import functools
import math

import jax
import jax.numpy as jnp
from jax import lax
from jax.experimental import pallas as pl
from jax.experimental.pallas import tpu as pltpu
from jax.sharding import PartitionSpec as P

OFFSETS = (1, -1, 2, -2)
FARTHEST_FIRST = (2, 3, 0, 1)
STEP_SIZE = 0.5
MESH = pl.DeviceIdType.MESH
F32, BF16 = jnp.float32, jnp.bfloat16
CHUNK = 32


def matmul(left, right):
    return jnp.dot(left, right, preferred_element_type=F32)


def sweep(
    n_space,
    plane,
    checkpoint_in,
    sources_in,
    pitch,
    metric_in,
    weight_in,
    end_in,
    lift_in,
    mixing,
    faces,
    send_idx,
    bounds,
    grads,
    states,
    sources,
    metric,
    weight,
    adjoint,
    kept,
    lift,
    lift_t,
    cosines,
    sines,
    pick,
    pick_t,
    near,
    near_t,
    far,
    far_t,
    squashed,
    gathered,
    lifted,
    base,
    slope,
    halo_lifted,
    halo_mixed,
    split,
    pulled,
    halo_pulled,
    mixed,
    far_mixed,
    fwd_out,
    fwd_in,
    rev_out,
    rev_in,
    bend_out,
    bend_in,
    bend_there,
    partial,
    plane_parts,
    plane_sum,
    layer_parts,
    in_sem,
    fwd_send,
    fwd_recv,
    rev_send,
    rev_recv,
    bend_send,
    bend_recv,
    bend_sem,
    state_send,
    state_recv,
    plane_send,
    plane_recv,
    layer_send,
    layer_recv,
    end_sem,
    out_sem,
):
    comps, blocks, nodes = states.shape[1:]
    slots = lift.shape[0]
    halo = fwd_in.shape[2]
    ghosts = 4 * halo
    levels = pitch.shape[0]
    half = levels // 2
    layers = n_space // plane
    t = lax.axis_index("tm")
    p = lax.axis_index("space")
    spot = lax.rem(p, plane)
    layer = p // plane
    first = t * half

    def exists(q):
        return jnp.logical_and(q >= 0, q < n_space)

    def lane(c):
        return slice(c * nodes, (c + 1) * nodes)

    loads = [
        pltpu.make_async_copy(checkpoint_in.at[0], states.at[first], in_sem.at[0]),
        pltpu.make_async_copy(lift_in, lift, in_sem.at[1]),
        pltpu.make_async_copy(metric_in, metric, in_sem.at[2]),
        pltpu.make_async_copy(sources_in, sources, in_sem.at[3]),
        pltpu.make_async_copy(weight_in, weight, in_sem.at[4]),
        pltpu.make_async_copy(end_in, adjoint, in_sem.at[5]),
    ]
    for load in loads:
        load.start()

    barrier = pltpu.get_barrier_semaphore()

    def greet(device):
        pl.semaphore_signal(barrier, inc=1, device_id=device, device_id_type=MESH)

    for offset in OFFSETS:

        @pl.when(exists(p + offset))
        def _():
            greet((t, p + offset))

    greet((1 - t, p))

    for r in range(1, layers):
        greet((1, lax.rem(layer + r, layers) * plane + spot))

    @pl.when(t == 1)
    def _():
        for r in range(1, plane):
            greet((1, layer * plane + lax.rem(spot + r, plane)))

    lane_of = lax.broadcasted_iota(jnp.int32, (1, blocks), 1)
    for d in range(4):
        for s in range(halo):
            row = d * halo + s
            pick[pl.ds(row, 1), :] = jnp.where(lane_of == send_idx[0, d, s], 1.0, 0.0)

    for d, offset in enumerate(OFFSETS):

        @pl.when(jnp.logical_not(exists(p - offset)))
        def _():
            bend_in[d] = jnp.zeros(bend_in.shape[1:], BF16)
            for i in range(half):
                fwd_in[i, d] = jnp.zeros(fwd_in.shape[2:], BF16)

        @pl.when(jnp.logical_not(exists(p + offset)))
        def _():
            for i in range(levels):
                rev_in[i, d] = jnp.zeros(rev_in.shape[2:], BF16)

    def fwd_copy(i, d, device):
        return pltpu.make_async_remote_copy(
            src_ref=fwd_out.at[i, d],
            dst_ref=fwd_in.at[i, d],
            send_sem=fwd_send.at[i, d],
            recv_sem=fwd_recv.at[i, d],
            device_id=(t, device),
            device_id_type=MESH,
        )

    def rev_copy(i, d, device):
        return pltpu.make_async_remote_copy(
            src_ref=rev_out.at[i, d],
            dst_ref=rev_in.at[i, d],
            send_sem=rev_send.at[i, d],
            recv_sem=rev_recv.at[i, d],
            device_id=(t, device),
            device_id_type=MESH,
        )

    def bend_copy(d, device):
        return pltpu.make_async_remote_copy(
            src_ref=bend_out.at[d],
            dst_ref=bend_in.at[d],
            send_sem=bend_send.at[d],
            recv_sem=bend_recv.at[d],
            device_id=(t, device),
            device_id_type=MESH,
        )

    def state_copy(i):
        return pltpu.make_async_remote_copy(
            src_ref=states.at[i],
            dst_ref=states.at[i],
            send_sem=state_send.at[i],
            recv_sem=state_recv.at[i],
            device_id=(1 - t, p),
            device_id_type=MESH,
        )

    def plane_copy(r):
        return pltpu.make_async_remote_copy(
            src_ref=partial,
            dst_ref=plane_parts.at[spot],
            send_sem=plane_send.at[r],
            recv_sem=plane_recv.at[spot],
            device_id=(1, layer * plane + lax.rem(spot + r, plane)),
            device_id_type=MESH,
        )

    def layer_copy(r, core):
        return pltpu.make_async_remote_copy(
            src_ref=plane_sum,
            dst_ref=layer_parts.at[layer],
            send_sem=layer_send.at[core, r],
            recv_sem=layer_recv.at[layer],
            device_id=(core, lax.rem(layer + r, layers) * plane + spot),
            device_id_type=MESH,
        )

    bend_pass = pltpu.make_async_remote_copy(
        src_ref=bend_in,
        dst_ref=bend_there,
        send_sem=bend_sem.at[0],
        recv_sem=bend_sem.at[1],
        device_id=(1 - t, p),
        device_id_type=MESH,
    )
    end_copy = pltpu.make_async_remote_copy(
        src_ref=adjoint,
        dst_ref=bounds.at[0],
        send_sem=end_sem.at[0],
        recv_sem=end_sem.at[1],
        device_id=(1 - t, p),
        device_id_type=MESH,
    )
    keep_copy = pltpu.make_async_copy(kept, bounds.at[0], out_sem)

    def squash(state):
        for c in range(comps):
            squashed[:, lane(c)] = jnp.tanh(state(c)).astype(BF16)

    def send_forward(i):
        packets = matmul(pick[...].astype(BF16), squashed[...]).astype(BF16)
        for d in FARTHEST_FIRST:
            fwd_out[i, d] = packets[d * halo : (d + 1) * halo]

            @pl.when(exists(p + OFFSETS[d]))
            def _():
                fwd_copy(i, d, p + OFFSETS[d]).start()

    def forward_near(i):
        gathered[...] = matmul(near[...], squashed[...]).astype(BF16)
        for k in range(slots):
            rows = squashed if k == 0 else gathered.at[pl.ds((k - 1) * blocks, blocks)]
            left = jnp.concatenate([rows[:, lane(c)] for c in range(comps)], axis=0)
            lifted[k] = matmul(left, lift_t[:, lane(k)])
        cosine = cosines[pl.ds(first + i, 1), :]
        sine = sines[pl.ds(first + i, 1), :]
        for start in range(0, blocks, CHUNK):
            some = slice(start, start + CHUNK)
            totals = [None] * comps
            for k in range(slots):
                for c in range(comps):
                    term = lifted[k, c * blocks + start : c * blocks + start + CHUNK, :]
                    for e in range(comps):
                        more = mixing[k, e, c] * term
                        totals[e] = more if totals[e] is None else totals[e] + more
            for e in range(comps):
                forcing = cosine * sources[0, e, some, :] + sine * sources[1, e, some, :]
                change = forcing - metric[some, :] * totals[e]
                base[e, some, :] = states[first + i, e, some, :] + STEP_SIZE * change

    def forward_far(i):
        for d, offset in enumerate(OFFSETS):

            @pl.when(exists(p - offset))
            def _():
                fwd_copy(i, d, p).wait_recv()

        ghost = jnp.concatenate([fwd_in[i, d] for d in range(4)], axis=0)
        left = jnp.concatenate([ghost[:, lane(c)] for c in range(comps)], axis=0)
        halo_lifted[...] = matmul(left, lift_t[:, nodes:])
        for k in range(1, slots):
            for start in range(0, ghosts, CHUNK):
                totals = [None] * comps
                for c in range(comps):
                    term = halo_lifted[c * ghosts + start : c * ghosts + start + CHUNK, lane(k - 1)]
                    for e in range(comps):
                        more = mixing[k, e, c] * term
                        totals[e] = more if totals[e] is None else totals[e] + more
                row = (k - 1) * ghosts + start
                for e in range(comps):
                    halo_mixed[row : row + CHUNK, lane(e)] = totals[e].astype(BF16)
        scale = STEP_SIZE * metric[...]
        arrived = matmul(far[...], halo_mixed[...])
        for e in range(comps):
            states[first + i + 1, e] = base[e] - scale * arrived[:, lane(e)]

    def send_reverse(j):
        for e in range(comps):
            weighted = metric[...] * adjoint[e]
            high = weighted.astype(BF16)
            split[:blocks, lane(e)] = high
            split[blocks:, lane(e)] = (weighted - high.astype(F32)).astype(BF16)
        halo_pulled[...] = matmul(far_t[...], split[...])
        for k in range(1, slots):
            for start in range(0, ghosts, CHUNK):
                row = (k - 1) * ghosts + start
                totals = [None] * comps
                for e in range(comps):
                    term = halo_pulled[row : row + CHUNK, lane(e)]
                    for c in range(comps):
                        more = mixing[k, e, c] * term
                        totals[c] = more if totals[c] is None else totals[c] + more
                for c in range(comps):
                    far_mixed[c * ghosts + start : c * ghosts + start + CHUNK, lane(k - 1)] = totals[
                        c
                    ].astype(BF16)
        right = jnp.concatenate([lift[k] for k in range(1, slots)], axis=0)
        packets = matmul(far_mixed[...], right).astype(BF16)
        for d in FARTHEST_FIRST:
            for c in range(comps):
                row = c * ghosts + d * halo
                rev_out[j, d, :, lane(c)] = packets[row : row + halo]

            @pl.when(exists(p - OFFSETS[d]))
            def _():
                rev_copy(j, d, p - OFFSETS[d]).start()

    def reverse_sum(n, field):
        by_cosine = jnp.zeros((8, nodes), F32)
        by_sine = jnp.zeros((8, nodes), F32)
        for e in range(comps):
            value = field[e]
            by_cosine += jnp.sum((value * sources[1, e]).reshape(blocks // 8, 8, nodes), axis=0)
            by_sine += jnp.sum((value * sources[0, e]).reshape(blocks // 8, 8, nodes), axis=0)
        both = cosines[pl.ds(n, 1), :] * by_cosine - sines[pl.ds(n, 1), :] * by_sine
        partial[pl.ds(n, 1), :] = jnp.sum(both, axis=0, keepdims=True)

    def reverse_near(n):
        pulled[...] = matmul(near_t[...], split[...])
        for k in range(slots):
            for start in range(0, blocks, CHUNK):
                some = slice(start, start + CHUNK)
                totals = [None] * comps
                for e in range(comps):
                    if k == 0:
                        term = metric[some, :] * adjoint[e, some, :]
                    else:
                        row = (k - 1) * blocks + start
                        term = pulled[row : row + CHUNK, lane(e)]
                    for c in range(comps):
                        more = mixing[k, e, c] * term
                        totals[c] = more if totals[c] is None else totals[c] + more
                for c in range(comps):
                    mixed[c * blocks + start : c * blocks + start + CHUNK, lane(k)] = totals[c].astype(
                        BF16
                    )
        right = jnp.concatenate([lift[k] for k in range(slots)], axis=0)
        pushed = matmul(mixed[...], right)
        inner = jnp.where(n > 0, 1.0, 0.0).astype(F32)
        for c in range(comps):
            state = states[n, c]
            bent = jnp.tanh(state)
            fall = STEP_SIZE * (1.0 - bent * bent)
            slope[c] = fall
            grown = adjoint[c] + inner * (weight[c] * state)
            base[c] = grown - fall * pushed[c * blocks : (c + 1) * blocks]

    def reverse_far(j):
        for d, offset in enumerate(OFFSETS):

            @pl.when(exists(p + offset))
            def _():
                rev_copy(j, d, p).wait_recv()

        ghost = jnp.concatenate([rev_in[j, d] for d in range(4)], axis=0)
        arrived = matmul(pick_t[...], ghost)
        for c in range(comps):
            adjoint[c] = base[c] - slope[c] * arrived[:, lane(c)]

    def send_bend():
        for e in range(comps):
            bent = jnp.tanh(states[1, e])
            turning = cosines[0:1, :] * sources[1, e] - sines[0:1, :] * sources[0, e]
            squashed[:, lane(e)] = (STEP_SIZE * (1.0 - bent * bent) * turning).astype(BF16)
        packets = matmul(pick[...].astype(BF16), squashed[...]).astype(BF16)
        for d, offset in enumerate(OFFSETS):
            bend_out[d] = packets[d * halo : (d + 1) * halo]

            @pl.when(exists(p + offset))
            def _():
                bend_copy(d, p + offset).start()

        for d, offset in enumerate(OFFSETS):

            @pl.when(exists(p - offset))
            def _():
                bend_copy(d, p).wait_recv()

        bend_pass.start()

    def last_sum(j):
        reverse_sum(0, base)
        bend_pass.wait_recv()
        sent = jnp.zeros((halo, nodes), F32)
        for d in range(4):
            both = rev_out[j, d].astype(F32) * bend_there[d].astype(F32)
            for c in range(comps):
                sent += both[:, lane(c)]
        partial[0:1, :] = partial[0:1, :] - jnp.sum(sent, axis=0, keepdims=True)

    loads[0].wait()
    squash(lambda c: states[first, c])
    near_peers = sum(exists(p + offset).astype(jnp.int32) for offset in OFFSETS)
    far_peers = t * (plane - 1 + 2 * (layers - 1))
    pl.semaphore_wait(barrier, near_peers + 1 + far_peers)
    send_forward(0)

    @pl.when(t == 0)
    def _():
        state_copy(0).start()

    loads[1].wait()
    for k in range(slots):
        lift_t[:, lane(k)] = lift[k].astype(F32).T.astype(BF16)
    pick_t[...] = pick[...].T.astype(BF16)
    row_of = lax.broadcasted_iota(jnp.int32, (levels, nodes), 0)
    angles = jnp.zeros((levels, nodes), F32)
    for n in range(levels):
        angles = jnp.where(row_of == n, pitch[n], angles)
    cosines[...] = jnp.cos(angles)
    sines[...] = jnp.sin(angles)
    row_at = lax.broadcasted_iota(jnp.int32, (blocks, blocks), 0)
    for k in range(1, slots):
        chosen = jnp.where(faces[k - 1 : k, :] == row_at, 1.0, 0.0)
        near[(k - 1) * blocks : k * blocks, :] = chosen.T.astype(BF16)
        turned = chosen.astype(BF16)
        near_t[(k - 1) * blocks : k * blocks, :blocks] = turned
        near_t[(k - 1) * blocks : k * blocks, blocks:] = turned
    slot_at = lax.rem(row_at, ghosts)
    for pair in range(2):
        upper = faces[2 * pair : 2 * pair + 1, :] - blocks
        lower = faces[2 * pair + 1 : 2 * pair + 2, :] - blocks
        wanted = jnp.where(row_at < ghosts, upper, lower)
        chosen = jnp.where(wanted == slot_at, 1.0, 0.0)
        far[:, pair * blocks : (pair + 1) * blocks] = chosen.T.astype(BF16)
        turned = chosen.astype(BF16)
        far_t[pair * blocks : (pair + 1) * blocks, :blocks] = turned
        far_t[pair * blocks : (pair + 1) * blocks, blocks:] = turned
    loads[2].wait()
    loads[3].wait()
    last = half - 2 + t

    def forward_level(i, carry):
        forward_near(i)
        forward_far(i)

        @pl.when(i < last)
        def _():
            squash(lambda c: states[first + i + 1, c])
            send_forward(i + 1)

        @pl.when(t == 0)
        def _():
            state_copy(i + 1).start()

        return carry

    lax.fori_loop(0, half - 1 + t, forward_level, 0)

    for load in loads[4:]:
        load.wait()

    @pl.when(t == 0)
    def _():
        send_bend()

    @pl.when(t == 1)
    def _():
        for e in range(comps):
            adjoint[e] = adjoint[e] + weight[e] * states[levels, e]

        def reverse_level(j, carry):
            n = levels - 1 - j

            @pl.when(n < half)
            def _():
                state_copy(n).wait_recv()

            send_reverse(j)
            reverse_sum(n, adjoint)
            reverse_near(n)

            reverse_far(j)

            @pl.when(n == half)
            def _():
                kept[...] = adjoint[...]
                keep_copy.start()

            return carry

        lax.fori_loop(0, levels - 2, reverse_level, 0)
        state_copy(1).wait_recv()
        send_reverse(levels - 2)
        reverse_sum(1, adjoint)
        reverse_near(1)
        last_sum(levels - 2)
        plane_parts[spot] = partial[...]
        for r in range(1, plane):
            plane_copy(r).start()
        reverse_far(levels - 2)
        state_copy(0).wait_recv()
        send_reverse(levels - 1)
        reverse_near(0)
        for r in range(1, plane):
            other = lax.rem(spot + r, plane)
            pltpu.make_async_remote_copy(
                src_ref=partial,
                dst_ref=plane_parts.at[other],
                send_sem=plane_send.at[r],
                recv_sem=plane_recv.at[other],
                device_id=(1, p),
                device_id_type=MESH,
            ).wait_recv()
        total = plane_parts[0]
        for s in range(1, plane):
            total = total + plane_parts[s]
        plane_sum[...] = total
        layer_parts[layer] = total
        for r in range(layers):
            layer_copy(r, 0).start()
            if r > 0:
                layer_copy(r, 1).start()
        reverse_far(levels - 1)
        end_copy.start()

    def layer_wait(r):
        other = lax.rem(layer + r, layers)
        pltpu.make_async_remote_copy(
            src_ref=plane_sum,
            dst_ref=layer_parts.at[other],
            send_sem=layer_send.at[0, r],
            recv_sem=layer_recv.at[other],
            device_id=(1 - t, p),
            device_id_type=MESH,
        ).wait_recv()

    for r in range(1, layers):
        layer_wait(r)

    @pl.when(t == 0)
    def _():
        layer_wait(0)

    total = layer_parts[0]
    for s in range(1, layers):
        total = total + layer_parts[s]
    norm = math.sqrt(comps * nodes * blocks * n_space)
    for n in range(levels):
        grads[n] = STEP_SIZE * jnp.sum(total[n : n + 1, :]) / norm

    def drain(i, carry):
        for d, offset in enumerate(OFFSETS):

            @pl.when(exists(p + offset))
            def _():
                fwd_copy(i, d, p).wait_send()

        return carry

    lax.fori_loop(0, half - 1 + t, drain, 0)

    @pl.when(t == 0)
    def _():
        end_copy.wait_recv()
        for i in range(half):
            state_copy(i).wait_send()
        for d, offset in enumerate(OFFSETS):

            @pl.when(exists(p + offset))
            def _():
                bend_copy(d, p).wait_send()

        bend_pass.wait_send()

    @pl.when(t == 1)
    def _():
        def drain_reverse(j, carry):
            for d, offset in enumerate(OFFSETS):

                @pl.when(exists(p - offset))
                def _():
                    rev_copy(j, d, p).wait_send()

            return carry

        lax.fori_loop(0, levels, drain_reverse, 0)
        keep_copy.wait()
        end_copy.wait_send()
        for r in range(1, plane):
            plane_copy(r).wait_send()
        for r in range(layers):
            layer_copy(r, 0).wait_send()
            if r > 0:
                layer_copy(r, 1).wait_send()


def solution(mesh):
    n_space = mesh.shape["space"]
    plane = 16 if n_space % 16 == 0 else 4

    def shards(
        checkpoints, sources, pitch, metric, obj_weight, adjoint_end, lift, mixing, faces, send_idx
    ):
        comps, blocks, nodes = obj_weight.shape
        slots = lift.shape[0]
        levels = pitch.shape[0]
        half = levels // 2
        halo = send_idx.shape[2]
        ghosts = 4 * halo
        wide = comps * nodes
        links = slots - 1
        layers = n_space // plane
        vmem = pltpu.VMEM
        dma = pltpu.SemaphoreType.DMA
        field = (comps, blocks, nodes)
        scratch = [
            vmem((levels + 1, *field), F32),
            vmem((2, *field), F32),
            vmem((blocks, nodes), F32),
            vmem(field, F32),
            vmem(field, F32),
            vmem(field, F32),
            vmem((slots, nodes, nodes), BF16),
            vmem((nodes, slots * nodes), BF16),
            vmem((levels, nodes), F32),
            vmem((levels, nodes), F32),
            vmem((ghosts, blocks), F32),
            vmem((blocks, ghosts), BF16),
            vmem((links * blocks, blocks), BF16),
            vmem((links * blocks, 2 * blocks), BF16),
            vmem((blocks, links * ghosts), BF16),
            vmem((links * ghosts, 2 * blocks), BF16),
            vmem((blocks, wide), BF16),
            vmem((links * blocks, wide), BF16),
            vmem((slots, comps * blocks, nodes), F32),
            vmem(field, F32),
            vmem(field, F32),
            vmem((comps * ghosts, links * nodes), F32),
            vmem((links * ghosts, wide), BF16),
            vmem((2 * blocks, wide), BF16),
            vmem((links * blocks, wide), F32),
            vmem((links * ghosts, wide), F32),
            vmem((comps * blocks, slots * nodes), BF16),
            vmem((comps * ghosts, links * nodes), BF16),
            vmem((half, 4, halo, wide), BF16),
            vmem((half, 4, halo, wide), BF16),
            vmem((levels, 4, halo, wide), BF16),
            vmem((levels, 4, halo, wide), BF16),
            vmem((4, halo, wide), BF16),
            vmem((4, halo, wide), BF16),
            vmem((4, halo, wide), BF16),
            vmem((levels, nodes), F32),
            vmem((plane, levels, nodes), F32),
            vmem((levels, nodes), F32),
            vmem((layers, levels, nodes), F32),
            dma((6,)),
            dma((half, 4)),
            dma((half, 4)),
            dma((levels, 4)),
            dma((levels, 4)),
            dma((4,)),
            dma((4,)),
            dma((2,)),
            dma((half,)),
            dma((half,)),
            dma((plane,)),
            dma((plane,)),
            dma((2, layers)),
            dma((layers,)),
            dma((2,)),
            dma,
        ]
        anywhere = pl.BlockSpec(memory_space=pl.ANY)
        scalars = pl.BlockSpec(memory_space=pltpu.SMEM)
        return pl.pallas_call(
            functools.partial(sweep, n_space, plane),
            out_shape=(
                jax.ShapeDtypeStruct((1, *field), F32),
                jax.ShapeDtypeStruct((levels,), F32),
            ),
            in_specs=[
                anywhere,
                anywhere,
                scalars,
                anywhere,
                anywhere,
                anywhere,
                anywhere,
                scalars,
                pl.BlockSpec(memory_space=pltpu.VMEM),
                scalars,
            ],
            out_specs=(anywhere, scalars),
            scratch_shapes=scratch,
            compiler_params=pltpu.CompilerParams(
                collective_id=0, has_side_effects=True, vmem_limit_bytes=67043328
            ),
            name="adjoint_window",
        )(checkpoints, sources, pitch, metric, obj_weight, adjoint_end, lift, mixing, faces.T, send_idx)

    return jax.shard_map(
        shards,
        mesh=mesh,
        in_specs=(
            P("tm", None, "space", None),
            P(None, None, "space", None),
            P(),
            P("space", None),
            P(None, "space", None),
            P(None, "space", None),
            P(),
            P(),
            P("space", None),
            P("space", None, None),
        ),
        out_specs=(P("tm", None, "space", None), P()),
        check_vma=False,
    )
```

```python
import functools
import math

import jax
import jax.numpy as jnp
from jax import lax
from jax.experimental import pallas as pl
from jax.experimental.pallas import tpu as pltpu
from jax.sharding import PartitionSpec as P

OFFSETS = (1, -1, 2, -2)
FARTHEST_FIRST = (2, 3, 0, 1)
STEP_SIZE = 0.5
MESH = pl.DeviceIdType.MESH
F32, BF16 = jnp.float32, jnp.bfloat16
CHUNK = 32


def matmul(left, right):
    return jnp.dot(left, right, preferred_element_type=F32)


def sweep(
    n_space,
    plane,
    checkpoint_in,
    sources_in,
    pitch,
    metric_in,
    weight_in,
    end_in,
    lift_in,
    mixing,
    faces,
    send_idx,
    bounds,
    grads,
    states,
    sources,
    metric,
    weight,
    adjoint,
    kept,
    lift,
    lift_t,
    cosines,
    sines,
    pick,
    pick_t,
    near,
    near_t,
    far,
    far_t,
    squashed,
    gathered,
    lifted,
    base,
    slope,
    halo_lifted,
    halo_mixed,
    split,
    pulled,
    halo_pulled,
    mixed,
    far_mixed,
    fwd_out,
    fwd_in,
    rev_out,
    rev_in,
    bend_out,
    bend_in,
    bend_there,
    partial,
    plane_parts,
    plane_sum,
    layer_parts,
    in_sem,
    fwd_send,
    fwd_recv,
    rev_send,
    rev_recv,
    bend_send,
    bend_recv,
    bend_sem,
    state_send,
    state_recv,
    plane_send,
    plane_recv,
    layer_send,
    layer_recv,
    end_sem,
    out_sem,
    hello,
):
    comps, blocks, nodes = states.shape[1:]
    slots = lift.shape[0]
    halo = fwd_in.shape[2]
    ghosts = 4 * halo
    levels = pitch.shape[0]
    half = levels // 2
    layers = n_space // plane
    t = lax.axis_index("tm")
    p = lax.axis_index("space")
    spot = lax.rem(p, plane)
    layer = p // plane
    first = t * half

    def exists(q):
        return jnp.logical_and(q >= 0, q < n_space)

    def lane(c):
        return slice(c * nodes, (c + 1) * nodes)

    loads = [
        pltpu.make_async_copy(checkpoint_in.at[0], states.at[first], in_sem.at[0]),
        pltpu.make_async_copy(lift_in, lift, in_sem.at[1]),
        pltpu.make_async_copy(metric_in, metric, in_sem.at[2]),
        pltpu.make_async_copy(sources_in, sources, in_sem.at[3]),
        pltpu.make_async_copy(weight_in, weight, in_sem.at[4]),
        pltpu.make_async_copy(end_in, adjoint, in_sem.at[5]),
    ]
    for load in loads:
        load.start()

    barrier = pltpu.get_barrier_semaphore()

    def greet(device):
        pl.semaphore_signal(barrier, inc=1, device_id=device, device_id_type=MESH)

    for offset in OFFSETS:

        @pl.when(exists(p + offset))
        def _():
            greet((t, p + offset))

    greet((1 - t, p))

    def in_layer(r):
        return (1, lax.rem(layer + r + layers, layers) * plane + spot)

    @pl.when(t == 1)
    def _():
        greet(in_layer(1))
        greet(in_layer(-1))

    def call(which, distance):
        for r in (distance, -distance):
            pl.semaphore_signal(
                hello.at[which], inc=1, device_id=in_layer(r), device_id_type=MESH
            )

    lane_of = lax.broadcasted_iota(jnp.int32, (1, blocks), 1)
    for d in range(4):
        for s in range(halo):
            row = d * halo + s
            pick[pl.ds(row, 1), :] = jnp.where(lane_of == send_idx[0, d, s], 1.0, 0.0)

    for d, offset in enumerate(OFFSETS):

        @pl.when(jnp.logical_not(exists(p - offset)))
        def _():
            bend_in[d] = jnp.zeros(bend_in.shape[1:], BF16)
            for i in range(half):
                fwd_in[i, d] = jnp.zeros(fwd_in.shape[2:], BF16)

        @pl.when(jnp.logical_not(exists(p + offset)))
        def _():
            for i in range(levels):
                rev_in[i, d] = jnp.zeros(rev_in.shape[2:], BF16)

    def fwd_copy(i, d, device):
        return pltpu.make_async_remote_copy(
            src_ref=fwd_out.at[i, d],
            dst_ref=fwd_in.at[i, d],
            send_sem=fwd_send.at[i, d],
            recv_sem=fwd_recv.at[i, d],
            device_id=(t, device),
            device_id_type=MESH,
        )

    def rev_copy(i, d, device):
        return pltpu.make_async_remote_copy(
            src_ref=rev_out.at[i, d],
            dst_ref=rev_in.at[i, d],
            send_sem=rev_send.at[i, d],
            recv_sem=rev_recv.at[i, d],
            device_id=(t, device),
            device_id_type=MESH,
        )

    def bend_copy(d, device):
        return pltpu.make_async_remote_copy(
            src_ref=bend_out.at[d],
            dst_ref=bend_in.at[d],
            send_sem=bend_send.at[d],
            recv_sem=bend_recv.at[d],
            device_id=(t, device),
            device_id_type=MESH,
        )

    def state_copy(i):
        return pltpu.make_async_remote_copy(
            src_ref=states.at[i],
            dst_ref=states.at[i],
            send_sem=state_send.at[i],
            recv_sem=state_recv.at[i],
            device_id=(1 - t, p),
            device_id_type=MESH,
        )

    def plane_copy(r):
        return pltpu.make_async_remote_copy(
            src_ref=partial,
            dst_ref=plane_parts.at[spot],
            send_sem=plane_send.at[r],
            recv_sem=plane_recv.at[spot],
            device_id=(1, layer * plane + lax.rem(spot + r, plane)),
            device_id_type=MESH,
        )

    def layer_copy(r, core):
        return pltpu.make_async_remote_copy(
            src_ref=plane_sum,
            dst_ref=layer_parts.at[layer],
            send_sem=layer_send.at[core, r],
            recv_sem=layer_recv.at[layer],
            device_id=(core, lax.rem(layer + r, layers) * plane + spot),
            device_id_type=MESH,
        )

    bend_pass = pltpu.make_async_remote_copy(
        src_ref=bend_in,
        dst_ref=bend_there,
        send_sem=bend_sem.at[0],
        recv_sem=bend_sem.at[1],
        device_id=(1 - t, p),
        device_id_type=MESH,
    )
    end_copy = pltpu.make_async_remote_copy(
        src_ref=adjoint,
        dst_ref=bounds.at[0],
        send_sem=end_sem.at[0],
        recv_sem=end_sem.at[1],
        device_id=(1 - t, p),
        device_id_type=MESH,
    )
    keep_copy = pltpu.make_async_copy(kept, bounds.at[0], out_sem)

    def squash(state):
        for c in range(comps):
            squashed[:, lane(c)] = jnp.tanh(state(c)).astype(BF16)

    def send_forward(i):
        packets = matmul(pick[...].astype(BF16), squashed[...]).astype(BF16)
        for d in FARTHEST_FIRST:
            fwd_out[i, d] = packets[d * halo : (d + 1) * halo]

            @pl.when(exists(p + OFFSETS[d]))
            def _():
                fwd_copy(i, d, p + OFFSETS[d]).start()

    def forward_near(i):
        gathered[...] = matmul(near[...], squashed[...]).astype(BF16)
        for k in range(slots):
            rows = squashed if k == 0 else gathered.at[pl.ds((k - 1) * blocks, blocks)]
            left = jnp.concatenate([rows[:, lane(c)] for c in range(comps)], axis=0)
            lifted[k] = matmul(left, lift_t[:, lane(k)])
        cosine = cosines[pl.ds(first + i, 1), :]
        sine = sines[pl.ds(first + i, 1), :]
        for start in range(0, blocks, CHUNK):
            some = slice(start, start + CHUNK)
            totals = [None] * comps
            for k in range(slots):
                for c in range(comps):
                    term = lifted[k, c * blocks + start : c * blocks + start + CHUNK, :]
                    for e in range(comps):
                        more = mixing[k, e, c] * term
                        totals[e] = more if totals[e] is None else totals[e] + more
            for e in range(comps):
                forcing = cosine * sources[0, e, some, :] + sine * sources[1, e, some, :]
                change = forcing - metric[some, :] * totals[e]
                base[e, some, :] = states[first + i, e, some, :] + STEP_SIZE * change

    def forward_far(i):
        for d, offset in enumerate(OFFSETS):

            @pl.when(exists(p - offset))
            def _():
                fwd_copy(i, d, p).wait_recv()

        ghost = jnp.concatenate([fwd_in[i, d] for d in range(4)], axis=0)
        left = jnp.concatenate([ghost[:, lane(c)] for c in range(comps)], axis=0)
        halo_lifted[...] = matmul(left, lift_t[:, nodes:])
        for k in range(1, slots):
            for start in range(0, ghosts, CHUNK):
                totals = [None] * comps
                for c in range(comps):
                    term = halo_lifted[c * ghosts + start : c * ghosts + start + CHUNK, lane(k - 1)]
                    for e in range(comps):
                        more = mixing[k, e, c] * term
                        totals[e] = more if totals[e] is None else totals[e] + more
                row = (k - 1) * ghosts + start
                for e in range(comps):
                    halo_mixed[row : row + CHUNK, lane(e)] = totals[e].astype(BF16)
        scale = STEP_SIZE * metric[...]
        arrived = matmul(far[...], halo_mixed[...])
        for e in range(comps):
            states[first + i + 1, e] = base[e] - scale * arrived[:, lane(e)]

    def send_reverse(j):
        for e in range(comps):
            weighted = metric[...] * adjoint[e]
            high = weighted.astype(BF16)
            split[:blocks, lane(e)] = high
            split[blocks:, lane(e)] = (weighted - high.astype(F32)).astype(BF16)
        halo_pulled[...] = matmul(far_t[...], split[...])
        for k in range(1, slots):
            for start in range(0, ghosts, CHUNK):
                row = (k - 1) * ghosts + start
                totals = [None] * comps
                for e in range(comps):
                    term = halo_pulled[row : row + CHUNK, lane(e)]
                    for c in range(comps):
                        more = mixing[k, e, c] * term
                        totals[c] = more if totals[c] is None else totals[c] + more
                for c in range(comps):
                    far_mixed[c * ghosts + start : c * ghosts + start + CHUNK, lane(k - 1)] = totals[
                        c
                    ].astype(BF16)
        right = jnp.concatenate([lift[k] for k in range(1, slots)], axis=0)
        packets = matmul(far_mixed[...], right).astype(BF16)
        for d in FARTHEST_FIRST:
            for c in range(comps):
                row = c * ghosts + d * halo
                rev_out[j, d, :, lane(c)] = packets[row : row + halo]

            @pl.when(exists(p - OFFSETS[d]))
            def _():
                rev_copy(j, d, p - OFFSETS[d]).start()

    def reverse_sum(n, field):
        by_cosine = jnp.zeros((8, nodes), F32)
        by_sine = jnp.zeros((8, nodes), F32)
        for e in range(comps):
            value = field[e]
            by_cosine += jnp.sum((value * sources[1, e]).reshape(blocks // 8, 8, nodes), axis=0)
            by_sine += jnp.sum((value * sources[0, e]).reshape(blocks // 8, 8, nodes), axis=0)
        both = cosines[pl.ds(n, 1), :] * by_cosine - sines[pl.ds(n, 1), :] * by_sine
        partial[pl.ds(n, 1), :] = jnp.sum(both, axis=0, keepdims=True)

    def reverse_near(n):
        pulled[...] = matmul(near_t[...], split[...])
        for k in range(slots):
            for start in range(0, blocks, CHUNK):
                some = slice(start, start + CHUNK)
                totals = [None] * comps
                for e in range(comps):
                    if k == 0:
                        term = metric[some, :] * adjoint[e, some, :]
                    else:
                        row = (k - 1) * blocks + start
                        term = pulled[row : row + CHUNK, lane(e)]
                    for c in range(comps):
                        more = mixing[k, e, c] * term
                        totals[c] = more if totals[c] is None else totals[c] + more
                for c in range(comps):
                    mixed[c * blocks + start : c * blocks + start + CHUNK, lane(k)] = totals[c].astype(
                        BF16
                    )
        right = jnp.concatenate([lift[k] for k in range(slots)], axis=0)
        pushed = matmul(mixed[...], right)
        inner = jnp.where(n > 0, 1.0, 0.0).astype(F32)
        for c in range(comps):
            state = states[n, c]
            bent = jnp.tanh(state)
            fall = STEP_SIZE * (1.0 - bent * bent)
            slope[c] = fall
            grown = adjoint[c] + inner * (weight[c] * state)
            base[c] = grown - fall * pushed[c * blocks : (c + 1) * blocks]

    def reverse_far(j):
        for d, offset in enumerate(OFFSETS):

            @pl.when(exists(p + offset))
            def _():
                rev_copy(j, d, p).wait_recv()

        ghost = jnp.concatenate([rev_in[j, d] for d in range(4)], axis=0)
        arrived = matmul(pick_t[...], ghost)
        for c in range(comps):
            adjoint[c] = base[c] - slope[c] * arrived[:, lane(c)]

    def send_bend():
        for e in range(comps):
            bent = jnp.tanh(states[1, e])
            turning = cosines[0:1, :] * sources[1, e] - sines[0:1, :] * sources[0, e]
            squashed[:, lane(e)] = (STEP_SIZE * (1.0 - bent * bent) * turning).astype(BF16)
        packets = matmul(pick[...].astype(BF16), squashed[...]).astype(BF16)
        for d, offset in enumerate(OFFSETS):
            bend_out[d] = packets[d * halo : (d + 1) * halo]

            @pl.when(exists(p + offset))
            def _():
                bend_copy(d, p + offset).start()

        for d, offset in enumerate(OFFSETS):

            @pl.when(exists(p - offset))
            def _():
                bend_copy(d, p).wait_recv()

        bend_pass.start()

    def last_sum(j):
        reverse_sum(0, base)
        bend_pass.wait_recv()
        sent = jnp.zeros((halo, nodes), F32)
        for d in range(4):
            both = rev_out[j, d].astype(F32) * bend_there[d].astype(F32)
            for c in range(comps):
                sent += both[:, lane(c)]
        partial[0:1, :] = partial[0:1, :] - jnp.sum(sent, axis=0, keepdims=True)

    loads[0].wait()
    squash(lambda c: states[first, c])
    near_peers = sum(exists(p + offset).astype(jnp.int32) for offset in OFFSETS)
    pl.semaphore_wait(barrier, near_peers + 1 + 2 * t)
    send_forward(0)

    @pl.when(t == 0)
    def _():
        state_copy(0).start()

    @pl.when(t == 1)
    def _():
        call(0, 1)

    loads[1].wait()
    for k in range(slots):
        lift_t[:, lane(k)] = lift[k].astype(F32).T.astype(BF16)
    pick_t[...] = pick[...].T.astype(BF16)
    row_of = lax.broadcasted_iota(jnp.int32, (levels, nodes), 0)
    angles = jnp.zeros((levels, nodes), F32)
    for n in range(levels):
        angles = jnp.where(row_of == n, pitch[n], angles)
    cosines[...] = jnp.cos(angles)
    sines[...] = jnp.sin(angles)
    row_at = lax.broadcasted_iota(jnp.int32, (blocks, blocks), 0)
    for k in range(1, slots):
        chosen = jnp.where(faces[k - 1 : k, :] == row_at, 1.0, 0.0)
        near[(k - 1) * blocks : k * blocks, :] = chosen.T.astype(BF16)
        turned = chosen.astype(BF16)
        near_t[(k - 1) * blocks : k * blocks, :blocks] = turned
        near_t[(k - 1) * blocks : k * blocks, blocks:] = turned
    slot_at = lax.rem(row_at, ghosts)
    for pair in range(2):
        upper = faces[2 * pair : 2 * pair + 1, :] - blocks
        lower = faces[2 * pair + 1 : 2 * pair + 2, :] - blocks
        wanted = jnp.where(row_at < ghosts, upper, lower)
        chosen = jnp.where(wanted == slot_at, 1.0, 0.0)
        far[:, pair * blocks : (pair + 1) * blocks] = chosen.T.astype(BF16)
        turned = chosen.astype(BF16)
        far_t[pair * blocks : (pair + 1) * blocks, :blocks] = turned
        far_t[pair * blocks : (pair + 1) * blocks, blocks:] = turned
    loads[2].wait()
    loads[3].wait()
    last = half - 2 + t

    def forward_level(i, carry):
        forward_near(i)
        forward_far(i)

        @pl.when(i < last)
        def _():
            squash(lambda c: states[first + i + 1, c])
            send_forward(i + 1)

        @pl.when(t == 0)
        def _():
            state_copy(i + 1).start()

        return carry

    lax.fori_loop(0, half - 1 + t, forward_level, 0)

    for load in loads[4:]:
        load.wait()

    @pl.when(t == 0)
    def _():
        send_bend()

    @pl.when(t == 1)
    def _():
        pl.semaphore_wait(hello.at[0], 2)
        call(1, 2)
        for e in range(comps):
            adjoint[e] = adjoint[e] + weight[e] * states[levels, e]

        def reverse_level(j, carry):
            n = levels - 1 - j

            @pl.when(n < half)
            def _():
                state_copy(n).wait_recv()

            send_reverse(j)
            reverse_sum(n, adjoint)
            reverse_near(n)

            reverse_far(j)

            @pl.when(n == half)
            def _():
                kept[...] = adjoint[...]
                keep_copy.start()

            return carry

        lax.fori_loop(0, levels - 2, reverse_level, 0)
        state_copy(1).wait_recv()
        send_reverse(levels - 2)
        reverse_sum(1, adjoint)
        reverse_near(1)
        pl.semaphore_wait(hello.at[1], 2)
        call(2, 2)
        last_sum(levels - 2)
        plane_parts[spot] = partial[...]
        for r in range(1, plane):
            plane_copy(r).start()
        reverse_far(levels - 2)
        state_copy(0).wait_recv()
        send_reverse(levels - 1)
        reverse_near(0)
        pl.semaphore_wait(hello.at[2], 2)
        for r in range(1, plane):
            other = lax.rem(spot + r, plane)
            pltpu.make_async_remote_copy(
                src_ref=partial,
                dst_ref=plane_parts.at[other],
                send_sem=plane_send.at[r],
                recv_sem=plane_recv.at[other],
                device_id=(1, p),
                device_id_type=MESH,
            ).wait_recv()
        total = plane_parts[0]
        for s in range(1, plane):
            total = total + plane_parts[s]
        plane_sum[...] = total
        layer_parts[layer] = total
        for r in range(layers):
            layer_copy(r, 0).start()
            if r > 0:
                layer_copy(r, 1).start()
        reverse_far(levels - 1)
        end_copy.start()

    def layer_wait(r):
        other = lax.rem(layer + r, layers)
        pltpu.make_async_remote_copy(
            src_ref=plane_sum,
            dst_ref=layer_parts.at[other],
            send_sem=layer_send.at[0, r],
            recv_sem=layer_recv.at[other],
            device_id=(1 - t, p),
            device_id_type=MESH,
        ).wait_recv()

    for r in range(1, layers):
        layer_wait(r)

    @pl.when(t == 0)
    def _():
        layer_wait(0)

    total = layer_parts[0]
    for s in range(1, layers):
        total = total + layer_parts[s]
    norm = math.sqrt(comps * nodes * blocks * n_space)
    for n in range(levels):
        grads[n] = STEP_SIZE * jnp.sum(total[n : n + 1, :]) / norm

    def drain(i, carry):
        for d, offset in enumerate(OFFSETS):

            @pl.when(exists(p + offset))
            def _():
                fwd_copy(i, d, p).wait_send()

        return carry

    lax.fori_loop(0, half - 1 + t, drain, 0)

    @pl.when(t == 0)
    def _():
        end_copy.wait_recv()
        for i in range(half):
            state_copy(i).wait_send()
        for d, offset in enumerate(OFFSETS):

            @pl.when(exists(p + offset))
            def _():
                bend_copy(d, p).wait_send()

        bend_pass.wait_send()

    @pl.when(t == 1)
    def _():
        def drain_reverse(j, carry):
            for d, offset in enumerate(OFFSETS):

                @pl.when(exists(p - offset))
                def _():
                    rev_copy(j, d, p).wait_send()

            return carry

        lax.fori_loop(0, levels, drain_reverse, 0)
        keep_copy.wait()
        end_copy.wait_send()
        for r in range(1, plane):
            plane_copy(r).wait_send()
        for r in range(layers):
            layer_copy(r, 0).wait_send()
            if r > 0:
                layer_copy(r, 1).wait_send()


def solution(mesh):
    n_space = mesh.shape["space"]
    plane = 16 if n_space % 16 == 0 else 4

    def shards(
        checkpoints, sources, pitch, metric, obj_weight, adjoint_end, lift, mixing, faces, send_idx
    ):
        comps, blocks, nodes = obj_weight.shape
        slots = lift.shape[0]
        levels = pitch.shape[0]
        half = levels // 2
        halo = send_idx.shape[2]
        ghosts = 4 * halo
        wide = comps * nodes
        links = slots - 1
        layers = n_space // plane
        vmem = pltpu.VMEM
        dma = pltpu.SemaphoreType.DMA
        field = (comps, blocks, nodes)
        scratch = [
            vmem((levels + 1, *field), F32),
            vmem((2, *field), F32),
            vmem((blocks, nodes), F32),
            vmem(field, F32),
            vmem(field, F32),
            vmem(field, F32),
            vmem((slots, nodes, nodes), BF16),
            vmem((nodes, slots * nodes), BF16),
            vmem((levels, nodes), F32),
            vmem((levels, nodes), F32),
            vmem((ghosts, blocks), F32),
            vmem((blocks, ghosts), BF16),
            vmem((links * blocks, blocks), BF16),
            vmem((links * blocks, 2 * blocks), BF16),
            vmem((blocks, links * ghosts), BF16),
            vmem((links * ghosts, 2 * blocks), BF16),
            vmem((blocks, wide), BF16),
            vmem((links * blocks, wide), BF16),
            vmem((slots, comps * blocks, nodes), F32),
            vmem(field, F32),
            vmem(field, F32),
            vmem((comps * ghosts, links * nodes), F32),
            vmem((links * ghosts, wide), BF16),
            vmem((2 * blocks, wide), BF16),
            vmem((links * blocks, wide), F32),
            vmem((links * ghosts, wide), F32),
            vmem((comps * blocks, slots * nodes), BF16),
            vmem((comps * ghosts, links * nodes), BF16),
            vmem((half, 4, halo, wide), BF16),
            vmem((half, 4, halo, wide), BF16),
            vmem((levels, 4, halo, wide), BF16),
            vmem((levels, 4, halo, wide), BF16),
            vmem((4, halo, wide), BF16),
            vmem((4, halo, wide), BF16),
            vmem((4, halo, wide), BF16),
            vmem((levels, nodes), F32),
            vmem((plane, levels, nodes), F32),
            vmem((levels, nodes), F32),
            vmem((layers, levels, nodes), F32),
            dma((6,)),
            dma((half, 4)),
            dma((half, 4)),
            dma((levels, 4)),
            dma((levels, 4)),
            dma((4,)),
            dma((4,)),
            dma((2,)),
            dma((half,)),
            dma((half,)),
            dma((plane,)),
            dma((plane,)),
            dma((2, layers)),
            dma((layers,)),
            dma((2,)),
            dma,
            pltpu.SemaphoreType.REGULAR((3,)),
        ]
        anywhere = pl.BlockSpec(memory_space=pl.ANY)
        scalars = pl.BlockSpec(memory_space=pltpu.SMEM)
        return pl.pallas_call(
            functools.partial(sweep, n_space, plane),
            out_shape=(
                jax.ShapeDtypeStruct((1, *field), F32),
                jax.ShapeDtypeStruct((levels,), F32),
            ),
            in_specs=[
                anywhere,
                anywhere,
                scalars,
                anywhere,
                anywhere,
                anywhere,
                anywhere,
                scalars,
                pl.BlockSpec(memory_space=pltpu.VMEM),
                scalars,
            ],
            out_specs=(anywhere, scalars),
            scratch_shapes=scratch,
            compiler_params=pltpu.CompilerParams(
                collective_id=0, has_side_effects=True, vmem_limit_bytes=67043328
            ),
            name="adjoint_window",
        )(checkpoints, sources, pitch, metric, obj_weight, adjoint_end, lift, mixing, faces.T, send_idx)

    return jax.shard_map(
        shards,
        mesh=mesh,
        in_specs=(
            P("tm", None, "space", None),
            P(None, None, "space", None),
            P(),
            P("space", None),
            P(None, "space", None),
            P(None, "space", None),
            P(),
            P(),
            P("space", None),
            P("space", None, None),
        ),
        out_specs=(P("tm", None, "space", None), P()),
        check_vma=False,
    )
```

```python
import functools
import math

import jax
import jax.numpy as jnp
from jax import lax
from jax.experimental import pallas as pl
from jax.experimental.pallas import tpu as pltpu
from jax.sharding import PartitionSpec as P

OFFSETS = (1, -1, 2, -2)
FARTHEST_FIRST = (2, 3, 0, 1)
STEP_SIZE = 0.5
MESH = pl.DeviceIdType.MESH
F32, BF16 = jnp.float32, jnp.bfloat16
CHUNK = 32


def matmul(left, right):
    return jnp.dot(left, right, preferred_element_type=F32)


def sweep(
    n_space,
    plane,
    checkpoint_in,
    sources_in,
    pitch,
    metric_in,
    weight_in,
    end_in,
    lift_in,
    mixing,
    faces,
    send_idx,
    bounds,
    grads,
    states,
    sources,
    metric,
    weight,
    adjoint,
    kept,
    lift,
    lift_t,
    cosines,
    sines,
    pick,
    pick_t,
    near,
    near_t,
    far,
    far_t,
    far_pick,
    cross,
    pick_wide,
    thirds,
    picked,
    picked_scale,
    gain,
    back_split,
    ahead,
    squashed,
    gathered,
    lifted,
    base,
    slope,
    halo_lifted,
    halo_mixed,
    split,
    pulled,
    halo_pulled,
    mixed,
    far_mixed,
    fwd_out,
    fwd_in,
    rev_out,
    rev_in,
    bend_out,
    bend_in,
    bend_there,
    partial,
    plane_parts,
    plane_sum,
    layer_parts,
    in_sem,
    fwd_send,
    fwd_recv,
    rev_send,
    rev_recv,
    bend_send,
    bend_recv,
    bend_sem,
    state_send,
    state_recv,
    plane_send,
    plane_recv,
    layer_send,
    layer_recv,
    end_sem,
    out_sem,
    hello,
):
    comps, blocks, nodes = states.shape[1:]
    slots = lift.shape[0]
    halo = fwd_in.shape[2]
    ghosts = 4 * halo
    levels = pitch.shape[0]
    half = levels // 2
    layers = n_space // plane
    t = lax.axis_index("tm")
    p = lax.axis_index("space")
    spot = lax.rem(p, plane)
    layer = p // plane
    first = t * half

    def exists(q):
        return jnp.logical_and(q >= 0, q < n_space)

    def lane(c):
        return slice(c * nodes, (c + 1) * nodes)

    loads = [
        pltpu.make_async_copy(checkpoint_in.at[0], states.at[first], in_sem.at[0]),
        pltpu.make_async_copy(lift_in, lift, in_sem.at[1]),
        pltpu.make_async_copy(metric_in, metric, in_sem.at[2]),
        pltpu.make_async_copy(sources_in, sources, in_sem.at[3]),
        pltpu.make_async_copy(weight_in, weight, in_sem.at[4]),
        pltpu.make_async_copy(end_in, adjoint, in_sem.at[5]),
    ]
    for load in loads:
        load.start()

    barrier = pltpu.get_barrier_semaphore()

    def greet(device):
        pl.semaphore_signal(barrier, inc=1, device_id=device, device_id_type=MESH)

    for offset in OFFSETS:

        @pl.when(exists(p + offset))
        def _():
            greet((t, p + offset))

    greet((1 - t, p))

    def in_layer(r):
        return (1, lax.rem(layer + r + layers, layers) * plane + spot)

    @pl.when(t == 1)
    def _():
        greet(in_layer(1))
        greet(in_layer(-1))

    def call(which, distance):
        for r in (distance, -distance):
            pl.semaphore_signal(
                hello.at[which], inc=1, device_id=in_layer(r), device_id_type=MESH
            )

    lane_of = lax.broadcasted_iota(jnp.int32, (1, blocks), 1)
    for d in range(4):
        for s in range(halo):
            row = d * halo + s
            pick[pl.ds(row, 1), :] = jnp.where(lane_of == send_idx[0, d, s], 1.0, 0.0)

    for d, offset in enumerate(OFFSETS):

        @pl.when(jnp.logical_not(exists(p - offset)))
        def _():
            bend_in[d] = jnp.zeros(bend_in.shape[1:], BF16)
            for i in range(half):
                fwd_in[i, d] = jnp.zeros(fwd_in.shape[2:], BF16)

        @pl.when(jnp.logical_not(exists(p + offset)))
        def _():
            for i in range(levels):
                rev_in[i, d] = jnp.zeros(rev_in.shape[2:], BF16)

    def fwd_copy(i, d, device):
        return pltpu.make_async_remote_copy(
            src_ref=fwd_out.at[i, d],
            dst_ref=fwd_in.at[i, d],
            send_sem=fwd_send.at[i, d],
            recv_sem=fwd_recv.at[i, d],
            device_id=(t, device),
            device_id_type=MESH,
        )

    def rev_copy(i, d, device):
        return pltpu.make_async_remote_copy(
            src_ref=rev_out.at[i, d],
            dst_ref=rev_in.at[i, d],
            send_sem=rev_send.at[i, d],
            recv_sem=rev_recv.at[i, d],
            device_id=(t, device),
            device_id_type=MESH,
        )

    def bend_copy(d, device):
        return pltpu.make_async_remote_copy(
            src_ref=bend_out.at[d],
            dst_ref=bend_in.at[d],
            send_sem=bend_send.at[d],
            recv_sem=bend_recv.at[d],
            device_id=(t, device),
            device_id_type=MESH,
        )

    def state_copy(i):
        return pltpu.make_async_remote_copy(
            src_ref=states.at[i],
            dst_ref=states.at[i],
            send_sem=state_send.at[i],
            recv_sem=state_recv.at[i],
            device_id=(1 - t, p),
            device_id_type=MESH,
        )

    def plane_copy(r):
        return pltpu.make_async_remote_copy(
            src_ref=partial,
            dst_ref=plane_parts.at[spot],
            send_sem=plane_send.at[r],
            recv_sem=plane_recv.at[spot],
            device_id=(1, layer * plane + lax.rem(spot + r, plane)),
            device_id_type=MESH,
        )

    def layer_copy(r, core):
        return pltpu.make_async_remote_copy(
            src_ref=plane_sum,
            dst_ref=layer_parts.at[layer],
            send_sem=layer_send.at[core, r],
            recv_sem=layer_recv.at[layer],
            device_id=(core, lax.rem(layer + r, layers) * plane + spot),
            device_id_type=MESH,
        )

    bend_pass = pltpu.make_async_remote_copy(
        src_ref=bend_in,
        dst_ref=bend_there,
        send_sem=bend_sem.at[0],
        recv_sem=bend_sem.at[1],
        device_id=(1 - t, p),
        device_id_type=MESH,
    )
    end_copy = pltpu.make_async_remote_copy(
        src_ref=adjoint,
        dst_ref=bounds.at[0],
        send_sem=end_sem.at[0],
        recv_sem=end_sem.at[1],
        device_id=(1 - t, p),
        device_id_type=MESH,
    )
    keep_copy = pltpu.make_async_copy(kept, bounds.at[0], out_sem)

    def in_halves(value, where, columns):
        rows = value.shape[0]
        high = value.astype(BF16)
        where[:rows, columns] = high
        where[rows:, columns] = (value - high.astype(F32)).astype(BF16)

    def in_thirds(value, columns):
        for part in range(3):
            high = value.astype(BF16)
            thirds[part * blocks : (part + 1) * blocks, columns] = high
            value = value - high.astype(F32)

    def squash(state):
        for c in range(comps):
            squashed[:, lane(c)] = jnp.tanh(state(c)).astype(BF16)

    def send_forward(i):
        packets = matmul(pick[...].astype(BF16), squashed[...]).astype(BF16)
        for d in FARTHEST_FIRST:
            fwd_out[i, d] = packets[d * halo : (d + 1) * halo]

            @pl.when(exists(p + OFFSETS[d]))
            def _():
                fwd_copy(i, d, p + OFFSETS[d]).start()

    def forward_near(i):
        gathered[...] = matmul(near[...], squashed[...]).astype(BF16)
        for k in range(slots):
            rows = squashed if k == 0 else gathered.at[pl.ds((k - 1) * blocks, blocks)]
            left = jnp.concatenate([rows[:, lane(c)] for c in range(comps)], axis=0)
            lifted[k] = matmul(left, lift_t[:, lane(k)])
        cosine = cosines[pl.ds(first + i, 1), :]
        sine = sines[pl.ds(first + i, 1), :]
        for start in range(0, blocks, CHUNK):
            some = slice(start, start + CHUNK)
            totals = [None] * comps
            for k in range(slots):
                for c in range(comps):
                    term = lifted[k, c * blocks + start : c * blocks + start + CHUNK, :]
                    for e in range(comps):
                        more = mixing[k, e, c] * term
                        totals[e] = more if totals[e] is None else totals[e] + more
            for e in range(comps):
                forcing = cosine * sources[0, e, some, :] + sine * sources[1, e, some, :]
                change = forcing - metric[some, :] * totals[e]
                base[e, some, :] = states[first + i, e, some, :] + STEP_SIZE * change

    def forward_far(i):
        for d, offset in enumerate(OFFSETS):

            @pl.when(exists(p - offset))
            def _():
                fwd_copy(i, d, p).wait_recv()

        ghost = jnp.concatenate([fwd_in[i, d] for d in range(4)], axis=0)
        left = jnp.concatenate([ghost[:, lane(c)] for c in range(comps)], axis=0)
        halo_lifted[...] = matmul(left, lift_t[:, nodes:])
        for k in range(1, slots):
            for start in range(0, ghosts, CHUNK):
                totals = [None] * comps
                for c in range(comps):
                    term = halo_lifted[c * ghosts + start : c * ghosts + start + CHUNK, lane(k - 1)]
                    for e in range(comps):
                        more = mixing[k, e, c] * term
                        totals[e] = more if totals[e] is None else totals[e] + more
                row = (k - 1) * ghosts + start
                for e in range(comps):
                    halo_mixed[row : row + CHUNK, lane(e)] = totals[e].astype(BF16)

    def forward_ahead():
        for e in range(comps):
            in_thirds(base[e], lane(e))
        picked[...] = matmul(pick_wide[...], thirds[...])

    def send_picked(i):
        change = matmul(far_pick[...], halo_mixed[...])
        wide_scale = jnp.concatenate([picked_scale[...]] * comps, axis=1)
        packets = jnp.tanh(picked[...] - wide_scale * change).astype(BF16)
        for d in FARTHEST_FIRST:
            fwd_out[i, d] = packets[d * halo : (d + 1) * halo]

            @pl.when(exists(p + OFFSETS[d]))
            def _():
                fwd_copy(i, d, p + OFFSETS[d]).start()

    def forward_end(i):
        scale = STEP_SIZE * metric[...]
        arrived = matmul(far[...], halo_mixed[...])
        for e in range(comps):
            states[first + i + 1, e] = base[e] - scale * arrived[:, lane(e)]

    def split_field(field):
        for e in range(comps):
            in_halves(metric[...] * field[e], split, lane(e))

    def far_product():
        for k in range(1, slots):
            for start in range(0, ghosts, CHUNK):
                row = (k - 1) * ghosts + start
                totals = [None] * comps
                for e in range(comps):
                    term = halo_pulled[row : row + CHUNK, lane(e)]
                    for c in range(comps):
                        more = mixing[k, e, c] * term
                        totals[c] = more if totals[c] is None else totals[c] + more
                for c in range(comps):
                    far_mixed[c * ghosts + start : c * ghosts + start + CHUNK, lane(k - 1)] = totals[
                        c
                    ].astype(BF16)
        right = jnp.concatenate([lift[k] for k in range(1, slots)], axis=0)
        return matmul(far_mixed[...], right)

    def ship_reverse(j, product):
        packets = product.astype(BF16)
        for d in FARTHEST_FIRST:
            for c in range(comps):
                row = c * ghosts + d * halo
                rev_out[j, d, :, lane(c)] = packets[row : row + halo]

            @pl.when(exists(p - OFFSETS[d]))
            def _():
                rev_copy(j, d, p - OFFSETS[d]).start()

    def send_reverse(j):
        halo_pulled[...] = matmul(far_t[...], split[...])
        ship_reverse(j, far_product())

    def reverse_ahead():
        split_field(slope)
        gain[...] = matmul(pick_wide[:, : 2 * blocks], split[...])
        split_field(base)
        halo_pulled[...] = matmul(far_t[...], split[...])
        ahead[...] = far_product()

    def send_ahead(j):
        for c in range(comps):
            back = jnp.concatenate([rev_in[j - 1, d, :, lane(c)] for d in range(4)], axis=0)
            in_halves(gain[:, lane(c)] * back.astype(F32), back_split, lane(c))
        halo_pulled[...] = matmul(cross[...], back_split[...])
        ship_reverse(j, ahead[...] - far_product())

    def reverse_sum(n, field):
        by_cosine = jnp.zeros((8, nodes), F32)
        by_sine = jnp.zeros((8, nodes), F32)
        for e in range(comps):
            value = field[e]
            by_cosine += jnp.sum((value * sources[1, e]).reshape(blocks // 8, 8, nodes), axis=0)
            by_sine += jnp.sum((value * sources[0, e]).reshape(blocks // 8, 8, nodes), axis=0)
        both = cosines[pl.ds(n, 1), :] * by_cosine - sines[pl.ds(n, 1), :] * by_sine
        partial[pl.ds(n, 1), :] = jnp.sum(both, axis=0, keepdims=True)

    def reverse_near(n):
        pulled[...] = matmul(near_t[...], split[...])
        for k in range(slots):
            for start in range(0, blocks, CHUNK):
                some = slice(start, start + CHUNK)
                totals = [None] * comps
                for e in range(comps):
                    if k == 0:
                        term = metric[some, :] * adjoint[e, some, :]
                    else:
                        row = (k - 1) * blocks + start
                        term = pulled[row : row + CHUNK, lane(e)]
                    for c in range(comps):
                        more = mixing[k, e, c] * term
                        totals[c] = more if totals[c] is None else totals[c] + more
                for c in range(comps):
                    mixed[c * blocks + start : c * blocks + start + CHUNK, lane(k)] = totals[c].astype(
                        BF16
                    )
        right = jnp.concatenate([lift[k] for k in range(slots)], axis=0)
        pushed = matmul(mixed[...], right)
        inner = jnp.where(n > 0, 1.0, 0.0).astype(F32)
        for c in range(comps):
            state = states[n, c]
            bent = jnp.tanh(state)
            fall = STEP_SIZE * (1.0 - bent * bent)
            slope[c] = fall
            grown = adjoint[c] + inner * (weight[c] * state)
            base[c] = grown - fall * pushed[c * blocks : (c + 1) * blocks]

    def reverse_wait(j):
        for d, offset in enumerate(OFFSETS):

            @pl.when(exists(p + offset))
            def _():
                rev_copy(j, d, p).wait_recv()

    def reverse_far(j):
        ghost = jnp.concatenate([rev_in[j, d] for d in range(4)], axis=0)
        arrived = matmul(pick_t[...], ghost)
        for c in range(comps):
            adjoint[c] = base[c] - slope[c] * arrived[:, lane(c)]

    def send_bend():
        for e in range(comps):
            bent = jnp.tanh(states[1, e])
            turning = cosines[0:1, :] * sources[1, e] - sines[0:1, :] * sources[0, e]
            squashed[:, lane(e)] = (STEP_SIZE * (1.0 - bent * bent) * turning).astype(BF16)
        packets = matmul(pick[...].astype(BF16), squashed[...]).astype(BF16)
        for d, offset in enumerate(OFFSETS):
            bend_out[d] = packets[d * halo : (d + 1) * halo]

            @pl.when(exists(p + offset))
            def _():
                bend_copy(d, p + offset).start()

        for d, offset in enumerate(OFFSETS):

            @pl.when(exists(p - offset))
            def _():
                bend_copy(d, p).wait_recv()

        bend_pass.start()

    def last_sum(j):
        reverse_sum(0, base)
        bend_pass.wait_recv()
        sent = jnp.zeros((halo, nodes), F32)
        for d in range(4):
            both = rev_out[j, d].astype(F32) * bend_there[d].astype(F32)
            for c in range(comps):
                sent += both[:, lane(c)]
        partial[0:1, :] = partial[0:1, :] - jnp.sum(sent, axis=0, keepdims=True)

    loads[0].wait()
    squash(lambda c: states[first, c])
    near_peers = sum(exists(p + offset).astype(jnp.int32) for offset in OFFSETS)
    pl.semaphore_wait(barrier, near_peers + 1 + 2 * t)
    send_forward(0)

    @pl.when(t == 0)
    def _():
        state_copy(0).start()

    @pl.when(t == 1)
    def _():
        call(0, 1)

    loads[1].wait()
    for k in range(slots):
        lift_t[:, lane(k)] = lift[k].astype(F32).T.astype(BF16)
    pick_t[...] = pick[...].T.astype(BF16)
    row_of = lax.broadcasted_iota(jnp.int32, (levels, nodes), 0)
    angles = jnp.zeros((levels, nodes), F32)
    for n in range(levels):
        angles = jnp.where(row_of == n, pitch[n], angles)
    cosines[...] = jnp.cos(angles)
    sines[...] = jnp.sin(angles)
    row_at = lax.broadcasted_iota(jnp.int32, (blocks, blocks), 0)
    for k in range(1, slots):
        chosen = jnp.where(faces[k - 1 : k, :] == row_at, 1.0, 0.0)
        near[(k - 1) * blocks : k * blocks, :] = chosen.T.astype(BF16)
        turned = chosen.astype(BF16)
        near_t[(k - 1) * blocks : k * blocks, :blocks] = turned
        near_t[(k - 1) * blocks : k * blocks, blocks:] = turned
    slot_at = lax.rem(row_at, ghosts)
    for pair in range(2):
        upper = faces[2 * pair : 2 * pair + 1, :] - blocks
        lower = faces[2 * pair + 1 : 2 * pair + 2, :] - blocks
        wanted = jnp.where(row_at < ghosts, upper, lower)
        chosen = jnp.where(wanted == slot_at, 1.0, 0.0)
        far[:, pair * blocks : (pair + 1) * blocks] = chosen.T.astype(BF16)
        turned = chosen.astype(BF16)
        far_t[pair * blocks : (pair + 1) * blocks, :blocks] = turned
        far_t[pair * blocks : (pair + 1) * blocks, blocks:] = turned
    wide_pick = pick[...].astype(BF16)
    for part in range(3):
        pick_wide[:, part * blocks : (part + 1) * blocks] = wide_pick
    far_pick[...] = matmul(wide_pick, far[...]).astype(BF16)
    crossed = matmul(far_t[:, :blocks], pick_t[...]).astype(BF16)
    cross[...] = jnp.concatenate([crossed, crossed], axis=1)
    loads[2].wait()
    in_thirds(STEP_SIZE * metric[...], lane(0))
    picked_scale[...] = matmul(pick_wide[...], thirds[:, lane(0)])
    loads[3].wait()
    last = half - 2 + t

    def forward_level(i, carry):
        forward_near(i)
        forward_ahead()
        forward_far(i)

        @pl.when(i < last)
        def _():
            send_picked(i + 1)

        forward_end(i)

        @pl.when(i < last)
        def _():
            squash(lambda c: states[first + i + 1, c])

        @pl.when(t == 0)
        def _():
            state_copy(i + 1).start()

        return carry

    lax.fori_loop(0, half - 1 + t, forward_level, 0)

    for load in loads[4:]:
        load.wait()

    @pl.when(t == 0)
    def _():
        send_bend()

    @pl.when(t == 1)
    def _():
        pl.semaphore_wait(hello.at[0], 2)
        call(1, 2)
        for e in range(comps):
            adjoint[e] = adjoint[e] + weight[e] * states[levels, e]
        split_field(adjoint)
        send_reverse(0)

        def reverse_level(j, carry):
            n = levels - 1 - j

            @pl.when(n < half)
            def _():
                state_copy(n).wait_recv()

            reverse_sum(n, adjoint)
            reverse_near(n)
            reverse_ahead()
            reverse_wait(j)
            send_ahead(j + 1)
            reverse_far(j)
            split_field(adjoint)

            @pl.when(n == half)
            def _():
                kept[...] = adjoint[...]
                keep_copy.start()

            return carry

        lax.fori_loop(0, levels - 2, reverse_level, 0)
        state_copy(1).wait_recv()
        reverse_sum(1, adjoint)
        reverse_near(1)
        pl.semaphore_wait(hello.at[1], 2)
        call(2, 2)
        last_sum(levels - 2)
        plane_parts[spot] = partial[...]
        for r in range(1, plane):
            plane_copy(r).start()
        reverse_ahead()
        reverse_wait(levels - 2)
        send_ahead(levels - 1)
        reverse_far(levels - 2)
        split_field(adjoint)
        state_copy(0).wait_recv()
        reverse_near(0)
        pl.semaphore_wait(hello.at[2], 2)
        for r in range(1, plane):
            other = lax.rem(spot + r, plane)
            pltpu.make_async_remote_copy(
                src_ref=partial,
                dst_ref=plane_parts.at[other],
                send_sem=plane_send.at[r],
                recv_sem=plane_recv.at[other],
                device_id=(1, p),
                device_id_type=MESH,
            ).wait_recv()
        total = plane_parts[0]
        for s in range(1, plane):
            total = total + plane_parts[s]
        plane_sum[...] = total
        layer_parts[layer] = total
        for r in range(layers):
            layer_copy(r, 0).start()
            if r > 0:
                layer_copy(r, 1).start()
        reverse_wait(levels - 1)
        reverse_far(levels - 1)
        end_copy.start()

    def layer_wait(r):
        other = lax.rem(layer + r, layers)
        pltpu.make_async_remote_copy(
            src_ref=plane_sum,
            dst_ref=layer_parts.at[other],
            send_sem=layer_send.at[0, r],
            recv_sem=layer_recv.at[other],
            device_id=(1 - t, p),
            device_id_type=MESH,
        ).wait_recv()

    for r in range(1, layers):
        layer_wait(r)

    @pl.when(t == 0)
    def _():
        layer_wait(0)

    total = layer_parts[0]
    for s in range(1, layers):
        total = total + layer_parts[s]
    norm = math.sqrt(comps * nodes * blocks * n_space)
    for n in range(levels):
        grads[n] = STEP_SIZE * jnp.sum(total[n : n + 1, :]) / norm

    def drain(i, carry):
        for d, offset in enumerate(OFFSETS):

            @pl.when(exists(p + offset))
            def _():
                fwd_copy(i, d, p).wait_send()

        return carry

    lax.fori_loop(0, half - 1 + t, drain, 0)

    @pl.when(t == 0)
    def _():
        end_copy.wait_recv()
        for i in range(half):
            state_copy(i).wait_send()
        for d, offset in enumerate(OFFSETS):

            @pl.when(exists(p + offset))
            def _():
                bend_copy(d, p).wait_send()

        bend_pass.wait_send()

    @pl.when(t == 1)
    def _():
        def drain_reverse(j, carry):
            for d, offset in enumerate(OFFSETS):

                @pl.when(exists(p - offset))
                def _():
                    rev_copy(j, d, p).wait_send()

            return carry

        lax.fori_loop(0, levels, drain_reverse, 0)
        keep_copy.wait()
        end_copy.wait_send()
        for r in range(1, plane):
            plane_copy(r).wait_send()
        for r in range(layers):
            layer_copy(r, 0).wait_send()
            if r > 0:
                layer_copy(r, 1).wait_send()


def solution(mesh):
    n_space = mesh.shape["space"]
    plane = 16 if n_space % 16 == 0 else 4

    def shards(
        checkpoints, sources, pitch, metric, obj_weight, adjoint_end, lift, mixing, faces, send_idx
    ):
        comps, blocks, nodes = obj_weight.shape
        slots = lift.shape[0]
        levels = pitch.shape[0]
        half = levels // 2
        halo = send_idx.shape[2]
        ghosts = 4 * halo
        wide = comps * nodes
        links = slots - 1
        layers = n_space // plane
        vmem = pltpu.VMEM
        dma = pltpu.SemaphoreType.DMA
        field = (comps, blocks, nodes)
        scratch = [
            vmem((levels + 1, *field), F32),
            vmem((2, *field), F32),
            vmem((blocks, nodes), F32),
            vmem(field, F32),
            vmem(field, F32),
            vmem(field, F32),
            vmem((slots, nodes, nodes), BF16),
            vmem((nodes, slots * nodes), BF16),
            vmem((levels, nodes), F32),
            vmem((levels, nodes), F32),
            vmem((ghosts, blocks), F32),
            vmem((blocks, ghosts), BF16),
            vmem((links * blocks, blocks), BF16),
            vmem((links * blocks, 2 * blocks), BF16),
            vmem((blocks, links * ghosts), BF16),
            vmem((links * ghosts, 2 * blocks), BF16),
            vmem((ghosts, links * ghosts), BF16),
            vmem((links * ghosts, 2 * ghosts), BF16),
            vmem((ghosts, 3 * blocks), BF16),
            vmem((3 * blocks, wide), BF16),
            vmem((ghosts, wide), F32),
            vmem((ghosts, nodes), F32),
            vmem((ghosts, wide), F32),
            vmem((2 * ghosts, wide), BF16),
            vmem((comps * ghosts, nodes), F32),
            vmem((blocks, wide), BF16),
            vmem((links * blocks, wide), BF16),
            vmem((slots, comps * blocks, nodes), F32),
            vmem(field, F32),
            vmem(field, F32),
            vmem((comps * ghosts, links * nodes), F32),
            vmem((links * ghosts, wide), BF16),
            vmem((2 * blocks, wide), BF16),
            vmem((links * blocks, wide), F32),
            vmem((links * ghosts, wide), F32),
            vmem((comps * blocks, slots * nodes), BF16),
            vmem((comps * ghosts, links * nodes), BF16),
            vmem((half, 4, halo, wide), BF16),
            vmem((half, 4, halo, wide), BF16),
            vmem((levels, 4, halo, wide), BF16),
            vmem((levels, 4, halo, wide), BF16),
            vmem((4, halo, wide), BF16),
            vmem((4, halo, wide), BF16),
            vmem((4, halo, wide), BF16),
            vmem((levels, nodes), F32),
            vmem((plane, levels, nodes), F32),
            vmem((levels, nodes), F32),
            vmem((layers, levels, nodes), F32),
            dma((6,)),
            dma((half, 4)),
            dma((half, 4)),
            dma((levels, 4)),
            dma((levels, 4)),
            dma((4,)),
            dma((4,)),
            dma((2,)),
            dma((half,)),
            dma((half,)),
            dma((plane,)),
            dma((plane,)),
            dma((2, layers)),
            dma((layers,)),
            dma((2,)),
            dma,
            pltpu.SemaphoreType.REGULAR((3,)),
        ]
        anywhere = pl.BlockSpec(memory_space=pl.ANY)
        scalars = pl.BlockSpec(memory_space=pltpu.SMEM)
        return pl.pallas_call(
            functools.partial(sweep, n_space, plane),
            out_shape=(
                jax.ShapeDtypeStruct((1, *field), F32),
                jax.ShapeDtypeStruct((levels,), F32),
            ),
            in_specs=[
                anywhere,
                anywhere,
                scalars,
                anywhere,
                anywhere,
                anywhere,
                anywhere,
                scalars,
                pl.BlockSpec(memory_space=pltpu.VMEM),
                scalars,
            ],
            out_specs=(anywhere, scalars),
            scratch_shapes=scratch,
            compiler_params=pltpu.CompilerParams(
                collective_id=0, has_side_effects=True, vmem_limit_bytes=67043328
            ),
            name="adjoint_window",
        )(checkpoints, sources, pitch, metric, obj_weight, adjoint_end, lift, mixing, faces.T, send_idx)

    return jax.shard_map(
        shards,
        mesh=mesh,
        in_specs=(
            P("tm", None, "space", None),
            P(None, None, "space", None),
            P(),
            P("space", None),
            P(None, "space", None),
            P(None, "space", None),
            P(),
            P(),
            P("space", None),
            P("space", None, None),
        ),
        out_specs=(P("tm", None, "space", None), P()),
        check_vma=False,
    )
```

```python
import functools
import math

import jax
import jax.numpy as jnp
from jax import lax
from jax.experimental import pallas as pl
from jax.experimental.pallas import tpu as pltpu
from jax.sharding import PartitionSpec as P

OFFSETS = (1, -1, 2, -2)
FARTHEST_FIRST = (2, 3, 0, 1)
STEP_SIZE = 0.5
MESH = pl.DeviceIdType.MESH
F32, BF16 = jnp.float32, jnp.bfloat16
CHUNK = 32


def matmul(left, right):
    return jnp.dot(left, right, preferred_element_type=F32)


def sweep(
    n_space,
    plane,
    checkpoint_in,
    sources_in,
    pitch_in,
    metric_in,
    weight_in,
    end_in,
    lift_in,
    mixing_in,
    faces_in,
    send_idx_in,
    bounds,
    grads,
    pitch,
    mixing,
    faces,
    send_idx,
    grads_row,
    states,
    sources,
    metric,
    weight,
    adjoint,
    kept,
    lift,
    lift_t,
    cosines,
    sines,
    pick,
    pick_t,
    near,
    near_t,
    far,
    far_t,
    far_pick,
    cross,
    pick_wide,
    thirds,
    picked,
    picked_scale,
    gain,
    back_split,
    ahead,
    squashed,
    gathered,
    lifted,
    base,
    slope,
    halo_lifted,
    halo_mixed,
    split,
    pulled,
    halo_pulled,
    mixed,
    far_mixed,
    fwd_out,
    fwd_in,
    rev_out,
    rev_in,
    bend_out,
    bend_in,
    bend_there,
    partial,
    plane_parts,
    plane_sum,
    layer_parts,
    in_sem,
    fwd_send,
    fwd_recv,
    rev_send,
    rev_recv,
    bend_send,
    bend_recv,
    bend_sem,
    state_send,
    state_recv,
    plane_send,
    plane_recv,
    layer_send,
    layer_recv,
    end_sem,
    out_sem,
    hello,
):
    comps, blocks, nodes = states.shape[1:]
    slots = lift.shape[0]
    halo = fwd_in.shape[2]
    ghosts = 4 * halo
    levels = pitch.shape[0]
    half = levels // 2
    layers = n_space // plane
    t = lax.axis_index("tm")
    p = lax.axis_index("space")
    spot = lax.rem(p, plane)
    layer = p // plane
    first = t * half

    def exists(q):
        return jnp.logical_and(q >= 0, q < n_space)

    def lane(c):
        return slice(c * nodes, (c + 1) * nodes)

    (
        load_first,
        load_idx,
        load_mixing,
        load_faces,
        load_pitch,
        load_lift,
        load_metric,
        load_sources,
        load_weight,
        load_end,
    ) = loads = [
        pltpu.make_async_copy(checkpoint_in.at[0], states.at[first], in_sem.at[0]),
        pltpu.make_async_copy(send_idx_in, send_idx, in_sem.at[6]),
        pltpu.make_async_copy(mixing_in, mixing, in_sem.at[7]),
        pltpu.make_async_copy(faces_in, faces, in_sem.at[8]),
        pltpu.make_async_copy(pitch_in, pitch, in_sem.at[9]),
        pltpu.make_async_copy(lift_in, lift, in_sem.at[1]),
        pltpu.make_async_copy(metric_in, metric, in_sem.at[2]),
        pltpu.make_async_copy(sources_in, sources, in_sem.at[3]),
        pltpu.make_async_copy(weight_in, weight, in_sem.at[4]),
        pltpu.make_async_copy(end_in, adjoint, in_sem.at[5]),
    ]
    barrier = pltpu.get_barrier_semaphore()

    def greet(device):
        pl.semaphore_signal(barrier, inc=1, device_id=device, device_id_type=MESH)

    for offset in OFFSETS:

        @pl.when(exists(p + offset))
        def _():
            greet((t, p + offset))

    greet((1 - t, p))

    def in_layer(r):
        return (1, lax.rem(layer + r + layers, layers) * plane + spot)

    @pl.when(t == 1)
    def _():
        greet(in_layer(1))
        greet(in_layer(-1))

    def call(which, distance):
        for r in (distance, -distance):
            pl.semaphore_signal(
                hello.at[which], inc=1, device_id=in_layer(r), device_id_type=MESH
            )

    for load in loads:
        load.start()

    load_idx.wait()
    lane_of = lax.broadcasted_iota(jnp.int32, (1, blocks), 1)
    for d in range(4):
        for s in range(halo):
            row = d * halo + s
            pick[pl.ds(row, 1), :] = jnp.where(lane_of == send_idx[0, d, s], 1.0, 0.0)

    for d, offset in enumerate(OFFSETS):

        @pl.when(jnp.logical_not(exists(p - offset)))
        def _():
            bend_in[d] = jnp.zeros(bend_in.shape[1:], BF16)
            for i in range(half):
                fwd_in[i, d] = jnp.zeros(fwd_in.shape[2:], BF16)

        @pl.when(jnp.logical_not(exists(p + offset)))
        def _():
            for i in range(levels):
                rev_in[i, d] = jnp.zeros(rev_in.shape[2:], BF16)

    def fwd_copy(i, d, device):
        return pltpu.make_async_remote_copy(
            src_ref=fwd_out.at[i, d],
            dst_ref=fwd_in.at[i, d],
            send_sem=fwd_send.at[i, d],
            recv_sem=fwd_recv.at[i, d],
            device_id=(t, device),
            device_id_type=MESH,
        )

    def rev_copy(i, d, device):
        return pltpu.make_async_remote_copy(
            src_ref=rev_out.at[i, d],
            dst_ref=rev_in.at[i, d],
            send_sem=rev_send.at[i, d],
            recv_sem=rev_recv.at[i, d],
            device_id=(t, device),
            device_id_type=MESH,
        )

    def bend_copy(d, device):
        return pltpu.make_async_remote_copy(
            src_ref=bend_out.at[d],
            dst_ref=bend_in.at[d],
            send_sem=bend_send.at[d],
            recv_sem=bend_recv.at[d],
            device_id=(t, device),
            device_id_type=MESH,
        )

    def state_copy(i):
        return pltpu.make_async_remote_copy(
            src_ref=states.at[i],
            dst_ref=states.at[i],
            send_sem=state_send.at[i],
            recv_sem=state_recv.at[i],
            device_id=(1 - t, p),
            device_id_type=MESH,
        )

    def plane_copy(r):
        return pltpu.make_async_remote_copy(
            src_ref=partial,
            dst_ref=plane_parts.at[spot],
            send_sem=plane_send.at[r],
            recv_sem=plane_recv.at[spot],
            device_id=(1, layer * plane + lax.rem(spot + r, plane)),
            device_id_type=MESH,
        )

    def layer_copy(r, core):
        return pltpu.make_async_remote_copy(
            src_ref=plane_sum,
            dst_ref=layer_parts.at[layer],
            send_sem=layer_send.at[core, r],
            recv_sem=layer_recv.at[layer],
            device_id=(core, lax.rem(layer + r, layers) * plane + spot),
            device_id_type=MESH,
        )

    bend_pass = pltpu.make_async_remote_copy(
        src_ref=bend_in,
        dst_ref=bend_there,
        send_sem=bend_sem.at[0],
        recv_sem=bend_sem.at[1],
        device_id=(1 - t, p),
        device_id_type=MESH,
    )
    end_copy = pltpu.make_async_remote_copy(
        src_ref=adjoint,
        dst_ref=bounds.at[0],
        send_sem=end_sem.at[0],
        recv_sem=end_sem.at[1],
        device_id=(1 - t, p),
        device_id_type=MESH,
    )
    keep_copy = pltpu.make_async_copy(kept, bounds.at[0], out_sem.at[0])

    def in_halves(value, where, columns):
        rows = value.shape[0]
        high = value.astype(BF16)
        where[:rows, columns] = high
        where[rows:, columns] = (value - high.astype(F32)).astype(BF16)

    def in_thirds(value, columns):
        for part in range(3):
            high = value.astype(BF16)
            thirds[part * blocks : (part + 1) * blocks, columns] = high
            value = value - high.astype(F32)

    def squash(state):
        for c in range(comps):
            squashed[:, lane(c)] = jnp.tanh(state(c)).astype(BF16)

    def send_forward(i):
        packets = matmul(pick[...].astype(BF16), squashed[...]).astype(BF16)
        for d in FARTHEST_FIRST:
            fwd_out[i, d] = packets[d * halo : (d + 1) * halo]

            @pl.when(exists(p + OFFSETS[d]))
            def _():
                fwd_copy(i, d, p + OFFSETS[d]).start()

    def forward_near(i):
        gathered[...] = matmul(near[...], squashed[...]).astype(BF16)
        for k in range(slots):
            rows = squashed if k == 0 else gathered.at[pl.ds((k - 1) * blocks, blocks)]
            left = jnp.concatenate([rows[:, lane(c)] for c in range(comps)], axis=0)
            lifted[k] = matmul(left, lift_t[:, lane(k)])
        cosine = cosines[pl.ds(first + i, 1), :]
        sine = sines[pl.ds(first + i, 1), :]
        for start in range(0, blocks, CHUNK):
            some = slice(start, start + CHUNK)
            totals = [None] * comps
            for k in range(slots):
                for c in range(comps):
                    term = lifted[k, c * blocks + start : c * blocks + start + CHUNK, :]
                    for e in range(comps):
                        more = mixing[k, e, c] * term
                        totals[e] = more if totals[e] is None else totals[e] + more
            for e in range(comps):
                forcing = cosine * sources[0, e, some, :] + sine * sources[1, e, some, :]
                change = forcing - metric[some, :] * totals[e]
                base[e, some, :] = states[first + i, e, some, :] + STEP_SIZE * change

    def forward_far(i):
        for d, offset in enumerate(OFFSETS):

            @pl.when(exists(p - offset))
            def _():
                fwd_copy(i, d, p).wait_recv()

        ghost = jnp.concatenate([fwd_in[i, d] for d in range(4)], axis=0)
        left = jnp.concatenate([ghost[:, lane(c)] for c in range(comps)], axis=0)
        halo_lifted[...] = matmul(left, lift_t[:, nodes:])
        for k in range(1, slots):
            for start in range(0, ghosts, CHUNK):
                totals = [None] * comps
                for c in range(comps):
                    term = halo_lifted[c * ghosts + start : c * ghosts + start + CHUNK, lane(k - 1)]
                    for e in range(comps):
                        more = mixing[k, e, c] * term
                        totals[e] = more if totals[e] is None else totals[e] + more
                row = (k - 1) * ghosts + start
                for e in range(comps):
                    halo_mixed[row : row + CHUNK, lane(e)] = totals[e].astype(BF16)

    def forward_ahead():
        for e in range(comps):
            in_thirds(base[e], lane(e))
        picked[...] = matmul(pick_wide[...], thirds[...])

    def send_picked(i):
        change = matmul(far_pick[...], halo_mixed[...])
        wide_scale = jnp.concatenate([picked_scale[...]] * comps, axis=1)
        packets = jnp.tanh(picked[...] - wide_scale * change).astype(BF16)
        for d in FARTHEST_FIRST:
            fwd_out[i, d] = packets[d * halo : (d + 1) * halo]

            @pl.when(exists(p + OFFSETS[d]))
            def _():
                fwd_copy(i, d, p + OFFSETS[d]).start()

    def forward_end(i):
        scale = STEP_SIZE * metric[...]
        arrived = matmul(far[...], halo_mixed[...])
        for e in range(comps):
            states[first + i + 1, e] = base[e] - scale * arrived[:, lane(e)]

    def split_field(field):
        for e in range(comps):
            in_halves(metric[...] * field[e], split, lane(e))

    def far_product():
        for k in range(1, slots):
            for start in range(0, ghosts, CHUNK):
                row = (k - 1) * ghosts + start
                totals = [None] * comps
                for e in range(comps):
                    term = halo_pulled[row : row + CHUNK, lane(e)]
                    for c in range(comps):
                        more = mixing[k, e, c] * term
                        totals[c] = more if totals[c] is None else totals[c] + more
                for c in range(comps):
                    far_mixed[c * ghosts + start : c * ghosts + start + CHUNK, lane(k - 1)] = totals[
                        c
                    ].astype(BF16)
        right = jnp.concatenate([lift[k] for k in range(1, slots)], axis=0)
        return matmul(far_mixed[...], right)

    def ship_reverse(j, product):
        packets = product.astype(BF16)
        for d in FARTHEST_FIRST:
            for c in range(comps):
                row = c * ghosts + d * halo
                rev_out[j, d, :, lane(c)] = packets[row : row + halo]

            @pl.when(exists(p - OFFSETS[d]))
            def _():
                rev_copy(j, d, p - OFFSETS[d]).start()

    def send_reverse(j):
        halo_pulled[...] = matmul(far_t[...], split[...])
        ship_reverse(j, far_product())

    def reverse_ahead():
        split_field(slope)
        gain[...] = matmul(pick_wide[:, : 2 * blocks], split[...])
        split_field(base)
        halo_pulled[...] = matmul(far_t[...], split[...])
        ahead[...] = far_product()

    def send_ahead(j):
        for c in range(comps):
            back = jnp.concatenate([rev_in[j - 1, d, :, lane(c)] for d in range(4)], axis=0)
            in_halves(gain[:, lane(c)] * back.astype(F32), back_split, lane(c))
        halo_pulled[...] = matmul(cross[...], back_split[...])
        ship_reverse(j, ahead[...] - far_product())

    def reverse_sum(n, field):
        by_cosine = jnp.zeros((8, nodes), F32)
        by_sine = jnp.zeros((8, nodes), F32)
        for e in range(comps):
            value = field[e]
            by_cosine += jnp.sum((value * sources[1, e]).reshape(blocks // 8, 8, nodes), axis=0)
            by_sine += jnp.sum((value * sources[0, e]).reshape(blocks // 8, 8, nodes), axis=0)
        both = cosines[pl.ds(n, 1), :] * by_cosine - sines[pl.ds(n, 1), :] * by_sine
        partial[pl.ds(n, 1), :] = jnp.sum(both, axis=0, keepdims=True)

    def reverse_near(n):
        pulled[...] = matmul(near_t[...], split[...])
        for k in range(slots):
            for start in range(0, blocks, CHUNK):
                some = slice(start, start + CHUNK)
                totals = [None] * comps
                for e in range(comps):
                    if k == 0:
                        term = metric[some, :] * adjoint[e, some, :]
                    else:
                        row = (k - 1) * blocks + start
                        term = pulled[row : row + CHUNK, lane(e)]
                    for c in range(comps):
                        more = mixing[k, e, c] * term
                        totals[c] = more if totals[c] is None else totals[c] + more
                for c in range(comps):
                    mixed[c * blocks + start : c * blocks + start + CHUNK, lane(k)] = totals[c].astype(
                        BF16
                    )
        right = jnp.concatenate([lift[k] for k in range(slots)], axis=0)
        pushed = matmul(mixed[...], right)
        inner = jnp.where(n > 0, 1.0, 0.0).astype(F32)
        for c in range(comps):
            state = states[n, c]
            bent = jnp.tanh(state)
            fall = STEP_SIZE * (1.0 - bent * bent)
            slope[c] = fall
            grown = adjoint[c] + inner * (weight[c] * state)
            base[c] = grown - fall * pushed[c * blocks : (c + 1) * blocks]

    def reverse_wait(j):
        for d, offset in enumerate(OFFSETS):

            @pl.when(exists(p + offset))
            def _():
                rev_copy(j, d, p).wait_recv()

    def reverse_far(j):
        ghost = jnp.concatenate([rev_in[j, d] for d in range(4)], axis=0)
        arrived = matmul(pick_t[...], ghost)
        for c in range(comps):
            adjoint[c] = base[c] - slope[c] * arrived[:, lane(c)]

    def send_bend():
        for e in range(comps):
            bent = jnp.tanh(states[1, e])
            turning = cosines[0:1, :] * sources[1, e] - sines[0:1, :] * sources[0, e]
            squashed[:, lane(e)] = (STEP_SIZE * (1.0 - bent * bent) * turning).astype(BF16)
        packets = matmul(pick[...].astype(BF16), squashed[...]).astype(BF16)
        for d, offset in enumerate(OFFSETS):
            bend_out[d] = packets[d * halo : (d + 1) * halo]

            @pl.when(exists(p + offset))
            def _():
                bend_copy(d, p + offset).start()

        for d, offset in enumerate(OFFSETS):

            @pl.when(exists(p - offset))
            def _():
                bend_copy(d, p).wait_recv()

        bend_pass.start()

    def last_sum(j):
        reverse_sum(0, base)
        bend_pass.wait_recv()
        sent = jnp.zeros((halo, nodes), F32)
        for d in range(4):
            both = rev_out[j, d].astype(F32) * bend_there[d].astype(F32)
            for c in range(comps):
                sent += both[:, lane(c)]
        partial[0:1, :] = partial[0:1, :] - jnp.sum(sent, axis=0, keepdims=True)

    load_first.wait()
    squash(lambda c: states[first, c])
    near_peers = sum(exists(p + offset).astype(jnp.int32) for offset in OFFSETS)
    pl.semaphore_wait(barrier, near_peers + 1 + 2 * t)
    send_forward(0)

    @pl.when(t == 0)
    def _():
        state_copy(0).start()

    @pl.when(t == 1)
    def _():
        call(0, 1)

    load_lift.wait()
    for k in range(slots):
        lift_t[:, lane(k)] = lift[k].astype(F32).T.astype(BF16)
    pick_t[...] = pick[...].T.astype(BF16)
    load_pitch.wait()
    load_faces.wait()
    load_mixing.wait()
    row_of = lax.broadcasted_iota(jnp.int32, (levels, nodes), 0)
    angles = jnp.zeros((levels, nodes), F32)
    for n in range(levels):
        angles = jnp.where(row_of == n, pitch[n], angles)
    cosines[...] = jnp.cos(angles)
    sines[...] = jnp.sin(angles)
    row_at = lax.broadcasted_iota(jnp.int32, (blocks, blocks), 0)
    for k in range(1, slots):
        chosen = jnp.where(faces[k - 1 : k, :] == row_at, 1.0, 0.0)
        near[(k - 1) * blocks : k * blocks, :] = chosen.T.astype(BF16)
        turned = chosen.astype(BF16)
        near_t[(k - 1) * blocks : k * blocks, :blocks] = turned
        near_t[(k - 1) * blocks : k * blocks, blocks:] = turned
    slot_at = lax.rem(row_at, ghosts)
    for pair in range(2):
        upper = faces[2 * pair : 2 * pair + 1, :] - blocks
        lower = faces[2 * pair + 1 : 2 * pair + 2, :] - blocks
        wanted = jnp.where(row_at < ghosts, upper, lower)
        chosen = jnp.where(wanted == slot_at, 1.0, 0.0)
        far[:, pair * blocks : (pair + 1) * blocks] = chosen.T.astype(BF16)
        turned = chosen.astype(BF16)
        far_t[pair * blocks : (pair + 1) * blocks, :blocks] = turned
        far_t[pair * blocks : (pair + 1) * blocks, blocks:] = turned
    wide_pick = pick[...].astype(BF16)
    for part in range(3):
        pick_wide[:, part * blocks : (part + 1) * blocks] = wide_pick
    far_pick[...] = matmul(wide_pick, far[...]).astype(BF16)
    crossed = matmul(far_t[:, :blocks], pick_t[...]).astype(BF16)
    cross[...] = jnp.concatenate([crossed, crossed], axis=1)
    load_metric.wait()
    in_thirds(STEP_SIZE * metric[...], lane(0))
    picked_scale[...] = matmul(pick_wide[...], thirds[:, lane(0)])
    load_sources.wait()
    last = half - 2 + t

    def forward_level(i, carry):
        forward_near(i)
        forward_ahead()
        forward_far(i)

        @pl.when(i < last)
        def _():
            send_picked(i + 1)

        forward_end(i)

        @pl.when(i < last)
        def _():
            squash(lambda c: states[first + i + 1, c])

        @pl.when(t == 0)
        def _():
            state_copy(i + 1).start()

        return carry

    lax.fori_loop(0, half - 1 + t, forward_level, 0)

    load_weight.wait()
    load_end.wait()

    @pl.when(t == 0)
    def _():
        send_bend()

    @pl.when(t == 1)
    def _():
        pl.semaphore_wait(hello.at[0], 2)
        call(1, 2)
        for e in range(comps):
            adjoint[e] = adjoint[e] + weight[e] * states[levels, e]
        split_field(adjoint)
        send_reverse(0)

        def reverse_level(j, carry):
            n = levels - 1 - j

            @pl.when(n < half)
            def _():
                state_copy(n).wait_recv()

            reverse_sum(n, adjoint)
            reverse_near(n)
            reverse_ahead()
            reverse_wait(j)
            send_ahead(j + 1)
            reverse_far(j)
            split_field(adjoint)

            @pl.when(n == half)
            def _():
                kept[...] = adjoint[...]
                keep_copy.start()

            return carry

        lax.fori_loop(0, levels - 2, reverse_level, 0)
        state_copy(1).wait_recv()
        reverse_sum(1, adjoint)
        reverse_near(1)
        pl.semaphore_wait(hello.at[1], 2)
        call(2, 2)
        last_sum(levels - 2)
        plane_parts[spot] = partial[...]
        for r in range(1, plane):
            plane_copy(r).start()
        reverse_ahead()
        reverse_wait(levels - 2)
        send_ahead(levels - 1)
        reverse_far(levels - 2)
        split_field(adjoint)
        pl.semaphore_wait(hello.at[2], 2)
        for r in range(1, plane):
            other = lax.rem(spot + r, plane)
            pltpu.make_async_remote_copy(
                src_ref=partial,
                dst_ref=plane_parts.at[other],
                send_sem=plane_send.at[r],
                recv_sem=plane_recv.at[other],
                device_id=(1, p),
                device_id_type=MESH,
            ).wait_recv()
        total = plane_parts[0]
        for s in range(1, plane):
            total = total + plane_parts[s]
        plane_sum[...] = total
        layer_parts[layer] = total
        for r in range(layers):
            layer_copy(r, 0).start()
            if r > 0:
                layer_copy(r, 1).start()
        state_copy(0).wait_recv()
        reverse_near(0)
        reverse_wait(levels - 1)
        reverse_far(levels - 1)
        end_copy.start()

    def layer_wait(r):
        other = lax.rem(layer + r, layers)
        pltpu.make_async_remote_copy(
            src_ref=plane_sum,
            dst_ref=layer_parts.at[other],
            send_sem=layer_send.at[0, r],
            recv_sem=layer_recv.at[other],
            device_id=(1 - t, p),
            device_id_type=MESH,
        ).wait_recv()

    for r in range(1, layers):
        layer_wait(r)

    @pl.when(t == 0)
    def _():
        layer_wait(0)

    total = layer_parts[0]
    for s in range(1, layers):
        total = total + layer_parts[s]
    norm = math.sqrt(comps * nodes * blocks * n_space)
    sums = jnp.sum(total, axis=1, keepdims=True) * (STEP_SIZE / norm)
    diagonal = lax.broadcasted_iota(jnp.int32, (levels, nodes), 1) == row_of
    grads_row[...] = jnp.sum(jnp.where(diagonal, sums, 0.0), axis=0, keepdims=True)
    give_sums = pltpu.make_async_copy(grads_row, grads, out_sem.at[1])
    give_sums.start()

    def drain(i, carry):
        for d, offset in enumerate(OFFSETS):

            @pl.when(exists(p + offset))
            def _():
                fwd_copy(i, d, p).wait_send()

        return carry

    lax.fori_loop(0, half - 1 + t, drain, 0)

    @pl.when(t == 0)
    def _():
        end_copy.wait_recv()
        for i in range(half):
            state_copy(i).wait_send()
        for d, offset in enumerate(OFFSETS):

            @pl.when(exists(p + offset))
            def _():
                bend_copy(d, p).wait_send()

        bend_pass.wait_send()

    @pl.when(t == 1)
    def _():
        def drain_reverse(j, carry):
            for d, offset in enumerate(OFFSETS):

                @pl.when(exists(p - offset))
                def _():
                    rev_copy(j, d, p).wait_send()

            return carry

        lax.fori_loop(0, levels, drain_reverse, 0)
        keep_copy.wait()
        end_copy.wait_send()
        for r in range(1, plane):
            plane_copy(r).wait_send()
        for r in range(layers):
            layer_copy(r, 0).wait_send()
            if r > 0:
                layer_copy(r, 1).wait_send()

    give_sums.wait()


def solution(mesh):
    n_space = mesh.shape["space"]
    plane = 16 if n_space % 16 == 0 else 4

    def shards(
        checkpoints, sources, pitch, metric, obj_weight, adjoint_end, lift, mixing, faces, send_idx
    ):
        comps, blocks, nodes = obj_weight.shape
        slots = lift.shape[0]
        levels = pitch.shape[0]
        half = levels // 2
        halo = send_idx.shape[2]
        ghosts = 4 * halo
        wide = comps * nodes
        links = slots - 1
        layers = n_space // plane
        vmem = pltpu.VMEM
        dma = pltpu.SemaphoreType.DMA
        field = (comps, blocks, nodes)
        smem = pltpu.SMEM
        scratch = [
            smem((levels,), F32),
            smem(mixing.shape, F32),
            vmem((links, blocks), jnp.int32),
            smem(send_idx.shape, jnp.int32),
            vmem((1, nodes), F32),
            vmem((levels + 1, *field), F32),
            vmem((2, *field), F32),
            vmem((blocks, nodes), F32),
            vmem(field, F32),
            vmem(field, F32),
            vmem(field, F32),
            vmem((slots, nodes, nodes), BF16),
            vmem((nodes, slots * nodes), BF16),
            vmem((levels, nodes), F32),
            vmem((levels, nodes), F32),
            vmem((ghosts, blocks), F32),
            vmem((blocks, ghosts), BF16),
            vmem((links * blocks, blocks), BF16),
            vmem((links * blocks, 2 * blocks), BF16),
            vmem((blocks, links * ghosts), BF16),
            vmem((links * ghosts, 2 * blocks), BF16),
            vmem((ghosts, links * ghosts), BF16),
            vmem((links * ghosts, 2 * ghosts), BF16),
            vmem((ghosts, 3 * blocks), BF16),
            vmem((3 * blocks, wide), BF16),
            vmem((ghosts, wide), F32),
            vmem((ghosts, nodes), F32),
            vmem((ghosts, wide), F32),
            vmem((2 * ghosts, wide), BF16),
            vmem((comps * ghosts, nodes), F32),
            vmem((blocks, wide), BF16),
            vmem((links * blocks, wide), BF16),
            vmem((slots, comps * blocks, nodes), F32),
            vmem(field, F32),
            vmem(field, F32),
            vmem((comps * ghosts, links * nodes), F32),
            vmem((links * ghosts, wide), BF16),
            vmem((2 * blocks, wide), BF16),
            vmem((links * blocks, wide), F32),
            vmem((links * ghosts, wide), F32),
            vmem((comps * blocks, slots * nodes), BF16),
            vmem((comps * ghosts, links * nodes), BF16),
            vmem((half, 4, halo, wide), BF16),
            vmem((half, 4, halo, wide), BF16),
            vmem((levels, 4, halo, wide), BF16),
            vmem((levels, 4, halo, wide), BF16),
            vmem((4, halo, wide), BF16),
            vmem((4, halo, wide), BF16),
            vmem((4, halo, wide), BF16),
            vmem((levels, nodes), F32),
            vmem((plane, levels, nodes), F32),
            vmem((levels, nodes), F32),
            vmem((layers, levels, nodes), F32),
            dma((10,)),
            dma((half, 4)),
            dma((half, 4)),
            dma((levels, 4)),
            dma((levels, 4)),
            dma((4,)),
            dma((4,)),
            dma((2,)),
            dma((half,)),
            dma((half,)),
            dma((plane,)),
            dma((plane,)),
            dma((2, layers)),
            dma((layers,)),
            dma((2,)),
            dma((2,)),
            pltpu.SemaphoreType.REGULAR((3,)),
        ]
        anywhere = pl.BlockSpec(memory_space=pl.ANY)
        results, sums = pl.pallas_call(
            functools.partial(sweep, n_space, plane),
            out_shape=(
                jax.ShapeDtypeStruct((1, *field), F32),
                jax.ShapeDtypeStruct((1, nodes), F32),
            ),
            in_specs=[pl.BlockSpec(memory_space=pltpu.HBM)] * 10,
            out_specs=(anywhere, anywhere),
            scratch_shapes=scratch,
            compiler_params=pltpu.CompilerParams(
                collective_id=0, has_side_effects=True, vmem_limit_bytes=67043328
            ),
            name="adjoint_window",
        )(checkpoints, sources, pitch, metric, obj_weight, adjoint_end, lift, mixing, faces.T, send_idx)
        return results, sums[0, :levels]

    return jax.shard_map(
        shards,
        mesh=mesh,
        in_specs=(
            P("tm", None, "space", None),
            P(None, None, "space", None),
            P(),
            P("space", None),
            P(None, "space", None),
            P(None, "space", None),
            P(),
            P(),
            P("space", None),
            P("space", None, None),
        ),
        out_specs=(P("tm", None, "space", None), P()),
        check_vma=False,
    )
```

```python
import functools
import math

import jax
import jax.numpy as jnp
from jax import lax
from jax.experimental import pallas as pl
from jax.experimental.pallas import tpu as pltpu
from jax.sharding import PartitionSpec as P

OFFSETS = (1, -1, 2, -2)
FARTHEST_FIRST = (2, 3, 0, 1)
STEP_SIZE = 0.5
MESH = pl.DeviceIdType.MESH
F32, BF16 = jnp.float32, jnp.bfloat16
CHUNK = 32
FAR_HALF_FIRST = (32, 0)


def matmul(left, right):
    return jnp.dot(left, right, preferred_element_type=F32)


def sweep(
    n_space,
    plane,
    checkpoint_in,
    sources_in,
    pitch_in,
    metric_in,
    weight_in,
    end_in,
    lift_in,
    mixing_in,
    faces_in,
    send_idx_in,
    bounds,
    grads,
    pitch,
    mixing,
    faces,
    send_idx,
    grads_row,
    states,
    sources,
    metric,
    weight,
    adjoint,
    kept,
    lift,
    lift_t,
    cosines,
    sines,
    pick,
    pick_t,
    near,
    near_t,
    far,
    far_t,
    far_pick,
    cross,
    pick_wide,
    thirds,
    picked,
    picked_scale,
    gain,
    back_split,
    ahead,
    squashed,
    gathered,
    lifted,
    base,
    slope,
    halo_lifted,
    halo_mixed,
    split,
    pulled,
    halo_pulled,
    mixed,
    far_mixed,
    fwd_out,
    fwd_in,
    rev_out,
    rev_in,
    bend_out,
    bend_in,
    bend_there,
    partial,
    plane_parts,
    plane_sum,
    layer_parts,
    in_sem,
    fwd_send,
    fwd_recv,
    rev_send,
    rev_recv,
    bend_send,
    bend_recv,
    bend_sem,
    state_send,
    state_recv,
    plane_send,
    plane_recv,
    layer_send,
    layer_recv,
    end_sem,
    out_sem,
    hello,
):
    comps, blocks, nodes = states.shape[1:]
    slots = lift.shape[0]
    halo = fwd_in.shape[2]
    ghosts = 4 * halo
    levels = pitch.shape[0]
    half = levels // 2
    layers = n_space // plane
    t = lax.axis_index("tm")
    p = lax.axis_index("space")
    spot = lax.rem(p, plane)
    layer = p // plane
    first = t * half

    def exists(q):
        return jnp.logical_and(q >= 0, q < n_space)

    def lane(c):
        return slice(c * nodes, (c + 1) * nodes)

    (
        load_first,
        load_idx,
        load_mixing,
        load_faces,
        load_pitch,
        load_lift,
        load_metric,
        load_sources,
        load_weight,
        load_end,
    ) = loads = [
        pltpu.make_async_copy(checkpoint_in.at[0], states.at[first], in_sem.at[0]),
        pltpu.make_async_copy(send_idx_in, send_idx, in_sem.at[6]),
        pltpu.make_async_copy(mixing_in, mixing, in_sem.at[7]),
        pltpu.make_async_copy(faces_in, faces, in_sem.at[8]),
        pltpu.make_async_copy(pitch_in, pitch, in_sem.at[9]),
        pltpu.make_async_copy(lift_in, lift, in_sem.at[1]),
        pltpu.make_async_copy(metric_in, metric, in_sem.at[2]),
        pltpu.make_async_copy(sources_in, sources, in_sem.at[3]),
        pltpu.make_async_copy(weight_in, weight, in_sem.at[4]),
        pltpu.make_async_copy(end_in, adjoint, in_sem.at[5]),
    ]
    barrier = pltpu.get_barrier_semaphore()

    def greet(device):
        pl.semaphore_signal(barrier, inc=1, device_id=device, device_id_type=MESH)

    for offset in OFFSETS:

        @pl.when(exists(p + offset))
        def _():
            greet((t, p + offset))

    greet((1 - t, p))

    def in_layer(r):
        return (1, lax.rem(layer + r + layers, layers) * plane + spot)

    @pl.when(t == 1)
    def _():
        greet(in_layer(1))
        greet(in_layer(-1))

    def call(which, distance):
        for r in (distance, -distance):
            pl.semaphore_signal(
                hello.at[which], inc=1, device_id=in_layer(r), device_id_type=MESH
            )

    for load in loads:
        load.start()

    load_idx.wait()
    lane_of = lax.broadcasted_iota(jnp.int32, (1, blocks), 1)
    for d in range(4):
        for s in range(halo):
            row = d * halo + s
            pick[pl.ds(row, 1), :] = jnp.where(lane_of == send_idx[0, d, s], 1.0, 0.0)

    for d, offset in enumerate(OFFSETS):

        @pl.when(jnp.logical_not(exists(p - offset)))
        def _():
            bend_in[d] = jnp.zeros(bend_in.shape[1:], BF16)
            for i in range(half):
                fwd_in[i, d] = jnp.zeros(fwd_in.shape[2:], BF16)

        @pl.when(jnp.logical_not(exists(p + offset)))
        def _():
            for i in range(levels):
                rev_in[i, d] = jnp.zeros(rev_in.shape[2:], BF16)

    def fwd_copy(i, d, device):
        return pltpu.make_async_remote_copy(
            src_ref=fwd_out.at[i, d],
            dst_ref=fwd_in.at[i, d],
            send_sem=fwd_send.at[i, d],
            recv_sem=fwd_recv.at[i, d],
            device_id=(t, device),
            device_id_type=MESH,
        )

    def rev_copy(i, d, device):
        return pltpu.make_async_remote_copy(
            src_ref=rev_out.at[i, d],
            dst_ref=rev_in.at[i, d],
            send_sem=rev_send.at[i, d],
            recv_sem=rev_recv.at[i, d],
            device_id=(t, device),
            device_id_type=MESH,
        )

    def bend_copy(d, device):
        return pltpu.make_async_remote_copy(
            src_ref=bend_out.at[d],
            dst_ref=bend_in.at[d],
            send_sem=bend_send.at[d],
            recv_sem=bend_recv.at[d],
            device_id=(t, device),
            device_id_type=MESH,
        )

    def state_copy(i):
        return pltpu.make_async_remote_copy(
            src_ref=states.at[i],
            dst_ref=states.at[i],
            send_sem=state_send.at[i],
            recv_sem=state_recv.at[i],
            device_id=(1 - t, p),
            device_id_type=MESH,
        )

    def plane_copy(r):
        return pltpu.make_async_remote_copy(
            src_ref=partial,
            dst_ref=plane_parts.at[spot],
            send_sem=plane_send.at[r],
            recv_sem=plane_recv.at[spot],
            device_id=(1, layer * plane + lax.rem(spot + r, plane)),
            device_id_type=MESH,
        )

    def layer_copy(r, core):
        return pltpu.make_async_remote_copy(
            src_ref=plane_sum,
            dst_ref=layer_parts.at[layer],
            send_sem=layer_send.at[core, r],
            recv_sem=layer_recv.at[layer],
            device_id=(core, lax.rem(layer + r, layers) * plane + spot),
            device_id_type=MESH,
        )

    bend_pass = pltpu.make_async_remote_copy(
        src_ref=bend_in,
        dst_ref=bend_there,
        send_sem=bend_sem.at[0],
        recv_sem=bend_sem.at[1],
        device_id=(1 - t, p),
        device_id_type=MESH,
    )
    end_copy = pltpu.make_async_remote_copy(
        src_ref=adjoint,
        dst_ref=bounds.at[0],
        send_sem=end_sem.at[0],
        recv_sem=end_sem.at[1],
        device_id=(1 - t, p),
        device_id_type=MESH,
    )
    keep_copy = pltpu.make_async_copy(kept, bounds.at[0], out_sem.at[0])

    def in_halves(value, where, columns):
        rows = value.shape[0]
        high = value.astype(BF16)
        where[:rows, columns] = high
        where[rows:, columns] = (value - high.astype(F32)).astype(BF16)

    def in_thirds(value, columns):
        for part in range(3):
            high = value.astype(BF16)
            thirds[part * blocks : (part + 1) * blocks, columns] = high
            value = value - high.astype(F32)

    def squash(state):
        for c in range(comps):
            squashed[:, lane(c)] = jnp.tanh(state(c)).astype(BF16)

    def send_forward(i):
        packets = matmul(pick[...].astype(BF16), squashed[...]).astype(BF16)
        for d in FARTHEST_FIRST:
            fwd_out[i, d] = packets[d * halo : (d + 1) * halo]

            @pl.when(exists(p + OFFSETS[d]))
            def _():
                fwd_copy(i, d, p + OFFSETS[d]).start()

    def forward_near(i):
        gathered[...] = matmul(near[...], squashed[...]).astype(BF16)
        for k in range(slots):
            rows = squashed if k == 0 else gathered.at[pl.ds((k - 1) * blocks, blocks)]
            left = jnp.concatenate([rows[:, lane(c)] for c in range(comps)], axis=0)
            lifted[k] = matmul(left, lift_t[:, lane(k)])
        cosine = cosines[pl.ds(first + i, 1), :]
        sine = sines[pl.ds(first + i, 1), :]
        for start in range(0, blocks, CHUNK):
            some = slice(start, start + CHUNK)
            totals = [None] * comps
            for k in range(slots):
                for c in range(comps):
                    term = lifted[k, c * blocks + start : c * blocks + start + CHUNK, :]
                    for e in range(comps):
                        more = mixing[k, e, c] * term
                        totals[e] = more if totals[e] is None else totals[e] + more
            for e in range(comps):
                forcing = cosine * sources[0, e, some, :] + sine * sources[1, e, some, :]
                change = forcing - metric[some, :] * totals[e]
                base[e, some, :] = states[first + i, e, some, :] + STEP_SIZE * change

    def forward_far(i):
        for d, offset in enumerate(OFFSETS):

            @pl.when(exists(p - offset))
            def _():
                fwd_copy(i, d, p).wait_recv()

        ghost = jnp.concatenate([fwd_in[i, d] for d in range(4)], axis=0)
        left = jnp.concatenate([ghost[:, lane(c)] for c in range(comps)], axis=0)
        halo_lifted[...] = matmul(left, lift_t[:, nodes:])
        for k in range(1, slots):
            for start in range(0, ghosts, CHUNK):
                totals = [None] * comps
                for c in range(comps):
                    term = halo_lifted[c * ghosts + start : c * ghosts + start + CHUNK, lane(k - 1)]
                    for e in range(comps):
                        more = mixing[k, e, c] * term
                        totals[e] = more if totals[e] is None else totals[e] + more
                row = (k - 1) * ghosts + start
                for e in range(comps):
                    halo_mixed[row : row + CHUNK, lane(e)] = totals[e].astype(BF16)

    def forward_ahead():
        for e in range(comps):
            in_thirds(base[e], lane(e))
        picked[...] = matmul(pick_wide[...], thirds[...])

    def send_picked(i):
        wide_scale = jnp.concatenate([picked_scale[...]] * comps, axis=1)
        for start in FAR_HALF_FIRST:
            some = slice(start, start + CHUNK)
            change = matmul(far_pick[some], halo_mixed[...])
            packets = jnp.tanh(picked[some] - wide_scale[some] * change).astype(BF16)
            for d in range(start // halo, (start + CHUNK) // halo):
                fwd_out[i, d] = packets[d * halo - start : (d + 1) * halo - start]

                @pl.when(exists(p + OFFSETS[d]))
                def _():
                    fwd_copy(i, d, p + OFFSETS[d]).start()

    def forward_end(i):
        scale = STEP_SIZE * metric[...]
        arrived = matmul(far[...], halo_mixed[...])
        for e in range(comps):
            states[first + i + 1, e] = base[e] - scale * arrived[:, lane(e)]

    def split_field(field):
        for e in range(comps):
            in_halves(metric[...] * field[e], split, lane(e))

    def far_product(start):
        for k in range(1, slots):
            row = (k - 1) * ghosts + start
            totals = [None] * comps
            for e in range(comps):
                term = halo_pulled[row : row + CHUNK, lane(e)]
                for c in range(comps):
                    more = mixing[k, e, c] * term
                    totals[c] = more if totals[c] is None else totals[c] + more
            for c in range(comps):
                far_mixed[c * ghosts + start : c * ghosts + start + CHUNK, lane(k - 1)] = totals[
                    c
                ].astype(BF16)
        left = jnp.concatenate(
            [far_mixed[c * ghosts + start : c * ghosts + start + CHUNK] for c in range(comps)], axis=0
        )
        right = jnp.concatenate([lift[k] for k in range(1, slots)], axis=0)
        return matmul(left, right)

    def ship_reverse(j, start, product):
        packets = product.astype(BF16)
        for d in range(start // halo, (start + CHUNK) // halo):
            for c in range(comps):
                row = c * CHUNK + d * halo - start
                rev_out[j, d, :, lane(c)] = packets[row : row + halo]

            @pl.when(exists(p - OFFSETS[d]))
            def _():
                rev_copy(j, d, p - OFFSETS[d]).start()

    def send_reverse(j):
        halo_pulled[...] = matmul(far_t[...], split[...])
        for start in FAR_HALF_FIRST:
            ship_reverse(j, start, far_product(start))

    def reverse_ahead():
        split_field(slope)
        gain[...] = matmul(pick_wide[:, : 2 * blocks], split[...])
        split_field(base)
        halo_pulled[...] = matmul(far_t[...], split[...])
        for start in FAR_HALF_FIRST:
            product = far_product(start)
            for c in range(comps):
                row = c * ghosts + start
                ahead[row : row + CHUNK] = product[c * CHUNK : (c + 1) * CHUNK]

    def send_ahead(j):
        for c in range(comps):
            back = jnp.concatenate([rev_in[j - 1, d, :, lane(c)] for d in range(4)], axis=0)
            in_halves(gain[:, lane(c)] * back.astype(F32), back_split, lane(c))
        for start in FAR_HALF_FIRST:
            rows = [slice(k * ghosts + start, k * ghosts + start + CHUNK) for k in range(slots - 1)]
            left = jnp.concatenate([cross[some] for some in rows], axis=0)
            product = matmul(left, back_split[...])
            for k, some in enumerate(rows):
                halo_pulled[some] = product[k * CHUNK : (k + 1) * CHUNK]
            made = jnp.concatenate(
                [ahead[c * ghosts + start : c * ghosts + start + CHUNK] for c in range(comps)], axis=0
            )
            ship_reverse(j, start, made - far_product(start))

    def reverse_sum(n, field):
        by_cosine = jnp.zeros((8, nodes), F32)
        by_sine = jnp.zeros((8, nodes), F32)
        for e in range(comps):
            value = field[e]
            by_cosine += jnp.sum((value * sources[1, e]).reshape(blocks // 8, 8, nodes), axis=0)
            by_sine += jnp.sum((value * sources[0, e]).reshape(blocks // 8, 8, nodes), axis=0)
        both = cosines[pl.ds(n, 1), :] * by_cosine - sines[pl.ds(n, 1), :] * by_sine
        partial[pl.ds(n, 1), :] = jnp.sum(both, axis=0, keepdims=True)

    def reverse_near(n):
        pulled[...] = matmul(near_t[...], split[...])
        for k in range(slots):
            for start in range(0, blocks, CHUNK):
                some = slice(start, start + CHUNK)
                totals = [None] * comps
                for e in range(comps):
                    if k == 0:
                        term = metric[some, :] * adjoint[e, some, :]
                    else:
                        row = (k - 1) * blocks + start
                        term = pulled[row : row + CHUNK, lane(e)]
                    for c in range(comps):
                        more = mixing[k, e, c] * term
                        totals[c] = more if totals[c] is None else totals[c] + more
                for c in range(comps):
                    mixed[c * blocks + start : c * blocks + start + CHUNK, lane(k)] = totals[c].astype(
                        BF16
                    )
        right = jnp.concatenate([lift[k] for k in range(slots)], axis=0)
        pushed = matmul(mixed[...], right)
        inner = jnp.where(n > 0, 1.0, 0.0).astype(F32)
        for c in range(comps):
            state = states[n, c]
            bent = jnp.tanh(state)
            fall = STEP_SIZE * (1.0 - bent * bent)
            slope[c] = fall
            grown = adjoint[c] + inner * (weight[c] * state)
            base[c] = grown - fall * pushed[c * blocks : (c + 1) * blocks]

    def reverse_wait(j):
        for d, offset in enumerate(OFFSETS):

            @pl.when(exists(p + offset))
            def _():
                rev_copy(j, d, p).wait_recv()

    def reverse_far(j):
        ghost = jnp.concatenate([rev_in[j, d] for d in range(4)], axis=0)
        arrived = matmul(pick_t[...], ghost)
        for c in range(comps):
            adjoint[c] = base[c] - slope[c] * arrived[:, lane(c)]

    def send_bend():
        for e in range(comps):
            bent = jnp.tanh(states[1, e])
            turning = cosines[0:1, :] * sources[1, e] - sines[0:1, :] * sources[0, e]
            squashed[:, lane(e)] = (STEP_SIZE * (1.0 - bent * bent) * turning).astype(BF16)
        packets = matmul(pick[...].astype(BF16), squashed[...]).astype(BF16)
        for d, offset in enumerate(OFFSETS):
            bend_out[d] = packets[d * halo : (d + 1) * halo]

            @pl.when(exists(p + offset))
            def _():
                bend_copy(d, p + offset).start()

        for d, offset in enumerate(OFFSETS):

            @pl.when(exists(p - offset))
            def _():
                bend_copy(d, p).wait_recv()

        bend_pass.start()

    def last_sum(j):
        reverse_sum(0, base)
        bend_pass.wait_recv()
        sent = jnp.zeros((halo, nodes), F32)
        for d in range(4):
            both = rev_out[j, d].astype(F32) * bend_there[d].astype(F32)
            for c in range(comps):
                sent += both[:, lane(c)]
        partial[0:1, :] = partial[0:1, :] - jnp.sum(sent, axis=0, keepdims=True)

    norm = math.sqrt(comps * nodes * blocks * n_space)

    def in_row(tile):
        sums = jnp.sum(tile, axis=1, keepdims=True) * (STEP_SIZE / norm)
        lanes = lax.broadcasted_iota(jnp.int32, (levels, nodes), 1)
        diagonal = lanes == lax.broadcasted_iota(jnp.int32, (levels, nodes), 0)
        return jnp.sum(jnp.where(diagonal, sums, 0.0), axis=0, keepdims=True)

    load_first.wait()
    squash(lambda c: states[first, c])
    near_peers = sum(exists(p + offset).astype(jnp.int32) for offset in OFFSETS)
    pl.semaphore_wait(barrier, near_peers + 1 + 2 * t)
    send_forward(0)

    @pl.when(t == 0)
    def _():
        state_copy(0).start()

    @pl.when(t == 1)
    def _():
        call(0, 1)

    load_lift.wait()
    for k in range(slots):
        lift_t[:, lane(k)] = lift[k].astype(F32).T.astype(BF16)
    pick_t[...] = pick[...].T.astype(BF16)
    load_pitch.wait()
    load_faces.wait()
    load_mixing.wait()
    row_of = lax.broadcasted_iota(jnp.int32, (levels, nodes), 0)
    angles = jnp.zeros((levels, nodes), F32)
    for n in range(levels):
        angles = jnp.where(row_of == n, pitch[n], angles)
    cosines[...] = jnp.cos(angles)
    sines[...] = jnp.sin(angles)
    row_at = lax.broadcasted_iota(jnp.int32, (blocks, blocks), 0)
    for k in range(1, slots):
        chosen = jnp.where(faces[k - 1 : k, :] == row_at, 1.0, 0.0)
        near[(k - 1) * blocks : k * blocks, :] = chosen.T.astype(BF16)
        turned = chosen.astype(BF16)
        near_t[(k - 1) * blocks : k * blocks, :blocks] = turned
        near_t[(k - 1) * blocks : k * blocks, blocks:] = turned
    slot_at = lax.rem(row_at, ghosts)
    for pair in range(2):
        upper = faces[2 * pair : 2 * pair + 1, :] - blocks
        lower = faces[2 * pair + 1 : 2 * pair + 2, :] - blocks
        wanted = jnp.where(row_at < ghosts, upper, lower)
        chosen = jnp.where(wanted == slot_at, 1.0, 0.0)
        far[:, pair * blocks : (pair + 1) * blocks] = chosen.T.astype(BF16)
        turned = chosen.astype(BF16)
        far_t[pair * blocks : (pair + 1) * blocks, :blocks] = turned
        far_t[pair * blocks : (pair + 1) * blocks, blocks:] = turned
    wide_pick = pick[...].astype(BF16)
    for part in range(3):
        pick_wide[:, part * blocks : (part + 1) * blocks] = wide_pick
    far_pick[...] = matmul(wide_pick, far[...]).astype(BF16)
    crossed = matmul(far_t[:, :blocks], pick_t[...]).astype(BF16)
    cross[...] = jnp.concatenate([crossed, crossed], axis=1)
    load_metric.wait()
    in_thirds(STEP_SIZE * metric[...], lane(0))
    picked_scale[...] = matmul(pick_wide[...], thirds[:, lane(0)])
    load_sources.wait()
    last = half - 2 + t

    def forward_level(i, carry):
        forward_near(i)
        forward_ahead()
        forward_far(i)

        @pl.when(i < last)
        def _():
            send_picked(i + 1)

        forward_end(i)

        @pl.when(i < last)
        def _():
            squash(lambda c: states[first + i + 1, c])

        @pl.when(t == 0)
        def _():
            state_copy(i + 1).start()

        return carry

    lax.fori_loop(0, half - 1 + t, forward_level, 0)

    load_weight.wait()
    load_end.wait()

    @pl.when(t == 0)
    def _():
        send_bend()

    @pl.when(t == 1)
    def _():
        pl.semaphore_wait(hello.at[0], 2)
        call(1, 2)
        for e in range(comps):
            adjoint[e] = adjoint[e] + weight[e] * states[levels, e]
        split_field(adjoint)
        send_reverse(0)

        def reverse_level(j, carry):
            n = levels - 1 - j

            @pl.when(n < half)
            def _():
                state_copy(n).wait_recv()

            reverse_sum(n, adjoint)
            reverse_near(n)
            reverse_ahead()
            reverse_wait(j)
            send_ahead(j + 1)
            reverse_far(j)
            split_field(adjoint)

            @pl.when(n == half)
            def _():
                kept[...] = adjoint[...]
                keep_copy.start()

            return carry

        lax.fori_loop(0, levels - 2, reverse_level, 0)
        state_copy(1).wait_recv()
        reverse_sum(1, adjoint)
        reverse_near(1)
        pl.semaphore_wait(hello.at[1], 2)
        call(2, 2)
        last_sum(levels - 2)
        plane_parts[spot] = partial[...]
        for r in range(1, plane):
            plane_copy(r).start()
        reverse_ahead()
        reverse_wait(levels - 2)
        send_ahead(levels - 1)
        reverse_far(levels - 2)
        split_field(adjoint)
        pl.semaphore_wait(hello.at[2], 2)
        for r in range(1, plane):
            other = lax.rem(spot + r, plane)
            pltpu.make_async_remote_copy(
                src_ref=partial,
                dst_ref=plane_parts.at[other],
                send_sem=plane_send.at[r],
                recv_sem=plane_recv.at[other],
                device_id=(1, p),
                device_id_type=MESH,
            ).wait_recv()
        total = plane_parts[0]
        for s in range(1, plane):
            total = total + plane_parts[s]
        row = in_row(total)
        plane_sum[...] = row
        layer_parts[layer] = row
        for r in range(layers):
            layer_copy(r, 0).start()
            if r > 0:
                layer_copy(r, 1).start()
        state_copy(0).wait_recv()
        reverse_near(0)
        reverse_wait(levels - 1)
        reverse_far(levels - 1)
        end_copy.start()

    def drain(i, carry):
        for d, offset in enumerate(OFFSETS):

            @pl.when(exists(p + offset))
            def _():
                fwd_copy(i, d, p).wait_send()

        return carry

    lax.fori_loop(0, half - 1 + t, drain, 0)

    @pl.when(t == 0)
    def _():
        for i in range(half):
            state_copy(i).wait_send()
        for d, offset in enumerate(OFFSETS):

            @pl.when(exists(p + offset))
            def _():
                bend_copy(d, p).wait_send()

        bend_pass.wait_send()

    @pl.when(t == 1)
    def _():
        def drain_reverse(j, carry):
            for d, offset in enumerate(OFFSETS):

                @pl.when(exists(p - offset))
                def _():
                    rev_copy(j, d, p).wait_send()

            return carry

        lax.fori_loop(0, levels, drain_reverse, 0)
        keep_copy.wait()
        for r in range(1, plane):
            plane_copy(r).wait_send()
        for r in range(layers):
            layer_copy(r, 0).wait_send()
            if r > 0:
                layer_copy(r, 1).wait_send()

    def layer_wait(r):
        other = lax.rem(layer + r, layers)
        pltpu.make_async_remote_copy(
            src_ref=plane_sum,
            dst_ref=layer_parts.at[other],
            send_sem=layer_send.at[0, r],
            recv_sem=layer_recv.at[other],
            device_id=(1 - t, p),
            device_id_type=MESH,
        ).wait_recv()

    for r in range(1, layers):
        layer_wait(r)

    @pl.when(t == 0)
    def _():
        layer_wait(0)

    total = layer_parts[0]
    for s in range(1, layers):
        total = total + layer_parts[s]
    grads_row[...] = total
    give_sums = pltpu.make_async_copy(grads_row, grads, out_sem.at[1])
    give_sums.start()

    @pl.when(t == 0)
    def _():
        end_copy.wait_recv()

    @pl.when(t == 1)
    def _():
        end_copy.wait_send()

    give_sums.wait()


def deliver(found, row, bounds, grads, held, sums, sums_out, sem):
    comps = held.shape[0]
    into = [pltpu.make_async_copy(found.at[0, c], held.at[c], sem.at[0, c]) for c in range(comps)]
    outof = [pltpu.make_async_copy(held.at[c], bounds.at[0, c], sem.at[1, c]) for c in range(comps)]
    row_in = pltpu.make_async_copy(row, sums, sem.at[0, comps])
    row_out = pltpu.make_async_copy(sums_out, grads, sem.at[1, comps])
    row_in.start()
    for copy in into:
        copy.start()
    row_in.wait()
    sums_out[...] = sums[0, : sums_out.shape[0]]
    row_out.start()
    for arrive, leave in zip(into, outof):
        arrive.wait()
        leave.start()
    row_out.wait()
    for leave in outof:
        leave.wait()


def solution(mesh):
    n_space = mesh.shape["space"]
    plane = 16 if n_space % 16 == 0 else 4

    def shards(
        checkpoints, sources, pitch, metric, obj_weight, adjoint_end, lift, mixing, faces, send_idx
    ):
        comps, blocks, nodes = obj_weight.shape
        slots = lift.shape[0]
        levels = pitch.shape[0]
        half = levels // 2
        halo = send_idx.shape[2]
        ghosts = 4 * halo
        wide = comps * nodes
        links = slots - 1
        layers = n_space // plane
        vmem = pltpu.VMEM
        dma = pltpu.SemaphoreType.DMA
        field = (comps, blocks, nodes)
        smem = pltpu.SMEM
        scratch = [
            smem((levels,), F32),
            smem(mixing.shape, F32),
            vmem((links, blocks), jnp.int32),
            smem(send_idx.shape, jnp.int32),
            vmem((1, nodes), F32),
            vmem((levels + 1, *field), F32),
            vmem((2, *field), F32),
            vmem((blocks, nodes), F32),
            vmem(field, F32),
            vmem(field, F32),
            vmem(field, F32),
            vmem((slots, nodes, nodes), BF16),
            vmem((nodes, slots * nodes), BF16),
            vmem((levels, nodes), F32),
            vmem((levels, nodes), F32),
            vmem((ghosts, blocks), F32),
            vmem((blocks, ghosts), BF16),
            vmem((links * blocks, blocks), BF16),
            vmem((links * blocks, 2 * blocks), BF16),
            vmem((blocks, links * ghosts), BF16),
            vmem((links * ghosts, 2 * blocks), BF16),
            vmem((ghosts, links * ghosts), BF16),
            vmem((links * ghosts, 2 * ghosts), BF16),
            vmem((ghosts, 3 * blocks), BF16),
            vmem((3 * blocks, wide), BF16),
            vmem((ghosts, wide), F32),
            vmem((ghosts, nodes), F32),
            vmem((ghosts, wide), F32),
            vmem((2 * ghosts, wide), BF16),
            vmem((comps * ghosts, nodes), F32),
            vmem((blocks, wide), BF16),
            vmem((links * blocks, wide), BF16),
            vmem((slots, comps * blocks, nodes), F32),
            vmem(field, F32),
            vmem(field, F32),
            vmem((comps * ghosts, links * nodes), F32),
            vmem((links * ghosts, wide), BF16),
            vmem((2 * blocks, wide), BF16),
            vmem((links * blocks, wide), F32),
            vmem((links * ghosts, wide), F32),
            vmem((comps * blocks, slots * nodes), BF16),
            vmem((comps * ghosts, links * nodes), BF16),
            vmem((half, 4, halo, wide), BF16),
            vmem((half, 4, halo, wide), BF16),
            vmem((levels, 4, halo, wide), BF16),
            vmem((levels, 4, halo, wide), BF16),
            vmem((4, halo, wide), BF16),
            vmem((4, halo, wide), BF16),
            vmem((4, halo, wide), BF16),
            vmem((levels, nodes), F32),
            vmem((plane, levels, nodes), F32),
            vmem((1, nodes), F32),
            vmem((layers, 1, nodes), F32),
            dma((10,)),
            dma((half, 4)),
            dma((half, 4)),
            dma((levels, 4)),
            dma((levels, 4)),
            dma((4,)),
            dma((4,)),
            dma((2,)),
            dma((half,)),
            dma((half,)),
            dma((plane,)),
            dma((plane,)),
            dma((2, layers)),
            dma((layers,)),
            dma((2,)),
            dma((2,)),
            pltpu.SemaphoreType.REGULAR((3,)),
        ]
        anywhere = pl.BlockSpec(memory_space=pl.ANY)
        results, sums = pl.pallas_call(
            functools.partial(sweep, n_space, plane),
            out_shape=(
                jax.ShapeDtypeStruct((1, *field), F32),
                jax.ShapeDtypeStruct((1, nodes), F32),
            ),
            in_specs=[pl.BlockSpec(memory_space=pltpu.HBM)] * 10,
            out_specs=(anywhere, anywhere),
            scratch_shapes=scratch,
            compiler_params=pltpu.CompilerParams(
                collective_id=0, has_side_effects=True, vmem_limit_bytes=67043328
            ),
            name="adjoint_window",
        )(checkpoints, sources, pitch, metric, obj_weight, adjoint_end, lift, mixing, faces.T, send_idx)
        return pl.pallas_call(
            deliver,
            out_shape=(
                jax.ShapeDtypeStruct((1, *field), F32),
                jax.ShapeDtypeStruct((levels,), F32),
            ),
            in_specs=[anywhere, anywhere],
            out_specs=(anywhere, anywhere),
            scratch_shapes=[
                vmem(field, F32),
                vmem((1, nodes), F32),
                vmem((levels,), F32),
                dma((2, comps + 1)),
            ],
            compiler_params=pltpu.CompilerParams(vmem_limit_bytes=67043328),
            name="deliver",
        )(results, sums)

    return jax.shard_map(
        shards,
        mesh=mesh,
        in_specs=(
            P("tm", None, "space", None),
            P(None, None, "space", None),
            P(),
            P("space", None),
            P(None, "space", None),
            P(None, "space", None),
            P(),
            P(),
            P("space", None),
            P("space", None, None),
        ),
        out_specs=(P("tm", None, "space", None), P()),
        check_vma=False,
    )
```

```python
import functools
import math

import jax
import jax.numpy as jnp
from jax import lax
from jax.experimental import pallas as pl
from jax.experimental.pallas import tpu as pltpu
from jax.sharding import PartitionSpec as P

OFFSETS = (1, -1, 2, -2)
FARTHEST_FIRST = (2, 3, 0, 1)
STEP_SIZE = 0.5
MESH = pl.DeviceIdType.MESH
F32, BF16 = jnp.float32, jnp.bfloat16
CHUNK = 32
FAR_HALF_FIRST = (32, 0)


def matmul(left, right):
    return jnp.dot(left, right, preferred_element_type=F32)


def parity(level):
    return level % 2 if isinstance(level, int) else lax.rem(level, 2)


def sweep(
    n_space,
    plane,
    checkpoint_in,
    sources_in,
    pitch_in,
    metric_in,
    weight_in,
    end_in,
    lift_in,
    mixing_in,
    faces_in,
    send_idx_in,
    bounds,
    grads,
    pitch,
    mixing,
    faces,
    send_idx,
    grads_row,
    states,
    sources,
    metric,
    weight,
    adjoint,
    kept,
    lift,
    lift_t,
    cosines,
    sines,
    pick,
    pick_t,
    near,
    near_t,
    far,
    far_t,
    far_pick,
    cross,
    pick_wide,
    thirds,
    picked,
    picked_scale,
    gain,
    back_split,
    ahead,
    squashed,
    gathered,
    lifted,
    base,
    slope,
    halo_lifted,
    halo_mixed,
    split,
    pulled,
    halo_pulled,
    mixed,
    far_mixed,
    fwd_out,
    fwd_in,
    rev_out,
    rev_in,
    bend_out,
    bend_in,
    bend_there,
    partial,
    plane_parts,
    plane_sum,
    layer_parts,
    in_sem,
    fwd_send,
    fwd_recv,
    rev_send,
    rev_recv,
    bend_send,
    bend_recv,
    bend_sem,
    state_send,
    state_recv,
    plane_send,
    plane_recv,
    layer_send,
    layer_recv,
    end_sem,
    out_sem,
    hello,
):
    comps, blocks, nodes = states.shape[1:]
    slots = lift.shape[0]
    halo = fwd_in.shape[2]
    ghosts = 4 * halo
    levels = pitch.shape[0]
    half = levels // 2
    layers = n_space // plane
    t = lax.axis_index("tm")
    p = lax.axis_index("space")
    spot = lax.rem(p, plane)
    layer = p // plane
    first = t * half

    def exists(q):
        return jnp.logical_and(q >= 0, q < n_space)

    def lane(c):
        return slice(c * nodes, (c + 1) * nodes)

    (
        load_first,
        load_idx,
        load_mixing,
        load_faces,
        load_pitch,
        load_lift,
        load_metric,
        load_sources,
        load_weight,
        load_end,
    ) = loads = [
        pltpu.make_async_copy(checkpoint_in.at[0], states.at[first], in_sem.at[0]),
        pltpu.make_async_copy(send_idx_in, send_idx, in_sem.at[6]),
        pltpu.make_async_copy(mixing_in, mixing, in_sem.at[7]),
        pltpu.make_async_copy(faces_in, faces, in_sem.at[8]),
        pltpu.make_async_copy(pitch_in, pitch, in_sem.at[9]),
        pltpu.make_async_copy(lift_in, lift, in_sem.at[1]),
        pltpu.make_async_copy(metric_in, metric, in_sem.at[2]),
        pltpu.make_async_copy(sources_in, sources, in_sem.at[3]),
        pltpu.make_async_copy(weight_in, weight, in_sem.at[4]),
        pltpu.make_async_copy(end_in, adjoint, in_sem.at[5]),
    ]
    barrier = pltpu.get_barrier_semaphore()

    def greet(device):
        pl.semaphore_signal(barrier, inc=1, device_id=device, device_id_type=MESH)

    for offset in OFFSETS:

        @pl.when(exists(p + offset))
        def _():
            greet((t, p + offset))

    greet((1 - t, p))

    def in_layer(r):
        return (1, lax.rem(layer + r + layers, layers) * plane + spot)

    @pl.when(t == 1)
    def _():
        greet(in_layer(1))
        greet(in_layer(-1))

    def call(which, distance):
        for r in (distance, -distance):
            pl.semaphore_signal(
                hello.at[which], inc=1, device_id=in_layer(r), device_id_type=MESH
            )

    for load in loads:
        load.start()

    load_idx.wait()
    lane_of = lax.broadcasted_iota(jnp.int32, (1, blocks), 1)
    for d in range(4):
        for s in range(halo):
            row = d * halo + s
            pick[pl.ds(row, 1), :] = jnp.where(lane_of == send_idx[0, d, s], 1.0, 0.0)

    for d, offset in enumerate(OFFSETS):

        @pl.when(jnp.logical_not(exists(p - offset)))
        def _():
            bend_in[d] = jnp.zeros(bend_in.shape[1:], BF16)
            for i in range(half):
                fwd_in[i, d] = jnp.zeros(fwd_in.shape[2:], BF16)

        @pl.when(jnp.logical_not(exists(p + offset)))
        def _():
            for i in range(levels):
                rev_in[i, d] = jnp.zeros(rev_in.shape[2:], BF16)

    def fwd_copy(i, d, device):
        return pltpu.make_async_remote_copy(
            src_ref=fwd_out.at[i, d],
            dst_ref=fwd_in.at[i, d],
            send_sem=fwd_send.at[parity(i), d],
            recv_sem=fwd_recv.at[parity(i), d],
            device_id=(t, device),
            device_id_type=MESH,
        )

    def rev_copy(i, d, device):
        return pltpu.make_async_remote_copy(
            src_ref=rev_out.at[i, d],
            dst_ref=rev_in.at[i, d],
            send_sem=rev_send.at[parity(i), d],
            recv_sem=rev_recv.at[parity(i), d],
            device_id=(t, device),
            device_id_type=MESH,
        )

    def bend_copy(d, device):
        return pltpu.make_async_remote_copy(
            src_ref=bend_out.at[d],
            dst_ref=bend_in.at[d],
            send_sem=bend_send.at[d],
            recv_sem=bend_recv.at[d],
            device_id=(t, device),
            device_id_type=MESH,
        )

    def state_copy(i):
        return pltpu.make_async_remote_copy(
            src_ref=states.at[i],
            dst_ref=states.at[i],
            send_sem=state_send.at[i],
            recv_sem=state_recv.at[i],
            device_id=(1 - t, p),
            device_id_type=MESH,
        )

    def plane_copy(r):
        return pltpu.make_async_remote_copy(
            src_ref=partial,
            dst_ref=plane_parts.at[spot],
            send_sem=plane_send,
            recv_sem=plane_recv,
            device_id=(1, layer * plane + lax.rem(spot + r, plane)),
            device_id_type=MESH,
        )

    def layer_copy(r, core):
        return pltpu.make_async_remote_copy(
            src_ref=plane_sum,
            dst_ref=layer_parts.at[layer],
            send_sem=layer_send,
            recv_sem=layer_recv,
            device_id=(core, lax.rem(layer + r, layers) * plane + spot),
            device_id_type=MESH,
        )

    bend_pass = pltpu.make_async_remote_copy(
        src_ref=bend_in,
        dst_ref=bend_there,
        send_sem=bend_sem.at[0],
        recv_sem=bend_sem.at[1],
        device_id=(1 - t, p),
        device_id_type=MESH,
    )
    def all_parts(parts, count, send_sem, recv_sem):
        return pltpu.make_async_remote_copy(
            src_ref=parts.at[pl.ds(0, count)],
            dst_ref=parts.at[pl.ds(0, count)],
            send_sem=send_sem,
            recv_sem=recv_sem,
            device_id=(1 - t, p),
            device_id_type=MESH,
        )

    end_copy = pltpu.make_async_remote_copy(
        src_ref=adjoint,
        dst_ref=bounds.at[0],
        send_sem=end_sem.at[0],
        recv_sem=end_sem.at[1],
        device_id=(1 - t, p),
        device_id_type=MESH,
    )
    keep_copy = pltpu.make_async_copy(kept, bounds.at[0], out_sem.at[0])

    def fwd_sent(i):
        for d, offset in enumerate(OFFSETS):

            @pl.when(exists(p + offset))
            def _():
                fwd_copy(i, d, p).wait_send()

    def rev_sent(j):
        for d, offset in enumerate(OFFSETS):

            @pl.when(exists(p - offset))
            def _():
                rev_copy(j, d, p).wait_send()

    def in_halves(value, where, columns):
        rows = value.shape[0]
        high = value.astype(BF16)
        where[:rows, columns] = high
        where[rows:, columns] = (value - high.astype(F32)).astype(BF16)

    def in_thirds(value, columns):
        for part in range(3):
            high = value.astype(BF16)
            thirds[part * blocks : (part + 1) * blocks, columns] = high
            value = value - high.astype(F32)

    def squash(state):
        for c in range(comps):
            squashed[:, lane(c)] = jnp.tanh(state(c)).astype(BF16)

    def send_forward(i):
        packets = matmul(pick[...].astype(BF16), squashed[...]).astype(BF16)
        for d in FARTHEST_FIRST:
            fwd_out[i, d] = packets[d * halo : (d + 1) * halo]

            @pl.when(exists(p + OFFSETS[d]))
            def _():
                fwd_copy(i, d, p + OFFSETS[d]).start()

    def forward_near(i):
        gathered[...] = matmul(near[...], squashed[...]).astype(BF16)
        for k in range(slots):
            rows = squashed if k == 0 else gathered.at[pl.ds((k - 1) * blocks, blocks)]
            left = jnp.concatenate([rows[:, lane(c)] for c in range(comps)], axis=0)
            lifted[k] = matmul(left, lift_t[:, lane(k)])
        cosine = cosines[pl.ds(first + i, 1), :]
        sine = sines[pl.ds(first + i, 1), :]
        for start in range(0, blocks, CHUNK):
            some = slice(start, start + CHUNK)
            totals = [None] * comps
            for k in range(slots):
                for c in range(comps):
                    term = lifted[k, c * blocks + start : c * blocks + start + CHUNK, :]
                    for e in range(comps):
                        more = mixing[k, e, c] * term
                        totals[e] = more if totals[e] is None else totals[e] + more
            for e in range(comps):
                forcing = cosine * sources[0, e, some, :] + sine * sources[1, e, some, :]
                change = forcing - metric[some, :] * totals[e]
                base[e, some, :] = states[first + i, e, some, :] + STEP_SIZE * change

    def forward_far(i):
        for d, offset in enumerate(OFFSETS):

            @pl.when(exists(p - offset))
            def _():
                fwd_copy(i, d, p).wait_recv()

        ghost = jnp.concatenate([fwd_in[i, d] for d in range(4)], axis=0)
        left = jnp.concatenate([ghost[:, lane(c)] for c in range(comps)], axis=0)
        halo_lifted[...] = matmul(left, lift_t[:, nodes:])
        for k in range(1, slots):
            for start in range(0, ghosts, CHUNK):
                totals = [None] * comps
                for c in range(comps):
                    term = halo_lifted[c * ghosts + start : c * ghosts + start + CHUNK, lane(k - 1)]
                    for e in range(comps):
                        more = mixing[k, e, c] * term
                        totals[e] = more if totals[e] is None else totals[e] + more
                row = (k - 1) * ghosts + start
                for e in range(comps):
                    halo_mixed[row : row + CHUNK, lane(e)] = totals[e].astype(BF16)

    def forward_ahead():
        for e in range(comps):
            in_thirds(base[e], lane(e))
        picked[...] = matmul(pick_wide[...], thirds[...])

    def send_picked(i):
        wide_scale = jnp.concatenate([picked_scale[...]] * comps, axis=1)
        for start in FAR_HALF_FIRST:
            some = slice(start, start + CHUNK)
            change = matmul(far_pick[some], halo_mixed[...])
            packets = jnp.tanh(picked[some] - wide_scale[some] * change).astype(BF16)
            for d in range(start // halo, (start + CHUNK) // halo):
                fwd_out[i, d] = packets[d * halo - start : (d + 1) * halo - start]

                @pl.when(exists(p + OFFSETS[d]))
                def _():
                    fwd_copy(i, d, p + OFFSETS[d]).start()

    def forward_end(i):
        scale = STEP_SIZE * metric[...]
        arrived = matmul(far[...], halo_mixed[...])
        for e in range(comps):
            states[first + i + 1, e] = base[e] - scale * arrived[:, lane(e)]

    def split_field(field):
        for e in range(comps):
            in_halves(metric[...] * field[e], split, lane(e))

    def far_product(start):
        for k in range(1, slots):
            row = (k - 1) * ghosts + start
            totals = [None] * comps
            for e in range(comps):
                term = halo_pulled[row : row + CHUNK, lane(e)]
                for c in range(comps):
                    more = mixing[k, e, c] * term
                    totals[c] = more if totals[c] is None else totals[c] + more
            for c in range(comps):
                far_mixed[c * ghosts + start : c * ghosts + start + CHUNK, lane(k - 1)] = totals[
                    c
                ].astype(BF16)
        left = jnp.concatenate(
            [far_mixed[c * ghosts + start : c * ghosts + start + CHUNK] for c in range(comps)], axis=0
        )
        right = jnp.concatenate([lift[k] for k in range(1, slots)], axis=0)
        return matmul(left, right)

    def ship_reverse(j, start, product):
        packets = product.astype(BF16)
        for d in range(start // halo, (start + CHUNK) // halo):
            for c in range(comps):
                row = c * CHUNK + d * halo - start
                rev_out[j, d, :, lane(c)] = packets[row : row + halo]

            @pl.when(exists(p - OFFSETS[d]))
            def _():
                rev_copy(j, d, p - OFFSETS[d]).start()

    def send_reverse(j):
        halo_pulled[...] = matmul(far_t[...], split[...])
        for start in FAR_HALF_FIRST:
            ship_reverse(j, start, far_product(start))

    def reverse_ahead():
        split_field(slope)
        gain[...] = matmul(pick_wide[:, : 2 * blocks], split[...])
        split_field(base)
        halo_pulled[...] = matmul(far_t[...], split[...])
        for start in FAR_HALF_FIRST:
            product = far_product(start)
            for c in range(comps):
                row = c * ghosts + start
                ahead[row : row + CHUNK] = product[c * CHUNK : (c + 1) * CHUNK]

    def send_ahead(j):
        for c in range(comps):
            back = jnp.concatenate([rev_in[j - 1, d, :, lane(c)] for d in range(4)], axis=0)
            in_halves(gain[:, lane(c)] * back.astype(F32), back_split, lane(c))
        for start in FAR_HALF_FIRST:
            rows = [slice(k * ghosts + start, k * ghosts + start + CHUNK) for k in range(slots - 1)]
            left = jnp.concatenate([cross[some] for some in rows], axis=0)
            product = matmul(left, back_split[...])
            for k, some in enumerate(rows):
                halo_pulled[some] = product[k * CHUNK : (k + 1) * CHUNK]
            made = jnp.concatenate(
                [ahead[c * ghosts + start : c * ghosts + start + CHUNK] for c in range(comps)], axis=0
            )
            ship_reverse(j, start, made - far_product(start))

    def reverse_sum(n, field):
        by_cosine = jnp.zeros((8, nodes), F32)
        by_sine = jnp.zeros((8, nodes), F32)
        for e in range(comps):
            value = field[e]
            by_cosine += jnp.sum((value * sources[1, e]).reshape(blocks // 8, 8, nodes), axis=0)
            by_sine += jnp.sum((value * sources[0, e]).reshape(blocks // 8, 8, nodes), axis=0)
        both = cosines[pl.ds(n, 1), :] * by_cosine - sines[pl.ds(n, 1), :] * by_sine
        partial[pl.ds(n, 1), :] = jnp.sum(both, axis=0, keepdims=True)

    def reverse_near(n):
        pulled[...] = matmul(near_t[...], split[...])
        for k in range(slots):
            for start in range(0, blocks, CHUNK):
                some = slice(start, start + CHUNK)
                totals = [None] * comps
                for e in range(comps):
                    if k == 0:
                        term = metric[some, :] * adjoint[e, some, :]
                    else:
                        row = (k - 1) * blocks + start
                        term = pulled[row : row + CHUNK, lane(e)]
                    for c in range(comps):
                        more = mixing[k, e, c] * term
                        totals[c] = more if totals[c] is None else totals[c] + more
                for c in range(comps):
                    mixed[c * blocks + start : c * blocks + start + CHUNK, lane(k)] = totals[c].astype(
                        BF16
                    )
        right = jnp.concatenate([lift[k] for k in range(slots)], axis=0)
        pushed = matmul(mixed[...], right)
        inner = jnp.where(n > 0, 1.0, 0.0).astype(F32)
        for c in range(comps):
            state = states[n, c]
            bent = jnp.tanh(state)
            fall = STEP_SIZE * (1.0 - bent * bent)
            slope[c] = fall
            grown = adjoint[c] + inner * (weight[c] * state)
            base[c] = grown - fall * pushed[c * blocks : (c + 1) * blocks]

    def reverse_wait(j):
        for d, offset in enumerate(OFFSETS):

            @pl.when(exists(p + offset))
            def _():
                rev_copy(j, d, p).wait_recv()

    def reverse_far(j):
        ghost = jnp.concatenate([rev_in[j, d] for d in range(4)], axis=0)
        arrived = matmul(pick_t[...], ghost)
        for c in range(comps):
            adjoint[c] = base[c] - slope[c] * arrived[:, lane(c)]

    def send_bend():
        for e in range(comps):
            bent = jnp.tanh(states[1, e])
            turning = cosines[0:1, :] * sources[1, e] - sines[0:1, :] * sources[0, e]
            squashed[:, lane(e)] = (STEP_SIZE * (1.0 - bent * bent) * turning).astype(BF16)
        packets = matmul(pick[...].astype(BF16), squashed[...]).astype(BF16)
        for d, offset in enumerate(OFFSETS):
            bend_out[d] = packets[d * halo : (d + 1) * halo]

            @pl.when(exists(p + offset))
            def _():
                bend_copy(d, p + offset).start()

        for d, offset in enumerate(OFFSETS):

            @pl.when(exists(p - offset))
            def _():
                bend_copy(d, p).wait_recv()

        bend_pass.start()

    def last_sum(j):
        reverse_sum(0, base)
        bend_pass.wait_recv()
        sent = jnp.zeros((halo, nodes), F32)
        for d in range(4):
            both = rev_out[j, d].astype(F32) * bend_there[d].astype(F32)
            for c in range(comps):
                sent += both[:, lane(c)]
        partial[0:1, :] = partial[0:1, :] - jnp.sum(sent, axis=0, keepdims=True)

    norm = math.sqrt(comps * nodes * blocks * n_space)

    def in_row(tile):
        sums = jnp.sum(tile, axis=1, keepdims=True) * (STEP_SIZE / norm)
        lanes = lax.broadcasted_iota(jnp.int32, (levels, nodes), 1)
        diagonal = lanes == lax.broadcasted_iota(jnp.int32, (levels, nodes), 0)
        return jnp.sum(jnp.where(diagonal, sums, 0.0), axis=0, keepdims=True)

    load_first.wait()
    squash(lambda c: states[first, c])
    near_peers = sum(exists(p + offset).astype(jnp.int32) for offset in OFFSETS)
    pl.semaphore_wait(barrier, near_peers + 1 + 2 * t)
    send_forward(0)

    @pl.when(t == 0)
    def _():
        state_copy(0).start()

    @pl.when(t == 1)
    def _():
        call(0, 1)

    load_lift.wait()
    for k in range(slots):
        lift_t[:, lane(k)] = lift[k].astype(F32).T.astype(BF16)
    pick_t[...] = pick[...].T.astype(BF16)
    load_pitch.wait()
    load_faces.wait()
    load_mixing.wait()
    row_of = lax.broadcasted_iota(jnp.int32, (levels, nodes), 0)
    angles = jnp.zeros((levels, nodes), F32)
    for n in range(levels):
        angles = jnp.where(row_of == n, pitch[n], angles)
    cosines[...] = jnp.cos(angles)
    sines[...] = jnp.sin(angles)
    row_at = lax.broadcasted_iota(jnp.int32, (blocks, blocks), 0)
    for k in range(1, slots):
        chosen = jnp.where(faces[k - 1 : k, :] == row_at, 1.0, 0.0)
        near[(k - 1) * blocks : k * blocks, :] = chosen.T.astype(BF16)
        turned = chosen.astype(BF16)
        near_t[(k - 1) * blocks : k * blocks, :blocks] = turned
        near_t[(k - 1) * blocks : k * blocks, blocks:] = turned
    slot_at = lax.rem(row_at, ghosts)
    for pair in range(2):
        upper = faces[2 * pair : 2 * pair + 1, :] - blocks
        lower = faces[2 * pair + 1 : 2 * pair + 2, :] - blocks
        wanted = jnp.where(row_at < ghosts, upper, lower)
        chosen = jnp.where(wanted == slot_at, 1.0, 0.0)
        far[:, pair * blocks : (pair + 1) * blocks] = chosen.T.astype(BF16)
        turned = chosen.astype(BF16)
        far_t[pair * blocks : (pair + 1) * blocks, :blocks] = turned
        far_t[pair * blocks : (pair + 1) * blocks, blocks:] = turned
    wide_pick = pick[...].astype(BF16)
    for part in range(3):
        pick_wide[:, part * blocks : (part + 1) * blocks] = wide_pick
    far_pick[...] = matmul(wide_pick, far[...]).astype(BF16)
    crossed = matmul(far_t[:, :blocks], pick_t[...]).astype(BF16)
    cross[...] = jnp.concatenate([crossed, crossed], axis=1)
    load_metric.wait()
    in_thirds(STEP_SIZE * metric[...], lane(0))
    picked_scale[...] = matmul(pick_wide[...], thirds[:, lane(0)])
    load_sources.wait()
    last = half - 2 + t

    def forward_level(i, carry):
        forward_near(i)
        forward_ahead()

        @pl.when(i > 0)
        def _():
            fwd_sent(i - 1)

        forward_far(i)

        @pl.when(i < last)
        def _():
            send_picked(i + 1)

        forward_end(i)

        @pl.when(i < last)
        def _():
            squash(lambda c: states[first + i + 1, c])

        @pl.when(t == 0)
        def _():
            state_copy(i + 1).start()

        return carry

    lax.fori_loop(0, half - 1 + t, forward_level, 0)

    load_weight.wait()
    load_end.wait()

    @pl.when(t == 0)
    def _():
        send_bend()

    @pl.when(t == 1)
    def _():
        pl.semaphore_wait(hello.at[0], 2)
        call(1, 2)
        for e in range(comps):
            adjoint[e] = adjoint[e] + weight[e] * states[levels, e]
        split_field(adjoint)
        send_reverse(0)

        def reverse_level(j, carry):
            n = levels - 1 - j

            @pl.when(n < half)
            def _():
                state_copy(n).wait_recv()

            reverse_sum(n, adjoint)
            reverse_near(n)
            reverse_ahead()

            @pl.when(j > 0)
            def _():
                rev_sent(j - 1)

            reverse_wait(j)
            send_ahead(j + 1)
            reverse_far(j)
            split_field(adjoint)

            @pl.when(n == half)
            def _():
                kept[...] = adjoint[...]
                keep_copy.start()

            return carry

        lax.fori_loop(0, levels - 2, reverse_level, 0)
        state_copy(1).wait_recv()
        reverse_sum(1, adjoint)
        reverse_near(1)
        pl.semaphore_wait(hello.at[1], 2)
        call(2, 2)
        last_sum(levels - 2)
        plane_parts[spot] = partial[...]
        for r in range(1, plane):
            plane_copy(r).start()
        reverse_ahead()
        rev_sent(levels - 3)
        reverse_wait(levels - 2)
        send_ahead(levels - 1)
        reverse_far(levels - 2)
        split_field(adjoint)
        pl.semaphore_wait(hello.at[2], 2)
        all_parts(plane_parts, plane - 1, plane_send, plane_recv).wait_recv()
        total = plane_parts[0]
        for s in range(1, plane):
            total = total + plane_parts[s]
        row = in_row(total)
        plane_sum[...] = row
        layer_parts[layer] = row
        for r in range(layers):
            layer_copy(r, 0).start()
            if r > 0:
                layer_copy(r, 1).start()
        state_copy(0).wait_recv()
        reverse_near(0)
        rev_sent(levels - 2)
        reverse_wait(levels - 1)
        reverse_far(levels - 1)
        end_copy.start()

    fwd_sent(last)

    @pl.when(t == 0)
    def _():
        for i in range(half):
            state_copy(i).wait_send()
        for d, offset in enumerate(OFFSETS):

            @pl.when(exists(p + offset))
            def _():
                bend_copy(d, p).wait_send()

        bend_pass.wait_send()

    @pl.when(t == 1)
    def _():
        rev_sent(levels - 1)
        keep_copy.wait()
        all_parts(plane_parts, plane - 1, plane_send, plane_recv).wait_send()
        all_parts(layer_parts, 2 * layers - 1, layer_send, layer_recv).wait_send()

    @pl.when(t == 0)
    def _():
        all_parts(layer_parts, layers, layer_send, layer_recv).wait_recv()

    @pl.when(t == 1)
    def _():
        all_parts(layer_parts, layers - 1, layer_send, layer_recv).wait_recv()

    total = layer_parts[0]
    for s in range(1, layers):
        total = total + layer_parts[s]
    grads_row[...] = total
    give_sums = pltpu.make_async_copy(grads_row, grads, out_sem.at[1])
    give_sums.start()

    @pl.when(t == 0)
    def _():
        end_copy.wait_recv()

    @pl.when(t == 1)
    def _():
        end_copy.wait_send()

    give_sums.wait()


def deliver(found, row, bounds, grads, held, sums, sums_out, sem):
    comps = held.shape[0]
    into = [pltpu.make_async_copy(found.at[0, c], held.at[c], sem.at[0, c]) for c in range(comps)]
    outof = [pltpu.make_async_copy(held.at[c], bounds.at[0, c], sem.at[1, c]) for c in range(comps)]
    row_in = pltpu.make_async_copy(row, sums, sem.at[0, comps])
    row_out = pltpu.make_async_copy(sums_out, grads, sem.at[1, comps])
    row_in.start()
    for copy in into:
        copy.start()
    row_in.wait()
    sums_out[...] = sums[0, : sums_out.shape[0]]
    row_out.start()
    for arrive, leave in zip(into, outof):
        arrive.wait()
        leave.start()
    row_out.wait()
    for leave in outof:
        leave.wait()


def solution(mesh):
    n_space = mesh.shape["space"]
    plane = 16 if n_space % 16 == 0 else 4

    def shards(
        checkpoints, sources, pitch, metric, obj_weight, adjoint_end, lift, mixing, faces, send_idx
    ):
        comps, blocks, nodes = obj_weight.shape
        slots = lift.shape[0]
        levels = pitch.shape[0]
        half = levels // 2
        halo = send_idx.shape[2]
        ghosts = 4 * halo
        wide = comps * nodes
        links = slots - 1
        layers = n_space // plane
        vmem = pltpu.VMEM
        dma = pltpu.SemaphoreType.DMA
        field = (comps, blocks, nodes)
        smem = pltpu.SMEM
        scratch = [
            smem((levels,), F32),
            smem(mixing.shape, F32),
            vmem((links, blocks), jnp.int32),
            smem(send_idx.shape, jnp.int32),
            vmem((1, nodes), F32),
            vmem((levels + 1, *field), F32),
            vmem((2, *field), F32),
            vmem((blocks, nodes), F32),
            vmem(field, F32),
            vmem(field, F32),
            vmem(field, F32),
            vmem((slots, nodes, nodes), BF16),
            vmem((nodes, slots * nodes), BF16),
            vmem((levels, nodes), F32),
            vmem((levels, nodes), F32),
            vmem((ghosts, blocks), F32),
            vmem((blocks, ghosts), BF16),
            vmem((links * blocks, blocks), BF16),
            vmem((links * blocks, 2 * blocks), BF16),
            vmem((blocks, links * ghosts), BF16),
            vmem((links * ghosts, 2 * blocks), BF16),
            vmem((ghosts, links * ghosts), BF16),
            vmem((links * ghosts, 2 * ghosts), BF16),
            vmem((ghosts, 3 * blocks), BF16),
            vmem((3 * blocks, wide), BF16),
            vmem((ghosts, wide), F32),
            vmem((ghosts, nodes), F32),
            vmem((ghosts, wide), F32),
            vmem((2 * ghosts, wide), BF16),
            vmem((comps * ghosts, nodes), F32),
            vmem((blocks, wide), BF16),
            vmem((links * blocks, wide), BF16),
            vmem((slots, comps * blocks, nodes), F32),
            vmem(field, F32),
            vmem(field, F32),
            vmem((comps * ghosts, links * nodes), F32),
            vmem((links * ghosts, wide), BF16),
            vmem((2 * blocks, wide), BF16),
            vmem((links * blocks, wide), F32),
            vmem((links * ghosts, wide), F32),
            vmem((comps * blocks, slots * nodes), BF16),
            vmem((comps * ghosts, links * nodes), BF16),
            vmem((half, 4, halo, wide), BF16),
            vmem((half, 4, halo, wide), BF16),
            vmem((levels, 4, halo, wide), BF16),
            vmem((levels, 4, halo, wide), BF16),
            vmem((4, halo, wide), BF16),
            vmem((4, halo, wide), BF16),
            vmem((4, halo, wide), BF16),
            vmem((levels, nodes), F32),
            vmem((plane, levels, nodes), F32),
            vmem((1, nodes), F32),
            vmem((2 * layers, 1, nodes), F32),
            dma((10,)),
            dma((2, 4)),
            dma((2, 4)),
            dma((2, 4)),
            dma((2, 4)),
            dma((4,)),
            dma((4,)),
            dma((2,)),
            dma((half,)),
            dma((half,)),
            dma,
            dma,
            dma,
            dma,
            dma((2,)),
            dma((2,)),
            pltpu.SemaphoreType.REGULAR((3,)),
        ]
        anywhere = pl.BlockSpec(memory_space=pl.ANY)
        results, sums = pl.pallas_call(
            functools.partial(sweep, n_space, plane),
            out_shape=(
                jax.ShapeDtypeStruct((1, *field), F32),
                jax.ShapeDtypeStruct((1, nodes), F32),
            ),
            in_specs=[pl.BlockSpec(memory_space=pltpu.HBM)] * 10,
            out_specs=(anywhere, anywhere),
            scratch_shapes=scratch,
            compiler_params=pltpu.CompilerParams(
                collective_id=0, has_side_effects=True, vmem_limit_bytes=67043328
            ),
            name="adjoint_window",
        )(checkpoints, sources, pitch, metric, obj_weight, adjoint_end, lift, mixing, faces.T, send_idx)
        return pl.pallas_call(
            deliver,
            out_shape=(
                jax.ShapeDtypeStruct((1, *field), F32),
                jax.ShapeDtypeStruct((levels,), F32),
            ),
            in_specs=[anywhere, anywhere],
            out_specs=(anywhere, anywhere),
            scratch_shapes=[
                vmem(field, F32),
                vmem((1, nodes), F32),
                vmem((levels,), F32),
                dma((2, comps + 1)),
            ],
            compiler_params=pltpu.CompilerParams(vmem_limit_bytes=67043328),
            name="deliver",
        )(results, sums)

    return jax.shard_map(
        shards,
        mesh=mesh,
        in_specs=(
            P("tm", None, "space", None),
            P(None, None, "space", None),
            P(),
            P("space", None),
            P(None, "space", None),
            P(None, "space", None),
            P(),
            P(),
            P("space", None),
            P("space", None, None),
        ),
        out_specs=(P("tm", None, "space", None), P()),
        check_vma=False,
    )
```

```python
import functools
import math

import jax
import jax.numpy as jnp
from jax import lax
from jax.experimental import pallas as pl
from jax.experimental.pallas import tpu as pltpu
from jax.sharding import PartitionSpec as P

OFFSETS = (1, -1, 2, -2)
FARTHEST_FIRST = (2, 3, 0, 1)
STEP_SIZE = 0.5
MESH = pl.DeviceIdType.MESH
F32, BF16 = jnp.float32, jnp.bfloat16
CHUNK = 32
FAR_HALF_FIRST = (32, 0)


def matmul(left, right):
    return jnp.dot(left, right, preferred_element_type=F32)


def parity(level):
    return level % 2 if isinstance(level, int) else lax.rem(level, 2)


def sweep(
    n_space,
    plane,
    checkpoint_in,
    sources_in,
    pitch_in,
    metric_in,
    weight_in,
    end_in,
    lift_in,
    mixing_in,
    faces_in,
    send_idx_in,
    bounds,
    grads,
    pitch,
    mixing,
    faces,
    send_idx,
    grads_row,
    states,
    sources,
    metric,
    weight,
    adjoint,
    kept,
    lift,
    lift_t,
    cosines,
    sines,
    pick,
    pick_t,
    near,
    near_t,
    far,
    far_t,
    far_pick,
    cross,
    pick_wide,
    thirds,
    picked,
    picked_scale,
    gain,
    back_split,
    ahead,
    squashed,
    gathered,
    lifted,
    base,
    slope,
    halo_lifted,
    halo_mixed,
    split,
    pulled,
    halo_pulled,
    mixed,
    far_mixed,
    fwd_out,
    fwd_in,
    rev_out,
    rev_in,
    bend_out,
    bend_in,
    bend_there,
    partial,
    plane_parts,
    plane_sum,
    layer_parts,
    in_sem,
    fwd_send,
    fwd_recv,
    rev_send,
    rev_recv,
    bend_send,
    bend_recv,
    bend_sem,
    state_send,
    state_recv,
    plane_send,
    plane_recv,
    layer_send,
    layer_recv,
    end_sem,
    out_sem,
    hello,
):
    comps, blocks, nodes = states.shape[1:]
    slots = lift.shape[0]
    halo = fwd_in.shape[2]
    ghosts = 4 * halo
    levels = pitch.shape[0]
    half = levels // 2
    layers = n_space // plane
    t = lax.axis_index("tm")
    p = lax.axis_index("space")
    spot = lax.rem(p, plane)
    layer = p // plane
    first = t * half

    hot = jnp.where(lax.rem(p, 4) >= 2, 1, 0)
    toward = 2 * hot - 1
    aim = (-2 * toward, -toward, 2 * toward, toward)
    pull_way = (2 + hot, hot, 3 - hot, 1 - hot)
    back_way = (3 - hot, 1 - hot, 2 + hot, hot)

    def exists(q):
        return jnp.logical_and(q >= 0, q < n_space)

    def lane(c):
        return slice(c * nodes, (c + 1) * nodes)

    (
        load_first,
        load_idx,
        load_mixing,
        load_faces,
        load_pitch,
        load_lift,
        load_metric,
        load_sources,
        load_weight,
        load_end,
    ) = loads = [
        pltpu.make_async_copy(checkpoint_in.at[0], states.at[first], in_sem.at[0]),
        pltpu.make_async_copy(send_idx_in, send_idx, in_sem.at[6]),
        pltpu.make_async_copy(mixing_in, mixing, in_sem.at[7]),
        pltpu.make_async_copy(faces_in, faces, in_sem.at[8]),
        pltpu.make_async_copy(pitch_in, pitch, in_sem.at[9]),
        pltpu.make_async_copy(lift_in, lift, in_sem.at[1]),
        pltpu.make_async_copy(metric_in, metric, in_sem.at[2]),
        pltpu.make_async_copy(sources_in, sources, in_sem.at[3]),
        pltpu.make_async_copy(weight_in, weight, in_sem.at[4]),
        pltpu.make_async_copy(end_in, adjoint, in_sem.at[5]),
    ]
    barrier = pltpu.get_barrier_semaphore()

    def greet(device):
        pl.semaphore_signal(barrier, inc=1, device_id=device, device_id_type=MESH)

    for offset in OFFSETS:

        @pl.when(exists(p + offset))
        def _():
            greet((t, p + offset))

    greet((1 - t, p))

    def in_layer(r):
        return (1, lax.rem(layer + r + layers, layers) * plane + spot)

    @pl.when(t == 1)
    def _():
        greet(in_layer(1))
        greet(in_layer(-1))

    def call(which, distance):
        for r in (distance, -distance):
            pl.semaphore_signal(
                hello.at[which], inc=1, device_id=in_layer(r), device_id_type=MESH
            )

    for load in loads:
        load.start()

    load_idx.wait()
    lane_of = lax.broadcasted_iota(jnp.int32, (1, blocks), 1)
    for d in range(4):
        for s in range(halo):
            row = d * halo + s
            pick[pl.ds(row, 1), :] = jnp.where(lane_of == send_idx[0, pull_way[d], s], 1.0, 0.0)

    for d, offset in enumerate(OFFSETS):

        @pl.when(jnp.logical_not(exists(p - offset)))
        def _():
            bend_in[d] = jnp.zeros(bend_in.shape[1:], BF16)
            for i in range(half):
                fwd_in[i, d] = jnp.zeros(fwd_in.shape[2:], BF16)

        @pl.when(jnp.logical_not(exists(p + offset)))
        def _():
            for i in range(levels):
                rev_in[i, d] = jnp.zeros(rev_in.shape[2:], BF16)

    def fwd_copy(i, d, device, q=0):
        return pltpu.make_async_remote_copy(
            src_ref=fwd_out.at[i, q],
            dst_ref=fwd_in.at[i, d],
            send_sem=fwd_send.at[parity(i), q],
            recv_sem=fwd_recv.at[parity(i), d],
            device_id=(t, device),
            device_id_type=MESH,
        )

    def rev_copy(i, d, device, q=0):
        return pltpu.make_async_remote_copy(
            src_ref=rev_out.at[i, q],
            dst_ref=rev_in.at[i, d],
            send_sem=rev_send.at[parity(i), q],
            recv_sem=rev_recv.at[parity(i), d],
            device_id=(t, device),
            device_id_type=MESH,
        )

    def bend_copy(d, device, q=0):
        return pltpu.make_async_remote_copy(
            src_ref=bend_out.at[q],
            dst_ref=bend_in.at[d],
            send_sem=bend_send.at[q],
            recv_sem=bend_recv.at[d],
            device_id=(t, device),
            device_id_type=MESH,
        )

    def state_copy(i):
        return pltpu.make_async_remote_copy(
            src_ref=states.at[i],
            dst_ref=states.at[i],
            send_sem=state_send.at[i],
            recv_sem=state_recv.at[i],
            device_id=(1 - t, p),
            device_id_type=MESH,
        )

    def plane_copy(r):
        return pltpu.make_async_remote_copy(
            src_ref=partial,
            dst_ref=plane_parts.at[spot],
            send_sem=plane_send,
            recv_sem=plane_recv,
            device_id=(1, layer * plane + lax.rem(spot + r, plane)),
            device_id_type=MESH,
        )

    def layer_copy(r, core):
        return pltpu.make_async_remote_copy(
            src_ref=plane_sum,
            dst_ref=layer_parts.at[layer],
            send_sem=layer_send,
            recv_sem=layer_recv,
            device_id=(core, lax.rem(layer + r, layers) * plane + spot),
            device_id_type=MESH,
        )

    bend_pass = pltpu.make_async_remote_copy(
        src_ref=bend_in,
        dst_ref=bend_there,
        send_sem=bend_sem.at[0],
        recv_sem=bend_sem.at[1],
        device_id=(1 - t, p),
        device_id_type=MESH,
    )
    def all_parts(parts, count, send_sem, recv_sem):
        return pltpu.make_async_remote_copy(
            src_ref=parts.at[pl.ds(0, count)],
            dst_ref=parts.at[pl.ds(0, count)],
            send_sem=send_sem,
            recv_sem=recv_sem,
            device_id=(1 - t, p),
            device_id_type=MESH,
        )

    end_copy = pltpu.make_async_remote_copy(
        src_ref=adjoint,
        dst_ref=bounds.at[0],
        send_sem=end_sem.at[0],
        recv_sem=end_sem.at[1],
        device_id=(1 - t, p),
        device_id_type=MESH,
    )
    keep_copy = pltpu.make_async_copy(kept, bounds.at[0], out_sem.at[0])

    def fwd_sent(i):
        for q in range(4):

            @pl.when(exists(p + aim[q]))
            def _():
                fwd_copy(i, pull_way[q], p, q).wait_send()

    def rev_sent(j):
        for q in range(4):

            @pl.when(exists(p + aim[q]))
            def _():
                rev_copy(j, back_way[q], p, q).wait_send()

    def in_halves(value, where, columns):
        rows = value.shape[0]
        high = value.astype(BF16)
        where[:rows, columns] = high
        where[rows:, columns] = (value - high.astype(F32)).astype(BF16)

    def in_thirds(value, columns):
        for part in range(3):
            high = value.astype(BF16)
            thirds[part * blocks : (part + 1) * blocks, columns] = high
            value = value - high.astype(F32)

    def squash(state):
        for c in range(comps):
            squashed[:, lane(c)] = jnp.tanh(state(c)).astype(BF16)

    def send_forward(i):
        packets = matmul(pick[...].astype(BF16), squashed[...]).astype(BF16)
        for q in FARTHEST_FIRST:
            fwd_out[i, q] = packets[q * halo : (q + 1) * halo]

            @pl.when(exists(p + aim[q]))
            def _():
                fwd_copy(i, pull_way[q], p + aim[q], q).start()

    def forward_near(i):
        gathered[...] = matmul(near[...], squashed[...]).astype(BF16)
        for k in range(slots):
            rows = squashed if k == 0 else gathered.at[pl.ds((k - 1) * blocks, blocks)]
            left = jnp.concatenate([rows[:, lane(c)] for c in range(comps)], axis=0)
            lifted[k] = matmul(left, lift_t[:, lane(k)])
        cosine = cosines[pl.ds(first + i, 1), :]
        sine = sines[pl.ds(first + i, 1), :]
        for start in range(0, blocks, CHUNK):
            some = slice(start, start + CHUNK)
            totals = [None] * comps
            for k in range(slots):
                for c in range(comps):
                    term = lifted[k, c * blocks + start : c * blocks + start + CHUNK, :]
                    for e in range(comps):
                        more = mixing[k, e, c] * term
                        totals[e] = more if totals[e] is None else totals[e] + more
            for e in range(comps):
                forcing = cosine * sources[0, e, some, :] + sine * sources[1, e, some, :]
                change = forcing - metric[some, :] * totals[e]
                base[e, some, :] = states[first + i, e, some, :] + STEP_SIZE * change

    def forward_far(i):
        for d, offset in enumerate(OFFSETS):

            @pl.when(exists(p - offset))
            def _():
                fwd_copy(i, d, p).wait_recv()

        ghost = jnp.concatenate([fwd_in[i, d] for d in range(4)], axis=0)
        left = jnp.concatenate([ghost[:, lane(c)] for c in range(comps)], axis=0)
        halo_lifted[...] = matmul(left, lift_t[:, nodes:])
        for k in range(1, slots):
            for start in range(0, ghosts, CHUNK):
                totals = [None] * comps
                for c in range(comps):
                    term = halo_lifted[c * ghosts + start : c * ghosts + start + CHUNK, lane(k - 1)]
                    for e in range(comps):
                        more = mixing[k, e, c] * term
                        totals[e] = more if totals[e] is None else totals[e] + more
                row = (k - 1) * ghosts + start
                for e in range(comps):
                    halo_mixed[row : row + CHUNK, lane(e)] = totals[e].astype(BF16)

    def forward_ahead():
        for e in range(comps):
            in_thirds(base[e], lane(e))
        picked[...] = matmul(pick_wide[...], thirds[...])

    def send_picked(i):
        wide_scale = jnp.concatenate([picked_scale[...]] * comps, axis=1)
        for start in FAR_HALF_FIRST:
            some = slice(start, start + CHUNK)
            change = matmul(far_pick[some], halo_mixed[...])
            packets = jnp.tanh(picked[some] - wide_scale[some] * change).astype(BF16)
            for q in range(start // halo, (start + CHUNK) // halo):
                fwd_out[i, q] = packets[q * halo - start : (q + 1) * halo - start]

                @pl.when(exists(p + aim[q]))
                def _():
                    fwd_copy(i, pull_way[q], p + aim[q], q).start()

    def forward_end(i):
        scale = STEP_SIZE * metric[...]
        arrived = matmul(far[...], halo_mixed[...])
        for e in range(comps):
            states[first + i + 1, e] = base[e] - scale * arrived[:, lane(e)]

    def split_field(field):
        for e in range(comps):
            in_halves(metric[...] * field[e], split, lane(e))

    def far_product(start):
        for k in range(1, slots):
            row = (k - 1) * ghosts + start
            totals = [None] * comps
            for e in range(comps):
                term = halo_pulled[row : row + CHUNK, lane(e)]
                for c in range(comps):
                    more = mixing[k, e, c] * term
                    totals[c] = more if totals[c] is None else totals[c] + more
            for c in range(comps):
                far_mixed[c * ghosts + start : c * ghosts + start + CHUNK, lane(k - 1)] = totals[
                    c
                ].astype(BF16)
        left = jnp.concatenate(
            [far_mixed[c * ghosts + start : c * ghosts + start + CHUNK] for c in range(comps)], axis=0
        )
        right = jnp.concatenate([lift[k] for k in range(1, slots)], axis=0)
        return matmul(left, right)

    def ship_reverse(j, start, product):
        packets = product.astype(BF16)
        for q in range(start // halo, (start + CHUNK) // halo):
            for c in range(comps):
                row = c * CHUNK + q * halo - start
                rev_out[j, q, :, lane(c)] = packets[row : row + halo]

            @pl.when(exists(p + aim[q]))
            def _():
                rev_copy(j, back_way[q], p + aim[q], q).start()

    def send_reverse(j):
        halo_pulled[...] = matmul(far_t[...], split[...])
        for start in FAR_HALF_FIRST:
            ship_reverse(j, start, far_product(start))

    def reverse_ahead():
        split_field(slope)
        gain[...] = matmul(pick_wide[:, : 2 * blocks], split[...])
        split_field(base)
        halo_pulled[...] = matmul(far_t[...], split[...])
        for start in FAR_HALF_FIRST:
            product = far_product(start)
            for c in range(comps):
                row = c * ghosts + start
                ahead[row : row + CHUNK] = product[c * CHUNK : (c + 1) * CHUNK]

    def send_ahead(j):
        for c in range(comps):
            back = jnp.concatenate([rev_in[j - 1, d, :, lane(c)] for d in pull_way], axis=0)
            in_halves(gain[:, lane(c)] * back.astype(F32), back_split, lane(c))
        for start in FAR_HALF_FIRST:
            rows = [slice(k * ghosts + start, k * ghosts + start + CHUNK) for k in range(slots - 1)]
            left = jnp.concatenate([cross[some] for some in rows], axis=0)
            product = matmul(left, back_split[...])
            for k, some in enumerate(rows):
                halo_pulled[some] = product[k * CHUNK : (k + 1) * CHUNK]
            made = jnp.concatenate(
                [ahead[c * ghosts + start : c * ghosts + start + CHUNK] for c in range(comps)], axis=0
            )
            ship_reverse(j, start, made - far_product(start))

    def reverse_sum(n, field):
        by_cosine = jnp.zeros((8, nodes), F32)
        by_sine = jnp.zeros((8, nodes), F32)
        for e in range(comps):
            value = field[e]
            by_cosine += jnp.sum((value * sources[1, e]).reshape(blocks // 8, 8, nodes), axis=0)
            by_sine += jnp.sum((value * sources[0, e]).reshape(blocks // 8, 8, nodes), axis=0)
        both = cosines[pl.ds(n, 1), :] * by_cosine - sines[pl.ds(n, 1), :] * by_sine
        partial[pl.ds(n, 1), :] = jnp.sum(both, axis=0, keepdims=True)

    def reverse_near(n):
        pulled[...] = matmul(near_t[...], split[...])
        for k in range(slots):
            for start in range(0, blocks, CHUNK):
                some = slice(start, start + CHUNK)
                totals = [None] * comps
                for e in range(comps):
                    if k == 0:
                        term = metric[some, :] * adjoint[e, some, :]
                    else:
                        row = (k - 1) * blocks + start
                        term = pulled[row : row + CHUNK, lane(e)]
                    for c in range(comps):
                        more = mixing[k, e, c] * term
                        totals[c] = more if totals[c] is None else totals[c] + more
                for c in range(comps):
                    mixed[c * blocks + start : c * blocks + start + CHUNK, lane(k)] = totals[c].astype(
                        BF16
                    )
        right = jnp.concatenate([lift[k] for k in range(slots)], axis=0)
        pushed = matmul(mixed[...], right)
        inner = jnp.where(n > 0, 1.0, 0.0).astype(F32)
        for c in range(comps):
            state = states[n, c]
            bent = jnp.tanh(state)
            fall = STEP_SIZE * (1.0 - bent * bent)
            slope[c] = fall
            grown = adjoint[c] + inner * (weight[c] * state)
            base[c] = grown - fall * pushed[c * blocks : (c + 1) * blocks]

    def reverse_wait(j):
        for d, offset in enumerate(OFFSETS):

            @pl.when(exists(p + offset))
            def _():
                rev_copy(j, d, p).wait_recv()

    def reverse_far(j):
        ghost = jnp.concatenate([rev_in[j, d] for d in pull_way], axis=0)
        arrived = matmul(pick_t[...], ghost)
        for c in range(comps):
            adjoint[c] = base[c] - slope[c] * arrived[:, lane(c)]

    def send_bend():
        for e in range(comps):
            bent = jnp.tanh(states[1, e])
            turning = cosines[0:1, :] * sources[1, e] - sines[0:1, :] * sources[0, e]
            squashed[:, lane(e)] = (STEP_SIZE * (1.0 - bent * bent) * turning).astype(BF16)
        packets = matmul(pick[...].astype(BF16), squashed[...]).astype(BF16)
        for q in range(4):
            bend_out[q] = packets[q * halo : (q + 1) * halo]

            @pl.when(exists(p + aim[q]))
            def _():
                bend_copy(pull_way[q], p + aim[q], q).start()

        for d, offset in enumerate(OFFSETS):

            @pl.when(exists(p - offset))
            def _():
                bend_copy(d, p).wait_recv()

        bend_pass.start()

    def last_sum(j):
        reverse_sum(0, base)
        bend_pass.wait_recv()
        sent = jnp.zeros((halo, nodes), F32)
        for d in range(4):
            both = rev_out[j, d].astype(F32) * bend_there[back_way[d]].astype(F32)
            for c in range(comps):
                sent += both[:, lane(c)]
        partial[0:1, :] = partial[0:1, :] - jnp.sum(sent, axis=0, keepdims=True)

    norm = math.sqrt(comps * nodes * blocks * n_space)

    def in_row(tile):
        sums = jnp.sum(tile, axis=1, keepdims=True) * (STEP_SIZE / norm)
        lanes = lax.broadcasted_iota(jnp.int32, (levels, nodes), 1)
        diagonal = lanes == lax.broadcasted_iota(jnp.int32, (levels, nodes), 0)
        return jnp.sum(jnp.where(diagonal, sums, 0.0), axis=0, keepdims=True)

    load_first.wait()
    squash(lambda c: states[first, c])
    near_peers = sum(exists(p + offset).astype(jnp.int32) for offset in OFFSETS)
    pl.semaphore_wait(barrier, near_peers + 1 + 2 * t)
    send_forward(0)

    @pl.when(t == 0)
    def _():
        state_copy(0).start()

    @pl.when(t == 1)
    def _():
        call(0, 1)

    load_lift.wait()
    for k in range(slots):
        lift_t[:, lane(k)] = lift[k].astype(F32).T.astype(BF16)
    pick_t[...] = pick[...].T.astype(BF16)
    load_pitch.wait()
    load_faces.wait()
    load_mixing.wait()
    row_of = lax.broadcasted_iota(jnp.int32, (levels, nodes), 0)
    angles = jnp.zeros((levels, nodes), F32)
    for n in range(levels):
        angles = jnp.where(row_of == n, pitch[n], angles)
    cosines[...] = jnp.cos(angles)
    sines[...] = jnp.sin(angles)
    row_at = lax.broadcasted_iota(jnp.int32, (blocks, blocks), 0)
    for k in range(1, slots):
        chosen = jnp.where(faces[k - 1 : k, :] == row_at, 1.0, 0.0)
        near[(k - 1) * blocks : k * blocks, :] = chosen.T.astype(BF16)
        turned = chosen.astype(BF16)
        near_t[(k - 1) * blocks : k * blocks, :blocks] = turned
        near_t[(k - 1) * blocks : k * blocks, blocks:] = turned
    slot_at = lax.rem(row_at, ghosts)
    group = slot_at // halo
    way = jnp.where(group == 0, back_way[0], back_way[1])
    way = jnp.where(group == 2, back_way[2], way)
    way = jnp.where(group == 3, back_way[3], way)
    sent_at = way * halo + lax.rem(slot_at, halo)
    for pair in range(2):
        upper = faces[2 * pair : 2 * pair + 1, :] - blocks
        lower = faces[2 * pair + 1 : 2 * pair + 2, :] - blocks
        wanted = jnp.where(row_at < ghosts, upper, lower)
        chosen = jnp.where(wanted == slot_at, 1.0, 0.0)
        far[:, pair * blocks : (pair + 1) * blocks] = chosen.T.astype(BF16)
        turned = jnp.where(wanted == sent_at, 1.0, 0.0).astype(BF16)
        far_t[pair * blocks : (pair + 1) * blocks, :blocks] = turned
        far_t[pair * blocks : (pair + 1) * blocks, blocks:] = turned
    wide_pick = pick[...].astype(BF16)
    for part in range(3):
        pick_wide[:, part * blocks : (part + 1) * blocks] = wide_pick
    far_pick[...] = matmul(wide_pick, far[...]).astype(BF16)
    crossed = matmul(far_t[:, :blocks], pick_t[...]).astype(BF16)
    cross[...] = jnp.concatenate([crossed, crossed], axis=1)
    load_metric.wait()
    in_thirds(STEP_SIZE * metric[...], lane(0))
    picked_scale[...] = matmul(pick_wide[...], thirds[:, lane(0)])
    load_sources.wait()
    last = half - 2 + t

    def forward_level(i, carry):
        forward_near(i)
        forward_ahead()

        @pl.when(i > 0)
        def _():
            fwd_sent(i - 1)

        forward_far(i)

        @pl.when(i < last)
        def _():
            send_picked(i + 1)

        forward_end(i)

        @pl.when(i < last)
        def _():
            squash(lambda c: states[first + i + 1, c])

        @pl.when(t == 0)
        def _():
            state_copy(i + 1).start()

        return carry

    lax.fori_loop(0, half - 1 + t, forward_level, 0)

    load_weight.wait()
    load_end.wait()

    @pl.when(t == 0)
    def _():
        send_bend()

    @pl.when(t == 1)
    def _():
        pl.semaphore_wait(hello.at[0], 2)
        call(1, 2)
        for e in range(comps):
            adjoint[e] = adjoint[e] + weight[e] * states[levels, e]
        split_field(adjoint)
        send_reverse(0)

        def reverse_level(j, carry):
            n = levels - 1 - j

            @pl.when(n < half)
            def _():
                state_copy(n).wait_recv()

            reverse_sum(n, adjoint)
            reverse_near(n)
            reverse_ahead()

            @pl.when(j > 0)
            def _():
                rev_sent(j - 1)

            reverse_wait(j)
            send_ahead(j + 1)
            reverse_far(j)
            split_field(adjoint)

            @pl.when(n == half)
            def _():
                kept[...] = adjoint[...]
                keep_copy.start()

            return carry

        lax.fori_loop(0, levels - 2, reverse_level, 0)
        state_copy(1).wait_recv()
        reverse_sum(1, adjoint)
        reverse_near(1)
        pl.semaphore_wait(hello.at[1], 2)
        call(2, 2)
        last_sum(levels - 2)
        plane_parts[spot] = partial[...]
        for r in range(1, plane):
            plane_copy(r).start()
        reverse_ahead()
        rev_sent(levels - 3)
        reverse_wait(levels - 2)
        send_ahead(levels - 1)
        reverse_far(levels - 2)
        split_field(adjoint)
        pl.semaphore_wait(hello.at[2], 2)
        all_parts(plane_parts, plane - 1, plane_send, plane_recv).wait_recv()
        total = plane_parts[0]
        for s in range(1, plane):
            total = total + plane_parts[s]
        row = in_row(total)
        plane_sum[...] = row
        layer_parts[layer] = row
        for r in range(layers):
            layer_copy(r, 0).start()
            if r > 0:
                layer_copy(r, 1).start()
        state_copy(0).wait_recv()
        reverse_near(0)
        rev_sent(levels - 2)
        reverse_wait(levels - 1)
        reverse_far(levels - 1)
        end_copy.start()

    fwd_sent(last)

    @pl.when(t == 0)
    def _():
        for i in range(half):
            state_copy(i).wait_send()
        for q in range(4):

            @pl.when(exists(p + aim[q]))
            def _():
                bend_copy(pull_way[q], p, q).wait_send()

        bend_pass.wait_send()

    @pl.when(t == 1)
    def _():
        rev_sent(levels - 1)
        keep_copy.wait()
        all_parts(plane_parts, plane - 1, plane_send, plane_recv).wait_send()
        all_parts(layer_parts, 2 * layers - 1, layer_send, layer_recv).wait_send()

    @pl.when(t == 0)
    def _():
        all_parts(layer_parts, layers, layer_send, layer_recv).wait_recv()

    @pl.when(t == 1)
    def _():
        all_parts(layer_parts, layers - 1, layer_send, layer_recv).wait_recv()

    total = layer_parts[0]
    for s in range(1, layers):
        total = total + layer_parts[s]
    grads_row[...] = total
    give_sums = pltpu.make_async_copy(grads_row, grads, out_sem.at[1])
    give_sums.start()

    @pl.when(t == 0)
    def _():
        end_copy.wait_recv()

    @pl.when(t == 1)
    def _():
        end_copy.wait_send()

    give_sums.wait()


def deliver(found, row, bounds, grads, held, sums, sums_out, sem):
    comps = held.shape[0]
    into = [pltpu.make_async_copy(found.at[0, c], held.at[c], sem.at[0, c]) for c in range(comps)]
    outof = [pltpu.make_async_copy(held.at[c], bounds.at[0, c], sem.at[1, c]) for c in range(comps)]
    row_in = pltpu.make_async_copy(row, sums, sem.at[0, comps])
    row_out = pltpu.make_async_copy(sums_out, grads, sem.at[1, comps])
    row_in.start()
    for copy in into:
        copy.start()
    row_in.wait()
    sums_out[...] = sums[0, : sums_out.shape[0]]
    row_out.start()
    for arrive, leave in zip(into, outof):
        arrive.wait()
        leave.start()
    row_out.wait()
    for leave in outof:
        leave.wait()


def solution(mesh):
    n_space = mesh.shape["space"]
    plane = 16 if n_space % 16 == 0 else 4

    def shards(
        checkpoints, sources, pitch, metric, obj_weight, adjoint_end, lift, mixing, faces, send_idx
    ):
        comps, blocks, nodes = obj_weight.shape
        slots = lift.shape[0]
        levels = pitch.shape[0]
        half = levels // 2
        halo = send_idx.shape[2]
        ghosts = 4 * halo
        wide = comps * nodes
        links = slots - 1
        layers = n_space // plane
        vmem = pltpu.VMEM
        dma = pltpu.SemaphoreType.DMA
        field = (comps, blocks, nodes)
        smem = pltpu.SMEM
        scratch = [
            smem((levels,), F32),
            smem(mixing.shape, F32),
            vmem((links, blocks), jnp.int32),
            smem(send_idx.shape, jnp.int32),
            vmem((1, nodes), F32),
            vmem((levels + 1, *field), F32),
            vmem((2, *field), F32),
            vmem((blocks, nodes), F32),
            vmem(field, F32),
            vmem(field, F32),
            vmem(field, F32),
            vmem((slots, nodes, nodes), BF16),
            vmem((nodes, slots * nodes), BF16),
            vmem((levels, nodes), F32),
            vmem((levels, nodes), F32),
            vmem((ghosts, blocks), F32),
            vmem((blocks, ghosts), BF16),
            vmem((links * blocks, blocks), BF16),
            vmem((links * blocks, 2 * blocks), BF16),
            vmem((blocks, links * ghosts), BF16),
            vmem((links * ghosts, 2 * blocks), BF16),
            vmem((ghosts, links * ghosts), BF16),
            vmem((links * ghosts, 2 * ghosts), BF16),
            vmem((ghosts, 3 * blocks), BF16),
            vmem((3 * blocks, wide), BF16),
            vmem((ghosts, wide), F32),
            vmem((ghosts, nodes), F32),
            vmem((ghosts, wide), F32),
            vmem((2 * ghosts, wide), BF16),
            vmem((comps * ghosts, nodes), F32),
            vmem((blocks, wide), BF16),
            vmem((links * blocks, wide), BF16),
            vmem((slots, comps * blocks, nodes), F32),
            vmem(field, F32),
            vmem(field, F32),
            vmem((comps * ghosts, links * nodes), F32),
            vmem((links * ghosts, wide), BF16),
            vmem((2 * blocks, wide), BF16),
            vmem((links * blocks, wide), F32),
            vmem((links * ghosts, wide), F32),
            vmem((comps * blocks, slots * nodes), BF16),
            vmem((comps * ghosts, links * nodes), BF16),
            vmem((half, 4, halo, wide), BF16),
            vmem((half, 4, halo, wide), BF16),
            vmem((levels, 4, halo, wide), BF16),
            vmem((levels, 4, halo, wide), BF16),
            vmem((4, halo, wide), BF16),
            vmem((4, halo, wide), BF16),
            vmem((4, halo, wide), BF16),
            vmem((levels, nodes), F32),
            vmem((plane, levels, nodes), F32),
            vmem((1, nodes), F32),
            vmem((2 * layers, 1, nodes), F32),
            dma((10,)),
            dma((2, 4)),
            dma((2, 4)),
            dma((2, 4)),
            dma((2, 4)),
            dma((4,)),
            dma((4,)),
            dma((2,)),
            dma((half,)),
            dma((half,)),
            dma,
            dma,
            dma,
            dma,
            dma((2,)),
            dma((2,)),
            pltpu.SemaphoreType.REGULAR((3,)),
        ]
        anywhere = pl.BlockSpec(memory_space=pl.ANY)
        results, sums = pl.pallas_call(
            functools.partial(sweep, n_space, plane),
            out_shape=(
                jax.ShapeDtypeStruct((1, *field), F32),
                jax.ShapeDtypeStruct((1, nodes), F32),
            ),
            in_specs=[pl.BlockSpec(memory_space=pltpu.HBM)] * 10,
            out_specs=(anywhere, anywhere),
            scratch_shapes=scratch,
            compiler_params=pltpu.CompilerParams(
                collective_id=0, has_side_effects=True, vmem_limit_bytes=67043328
            ),
            name="adjoint_window",
        )(checkpoints, sources, pitch, metric, obj_weight, adjoint_end, lift, mixing, faces.T, send_idx)
        return pl.pallas_call(
            deliver,
            out_shape=(
                jax.ShapeDtypeStruct((1, *field), F32),
                jax.ShapeDtypeStruct((levels,), F32),
            ),
            in_specs=[anywhere, anywhere],
            out_specs=(anywhere, anywhere),
            scratch_shapes=[
                vmem(field, F32),
                vmem((1, nodes), F32),
                vmem((levels,), F32),
                dma((2, comps + 1)),
            ],
            compiler_params=pltpu.CompilerParams(vmem_limit_bytes=67043328),
            name="deliver",
        )(results, sums)

    return jax.shard_map(
        shards,
        mesh=mesh,
        in_specs=(
            P("tm", None, "space", None),
            P(None, None, "space", None),
            P(),
            P("space", None),
            P(None, "space", None),
            P(None, "space", None),
            P(),
            P(),
            P("space", None),
            P("space", None, None),
        ),
        out_specs=(P("tm", None, "space", None), P()),
        check_vma=False,
    )
```

```python
import functools
import math

import jax
import jax.numpy as jnp
from jax import lax
from jax.experimental import pallas as pl
from jax.experimental.pallas import tpu as pltpu
from jax.sharding import PartitionSpec as P

OFFSETS = (1, -1, 2, -2)
FARTHEST_FIRST = (2, 3, 0, 1)
STEP_SIZE = 0.5
MESH = pl.DeviceIdType.MESH
F32, BF16 = jnp.float32, jnp.bfloat16
CHUNK = 32
FAR_HALF_FIRST = (32, 0)


def matmul(left, right):
    return jnp.dot(left, right, preferred_element_type=F32)


def parity(level):
    return level % 2 if isinstance(level, int) else lax.rem(level, 2)


def sweep(
    n_space,
    plane,
    checkpoint_in,
    sources_in,
    pitch_in,
    metric_in,
    weight_in,
    end_in,
    lift_in,
    mixing_in,
    faces_in,
    send_idx_in,
    bounds,
    grads,
    pitch,
    mixing,
    faces,
    send_idx,
    grads_row,
    states,
    sources,
    metric,
    weight,
    adjoint,
    kept,
    lift,
    lift_t,
    cosines,
    sines,
    pick,
    pick_t,
    near,
    near_t,
    far,
    far_t,
    far_pick,
    cross,
    pick_wide,
    thirds,
    picked,
    picked_scale,
    gain,
    back_split,
    ahead,
    squashed,
    gathered,
    lifted,
    base,
    slope,
    halo_lifted,
    halo_mixed,
    split,
    pulled,
    halo_pulled,
    mixed,
    far_mixed,
    fwd_out,
    fwd_in,
    rev_out,
    rev_in,
    bend_out,
    bend_in,
    bend_there,
    partial,
    plane_row,
    plane_parts,
    plane_sum,
    layer_parts,
    in_sem,
    fwd_send,
    fwd_recv,
    rev_send,
    rev_recv,
    bend_send,
    bend_recv,
    bend_sem,
    state_send,
    state_recv,
    plane_send,
    plane_recv,
    layer_send,
    layer_recv,
    end_sem,
    out_sem,
    hello,
):
    comps, blocks, nodes = states.shape[1:]
    slots = lift.shape[0]
    halo = fwd_in.shape[2]
    ghosts = 4 * halo
    levels = pitch.shape[0]
    half = levels // 2
    layers = n_space // plane
    t = lax.axis_index("tm")
    p = lax.axis_index("space")
    spot = lax.rem(p, plane)
    layer = p // plane
    first = t * half

    hot = jnp.where(lax.rem(p, 4) >= 2, 1, 0)
    toward = 2 * hot - 1
    aim = (-2 * toward, -toward, 2 * toward, toward)
    pull_way = (2 + hot, hot, 3 - hot, 1 - hot)
    back_way = (3 - hot, 1 - hot, 2 + hot, hot)

    def exists(q):
        return jnp.logical_and(q >= 0, q < n_space)

    def lane(c):
        return slice(c * nodes, (c + 1) * nodes)

    (
        load_first,
        load_idx,
        load_mixing,
        load_faces,
        load_pitch,
        load_lift,
        load_metric,
        load_sources,
        load_weight,
        load_end,
    ) = loads = [
        pltpu.make_async_copy(checkpoint_in.at[0], states.at[first], in_sem.at[0]),
        pltpu.make_async_copy(send_idx_in, send_idx, in_sem.at[6]),
        pltpu.make_async_copy(mixing_in, mixing, in_sem.at[7]),
        pltpu.make_async_copy(faces_in, faces, in_sem.at[8]),
        pltpu.make_async_copy(pitch_in, pitch, in_sem.at[9]),
        pltpu.make_async_copy(lift_in, lift, in_sem.at[1]),
        pltpu.make_async_copy(metric_in, metric, in_sem.at[2]),
        pltpu.make_async_copy(sources_in, sources, in_sem.at[3]),
        pltpu.make_async_copy(weight_in, weight, in_sem.at[4]),
        pltpu.make_async_copy(end_in, adjoint, in_sem.at[5]),
    ]
    barrier = pltpu.get_barrier_semaphore()

    def greet(device):
        pl.semaphore_signal(barrier, inc=1, device_id=device, device_id_type=MESH)

    for offset in OFFSETS:

        @pl.when(exists(p + offset))
        def _():
            greet((t, p + offset))

    greet((1 - t, p))

    def in_layer(r):
        return (1, lax.rem(layer + r + layers, layers) * plane + spot)

    @pl.when(t == 1)
    def _():
        greet(in_layer(1))
        greet(in_layer(-1))

    def call(which, distance):
        for r in (distance, -distance):
            pl.semaphore_signal(
                hello.at[which], inc=1, device_id=in_layer(r), device_id_type=MESH
            )

    for load in loads:
        load.start()

    load_idx.wait()
    lane_of = lax.broadcasted_iota(jnp.int32, (1, blocks), 1)
    for d in range(4):
        for s in range(halo):
            row = d * halo + s
            pick[pl.ds(row, 1), :] = jnp.where(lane_of == send_idx[0, pull_way[d], s], 1.0, 0.0)

    for d, offset in enumerate(OFFSETS):

        @pl.when(jnp.logical_not(exists(p - offset)))
        def _():
            bend_in[d] = jnp.zeros(bend_in.shape[1:], BF16)
            for i in range(half):
                fwd_in[i, d] = jnp.zeros(fwd_in.shape[2:], BF16)

        @pl.when(jnp.logical_not(exists(p + offset)))
        def _():
            for i in range(levels):
                rev_in[i, d] = jnp.zeros(rev_in.shape[2:], BF16)

    def fwd_copy(i, d, device, q=0):
        return pltpu.make_async_remote_copy(
            src_ref=fwd_out.at[i, q],
            dst_ref=fwd_in.at[i, d],
            send_sem=fwd_send.at[parity(i), q],
            recv_sem=fwd_recv.at[parity(i), d],
            device_id=(t, device),
            device_id_type=MESH,
        )

    def rev_copy(i, d, device, q=0):
        return pltpu.make_async_remote_copy(
            src_ref=rev_out.at[i, q],
            dst_ref=rev_in.at[i, d],
            send_sem=rev_send.at[parity(i), q],
            recv_sem=rev_recv.at[parity(i), d],
            device_id=(t, device),
            device_id_type=MESH,
        )

    def bend_copy(d, device, q=0):
        return pltpu.make_async_remote_copy(
            src_ref=bend_out.at[q],
            dst_ref=bend_in.at[d],
            send_sem=bend_send.at[q],
            recv_sem=bend_recv.at[d],
            device_id=(t, device),
            device_id_type=MESH,
        )

    def state_copy(i):
        return pltpu.make_async_remote_copy(
            src_ref=states.at[i],
            dst_ref=states.at[i],
            send_sem=state_send.at[i],
            recv_sem=state_recv.at[i],
            device_id=(1 - t, p),
            device_id_type=MESH,
        )

    def plane_copy(r):
        return pltpu.make_async_remote_copy(
            src_ref=plane_row,
            dst_ref=plane_parts.at[spot],
            send_sem=plane_send,
            recv_sem=plane_recv,
            device_id=(1, layer * plane + lax.rem(spot + r, plane)),
            device_id_type=MESH,
        )

    def layer_copy(r, core):
        return pltpu.make_async_remote_copy(
            src_ref=plane_sum,
            dst_ref=layer_parts.at[layer],
            send_sem=layer_send,
            recv_sem=layer_recv,
            device_id=(core, lax.rem(layer + r, layers) * plane + spot),
            device_id_type=MESH,
        )

    bend_pass = pltpu.make_async_remote_copy(
        src_ref=bend_in,
        dst_ref=bend_there,
        send_sem=bend_sem.at[0],
        recv_sem=bend_sem.at[1],
        device_id=(1 - t, p),
        device_id_type=MESH,
    )
    def all_parts(parts, count, send_sem, recv_sem):
        return pltpu.make_async_remote_copy(
            src_ref=parts.at[pl.ds(0, count)],
            dst_ref=parts.at[pl.ds(0, count)],
            send_sem=send_sem,
            recv_sem=recv_sem,
            device_id=(1 - t, p),
            device_id_type=MESH,
        )

    end_copy = pltpu.make_async_remote_copy(
        src_ref=adjoint,
        dst_ref=bounds.at[0],
        send_sem=end_sem.at[0],
        recv_sem=end_sem.at[1],
        device_id=(1 - t, p),
        device_id_type=MESH,
    )
    keep_copy = pltpu.make_async_copy(kept, bounds.at[0], out_sem.at[0])

    def fwd_sent(i):
        for q in range(4):

            @pl.when(exists(p + aim[q]))
            def _():
                fwd_copy(i, pull_way[q], p, q).wait_send()

    def rev_sent(j):
        for q in range(4):

            @pl.when(exists(p + aim[q]))
            def _():
                rev_copy(j, back_way[q], p, q).wait_send()

    def in_halves(value, where, columns):
        rows = value.shape[0]
        high = value.astype(BF16)
        where[:rows, columns] = high
        where[rows:, columns] = (value - high.astype(F32)).astype(BF16)

    def in_thirds(value, columns):
        for part in range(3):
            high = value.astype(BF16)
            thirds[part * blocks : (part + 1) * blocks, columns] = high
            value = value - high.astype(F32)

    def squash(state):
        for c in range(comps):
            squashed[:, lane(c)] = jnp.tanh(state(c)).astype(BF16)

    def send_forward(i):
        packets = matmul(pick[...].astype(BF16), squashed[...]).astype(BF16)
        for q in FARTHEST_FIRST:
            fwd_out[i, q] = packets[q * halo : (q + 1) * halo]

            @pl.when(exists(p + aim[q]))
            def _():
                fwd_copy(i, pull_way[q], p + aim[q], q).start()

    def forward_near(i):
        gathered[...] = matmul(near[...], squashed[...]).astype(BF16)
        for k in range(slots):
            rows = squashed if k == 0 else gathered.at[pl.ds((k - 1) * blocks, blocks)]
            left = jnp.concatenate([rows[:, lane(c)] for c in range(comps)], axis=0)
            lifted[k] = matmul(left, lift_t[:, lane(k)])
        cosine = cosines[pl.ds(first + i, 1), :]
        sine = sines[pl.ds(first + i, 1), :]
        for start in range(0, blocks, CHUNK):
            some = slice(start, start + CHUNK)
            totals = [None] * comps
            for k in range(slots):
                for c in range(comps):
                    term = lifted[k, c * blocks + start : c * blocks + start + CHUNK, :]
                    for e in range(comps):
                        more = mixing[k, e, c] * term
                        totals[e] = more if totals[e] is None else totals[e] + more
            for e in range(comps):
                forcing = cosine * sources[0, e, some, :] + sine * sources[1, e, some, :]
                change = forcing - metric[some, :] * totals[e]
                base[e, some, :] = states[first + i, e, some, :] + STEP_SIZE * change

    def forward_far(i):
        for d, offset in enumerate(OFFSETS):

            @pl.when(exists(p - offset))
            def _():
                fwd_copy(i, d, p).wait_recv()

        ghost = jnp.concatenate([fwd_in[i, d] for d in range(4)], axis=0)
        left = jnp.concatenate([ghost[:, lane(c)] for c in range(comps)], axis=0)
        halo_lifted[...] = matmul(left, lift_t[:, nodes:])
        for k in range(1, slots):
            for start in range(0, ghosts, CHUNK):
                totals = [None] * comps
                for c in range(comps):
                    term = halo_lifted[c * ghosts + start : c * ghosts + start + CHUNK, lane(k - 1)]
                    for e in range(comps):
                        more = mixing[k, e, c] * term
                        totals[e] = more if totals[e] is None else totals[e] + more
                row = (k - 1) * ghosts + start
                for e in range(comps):
                    halo_mixed[row : row + CHUNK, lane(e)] = totals[e].astype(BF16)

    def forward_ahead():
        for e in range(comps):
            in_thirds(base[e], lane(e))
        picked[...] = matmul(pick_wide[...], thirds[...])

    def send_picked(i):
        wide_scale = jnp.concatenate([picked_scale[...]] * comps, axis=1)
        for start in FAR_HALF_FIRST:
            some = slice(start, start + CHUNK)
            change = matmul(far_pick[some], halo_mixed[...])
            packets = jnp.tanh(picked[some] - wide_scale[some] * change).astype(BF16)
            for q in range(start // halo, (start + CHUNK) // halo):
                fwd_out[i, q] = packets[q * halo - start : (q + 1) * halo - start]

                @pl.when(exists(p + aim[q]))
                def _():
                    fwd_copy(i, pull_way[q], p + aim[q], q).start()

    def forward_end(i):
        scale = STEP_SIZE * metric[...]
        arrived = matmul(far[...], halo_mixed[...])
        for e in range(comps):
            states[first + i + 1, e] = base[e] - scale * arrived[:, lane(e)]

    def split_field(field):
        for e in range(comps):
            in_halves(metric[...] * field[e], split, lane(e))

    def far_product(start):
        for k in range(1, slots):
            row = (k - 1) * ghosts + start
            totals = [None] * comps
            for e in range(comps):
                term = halo_pulled[row : row + CHUNK, lane(e)]
                for c in range(comps):
                    more = mixing[k, e, c] * term
                    totals[c] = more if totals[c] is None else totals[c] + more
            for c in range(comps):
                far_mixed[c * ghosts + start : c * ghosts + start + CHUNK, lane(k - 1)] = totals[
                    c
                ].astype(BF16)
        left = jnp.concatenate(
            [far_mixed[c * ghosts + start : c * ghosts + start + CHUNK] for c in range(comps)], axis=0
        )
        right = jnp.concatenate([lift[k] for k in range(1, slots)], axis=0)
        return matmul(left, right)

    def ship_reverse(j, start, product):
        packets = product.astype(BF16)
        for q in range(start // halo, (start + CHUNK) // halo):
            for c in range(comps):
                row = c * CHUNK + q * halo - start
                rev_out[j, q, :, lane(c)] = packets[row : row + halo]

            @pl.when(exists(p + aim[q]))
            def _():
                rev_copy(j, back_way[q], p + aim[q], q).start()

    def send_reverse(j):
        halo_pulled[...] = matmul(far_t[...], split[...])
        for start in FAR_HALF_FIRST:
            ship_reverse(j, start, far_product(start))

    def reverse_ahead():
        split_field(slope)
        gain[...] = matmul(pick_wide[:, : 2 * blocks], split[...])
        split_field(base)
        halo_pulled[...] = matmul(far_t[...], split[...])
        for start in FAR_HALF_FIRST:
            product = far_product(start)
            for c in range(comps):
                row = c * ghosts + start
                ahead[row : row + CHUNK] = product[c * CHUNK : (c + 1) * CHUNK]

    def send_ahead(j):
        for c in range(comps):
            back = jnp.concatenate([rev_in[j - 1, d, :, lane(c)] for d in pull_way], axis=0)
            in_halves(gain[:, lane(c)] * back.astype(F32), back_split, lane(c))
        for start in FAR_HALF_FIRST:
            rows = [slice(k * ghosts + start, k * ghosts + start + CHUNK) for k in range(slots - 1)]
            left = jnp.concatenate([cross[some] for some in rows], axis=0)
            product = matmul(left, back_split[...])
            for k, some in enumerate(rows):
                halo_pulled[some] = product[k * CHUNK : (k + 1) * CHUNK]
            made = jnp.concatenate(
                [ahead[c * ghosts + start : c * ghosts + start + CHUNK] for c in range(comps)], axis=0
            )
            ship_reverse(j, start, made - far_product(start))

    def reverse_sum(n, field):
        by_cosine = jnp.zeros((8, nodes), F32)
        by_sine = jnp.zeros((8, nodes), F32)
        for e in range(comps):
            value = field[e]
            by_cosine += jnp.sum((value * sources[1, e]).reshape(blocks // 8, 8, nodes), axis=0)
            by_sine += jnp.sum((value * sources[0, e]).reshape(blocks // 8, 8, nodes), axis=0)
        both = cosines[pl.ds(n, 1), :] * by_cosine - sines[pl.ds(n, 1), :] * by_sine
        partial[pl.ds(n, 1), :] = jnp.sum(both, axis=0, keepdims=True)

    def reverse_near(n):
        pulled[...] = matmul(near_t[...], split[...])
        for k in range(slots):
            for start in range(0, blocks, CHUNK):
                some = slice(start, start + CHUNK)
                totals = [None] * comps
                for e in range(comps):
                    if k == 0:
                        term = metric[some, :] * adjoint[e, some, :]
                    else:
                        row = (k - 1) * blocks + start
                        term = pulled[row : row + CHUNK, lane(e)]
                    for c in range(comps):
                        more = mixing[k, e, c] * term
                        totals[c] = more if totals[c] is None else totals[c] + more
                for c in range(comps):
                    mixed[c * blocks + start : c * blocks + start + CHUNK, lane(k)] = totals[c].astype(
                        BF16
                    )
        right = jnp.concatenate([lift[k] for k in range(slots)], axis=0)
        pushed = matmul(mixed[...], right)
        inner = jnp.where(n > 0, 1.0, 0.0).astype(F32)
        for c in range(comps):
            state = states[n, c]
            bent = jnp.tanh(state)
            fall = STEP_SIZE * (1.0 - bent * bent)
            slope[c] = fall
            grown = adjoint[c] + inner * (weight[c] * state)
            base[c] = grown - fall * pushed[c * blocks : (c + 1) * blocks]

    def reverse_wait(j):
        for d, offset in enumerate(OFFSETS):

            @pl.when(exists(p + offset))
            def _():
                rev_copy(j, d, p).wait_recv()

    def reverse_far(j):
        ghost = jnp.concatenate([rev_in[j, d] for d in pull_way], axis=0)
        arrived = matmul(pick_t[...], ghost)
        for c in range(comps):
            adjoint[c] = base[c] - slope[c] * arrived[:, lane(c)]

    def send_bend():
        for e in range(comps):
            bent = jnp.tanh(states[1, e])
            turning = cosines[0:1, :] * sources[1, e] - sines[0:1, :] * sources[0, e]
            squashed[:, lane(e)] = (STEP_SIZE * (1.0 - bent * bent) * turning).astype(BF16)
        packets = matmul(pick[...].astype(BF16), squashed[...]).astype(BF16)
        for q in range(4):
            bend_out[q] = packets[q * halo : (q + 1) * halo]

            @pl.when(exists(p + aim[q]))
            def _():
                bend_copy(pull_way[q], p + aim[q], q).start()

        for d, offset in enumerate(OFFSETS):

            @pl.when(exists(p - offset))
            def _():
                bend_copy(d, p).wait_recv()

        bend_pass.start()

    def last_sum(j):
        reverse_sum(0, base)
        bend_pass.wait_recv()
        sent = jnp.zeros((halo, nodes), F32)
        for d in range(4):
            both = rev_out[j, d].astype(F32) * bend_there[back_way[d]].astype(F32)
            for c in range(comps):
                sent += both[:, lane(c)]
        partial[0:1, :] = partial[0:1, :] - jnp.sum(sent, axis=0, keepdims=True)

    norm = math.sqrt(comps * nodes * blocks * n_space)

    def in_row(tile):
        sums = jnp.sum(tile, axis=1, keepdims=True) * (STEP_SIZE / norm)
        lanes = lax.broadcasted_iota(jnp.int32, (levels, nodes), 1)
        diagonal = lanes == lax.broadcasted_iota(jnp.int32, (levels, nodes), 0)
        return jnp.sum(jnp.where(diagonal, sums, 0.0), axis=0, keepdims=True)

    load_first.wait()
    squash(lambda c: states[first, c])
    near_peers = sum(exists(p + offset).astype(jnp.int32) for offset in OFFSETS)
    pl.semaphore_wait(barrier, near_peers + 1 + 2 * t)
    send_forward(0)

    @pl.when(t == 0)
    def _():
        state_copy(0).start()

    @pl.when(t == 1)
    def _():
        call(0, 1)

    load_lift.wait()
    for k in range(slots):
        lift_t[:, lane(k)] = lift[k].astype(F32).T.astype(BF16)
    pick_t[...] = pick[...].T.astype(BF16)
    load_pitch.wait()
    load_faces.wait()
    load_mixing.wait()
    row_of = lax.broadcasted_iota(jnp.int32, (levels, nodes), 0)
    angles = jnp.zeros((levels, nodes), F32)
    for n in range(levels):
        angles = jnp.where(row_of == n, pitch[n], angles)
    cosines[...] = jnp.cos(angles)
    sines[...] = jnp.sin(angles)
    row_at = lax.broadcasted_iota(jnp.int32, (blocks, blocks), 0)
    for k in range(1, slots):
        chosen = jnp.where(faces[k - 1 : k, :] == row_at, 1.0, 0.0)
        near[(k - 1) * blocks : k * blocks, :] = chosen.T.astype(BF16)
        turned = chosen.astype(BF16)
        near_t[(k - 1) * blocks : k * blocks, :blocks] = turned
        near_t[(k - 1) * blocks : k * blocks, blocks:] = turned
    slot_at = lax.rem(row_at, ghosts)
    group = slot_at // halo
    way = jnp.where(group == 0, back_way[0], back_way[1])
    way = jnp.where(group == 2, back_way[2], way)
    way = jnp.where(group == 3, back_way[3], way)
    sent_at = way * halo + lax.rem(slot_at, halo)
    for pair in range(2):
        upper = faces[2 * pair : 2 * pair + 1, :] - blocks
        lower = faces[2 * pair + 1 : 2 * pair + 2, :] - blocks
        wanted = jnp.where(row_at < ghosts, upper, lower)
        chosen = jnp.where(wanted == slot_at, 1.0, 0.0)
        far[:, pair * blocks : (pair + 1) * blocks] = chosen.T.astype(BF16)
        turned = jnp.where(wanted == sent_at, 1.0, 0.0).astype(BF16)
        far_t[pair * blocks : (pair + 1) * blocks, :blocks] = turned
        far_t[pair * blocks : (pair + 1) * blocks, blocks:] = turned
    wide_pick = pick[...].astype(BF16)
    for part in range(3):
        pick_wide[:, part * blocks : (part + 1) * blocks] = wide_pick
    far_pick[...] = matmul(wide_pick, far[...]).astype(BF16)
    crossed = matmul(far_t[:, :blocks], pick_t[...]).astype(BF16)
    cross[...] = jnp.concatenate([crossed, crossed], axis=1)
    load_metric.wait()
    in_thirds(STEP_SIZE * metric[...], lane(0))
    picked_scale[...] = matmul(pick_wide[...], thirds[:, lane(0)])
    load_sources.wait()
    last = half - 2 + t

    def forward_level(i, carry):
        forward_near(i)
        forward_ahead()

        @pl.when(i > 0)
        def _():
            fwd_sent(i - 1)

        forward_far(i)

        @pl.when(i < last)
        def _():
            send_picked(i + 1)

        forward_end(i)

        @pl.when(i < last)
        def _():
            squash(lambda c: states[first + i + 1, c])

        @pl.when(t == 0)
        def _():
            state_copy(i + 1).start()

        return carry

    lax.fori_loop(0, half - 1 + t, forward_level, 0)

    load_weight.wait()
    load_end.wait()

    @pl.when(t == 0)
    def _():
        send_bend()

    @pl.when(t == 1)
    def _():
        pl.semaphore_wait(hello.at[0], 2)
        call(1, 2)
        for e in range(comps):
            adjoint[e] = adjoint[e] + weight[e] * states[levels, e]
        split_field(adjoint)
        send_reverse(0)

        def reverse_level(j, carry):
            n = levels - 1 - j

            @pl.when(n < half)
            def _():
                state_copy(n).wait_recv()

            reverse_sum(n, adjoint)
            reverse_near(n)
            reverse_ahead()

            @pl.when(j > 0)
            def _():
                rev_sent(j - 1)

            reverse_wait(j)
            send_ahead(j + 1)
            reverse_far(j)
            split_field(adjoint)

            @pl.when(n == half)
            def _():
                kept[...] = adjoint[...]
                keep_copy.start()

            return carry

        lax.fori_loop(0, levels - 2, reverse_level, 0)
        state_copy(1).wait_recv()
        reverse_sum(1, adjoint)
        reverse_near(1)
        pl.semaphore_wait(hello.at[1], 2)
        call(2, 2)
        last_sum(levels - 2)
        row = in_row(partial[...])
        plane_row[...] = row
        plane_parts[spot] = row
        for r in range(1, plane):
            plane_copy(r).start()
        reverse_ahead()
        rev_sent(levels - 3)
        reverse_wait(levels - 2)
        send_ahead(levels - 1)
        reverse_far(levels - 2)
        split_field(adjoint)
        pl.semaphore_wait(hello.at[2], 2)
        all_parts(plane_parts, plane - 1, plane_send, plane_recv).wait_recv()
        total = plane_parts[0]
        for s in range(1, plane):
            total = total + plane_parts[s]
        plane_sum[...] = total
        layer_parts[layer] = total
        for r in range(layers):
            layer_copy(r, 0).start()
            if r > 0:
                layer_copy(r, 1).start()
        state_copy(0).wait_recv()
        reverse_near(0)
        rev_sent(levels - 2)
        reverse_wait(levels - 1)
        reverse_far(levels - 1)
        end_copy.start()

    fwd_sent(last)

    @pl.when(t == 0)
    def _():
        for i in range(half):
            state_copy(i).wait_send()
        for q in range(4):

            @pl.when(exists(p + aim[q]))
            def _():
                bend_copy(pull_way[q], p, q).wait_send()

        bend_pass.wait_send()

    @pl.when(t == 1)
    def _():
        rev_sent(levels - 1)
        keep_copy.wait()
        all_parts(plane_parts, plane - 1, plane_send, plane_recv).wait_send()
        all_parts(layer_parts, 2 * layers - 1, layer_send, layer_recv).wait_send()

    @pl.when(t == 0)
    def _():
        all_parts(layer_parts, layers, layer_send, layer_recv).wait_recv()

    @pl.when(t == 1)
    def _():
        all_parts(layer_parts, layers - 1, layer_send, layer_recv).wait_recv()

    total = layer_parts[0]
    for s in range(1, layers):
        total = total + layer_parts[s]
    grads_row[...] = total
    give_sums = pltpu.make_async_copy(grads_row, grads, out_sem.at[1])
    give_sums.start()

    @pl.when(t == 0)
    def _():
        end_copy.wait_recv()

    @pl.when(t == 1)
    def _():
        end_copy.wait_send()

    give_sums.wait()


def deliver(found, row, bounds, grads, held, sums, sums_out, sem):
    comps = held.shape[0]
    into = [pltpu.make_async_copy(found.at[0, c], held.at[c], sem.at[0, c]) for c in range(comps)]
    outof = [pltpu.make_async_copy(held.at[c], bounds.at[0, c], sem.at[1, c]) for c in range(comps)]
    row_in = pltpu.make_async_copy(row, sums, sem.at[0, comps])
    row_out = pltpu.make_async_copy(sums_out, grads, sem.at[1, comps])
    row_in.start()
    for copy in into:
        copy.start()
    row_in.wait()
    sums_out[...] = sums[0, : sums_out.shape[0]]
    row_out.start()
    for arrive, leave in zip(into, outof):
        arrive.wait()
        leave.start()
    row_out.wait()
    for leave in outof:
        leave.wait()


def solution(mesh):
    n_space = mesh.shape["space"]
    plane = 16 if n_space % 16 == 0 else 4

    def shards(
        checkpoints, sources, pitch, metric, obj_weight, adjoint_end, lift, mixing, faces, send_idx
    ):
        comps, blocks, nodes = obj_weight.shape
        slots = lift.shape[0]
        levels = pitch.shape[0]
        half = levels // 2
        halo = send_idx.shape[2]
        ghosts = 4 * halo
        wide = comps * nodes
        links = slots - 1
        layers = n_space // plane
        vmem = pltpu.VMEM
        dma = pltpu.SemaphoreType.DMA
        field = (comps, blocks, nodes)
        smem = pltpu.SMEM
        scratch = [
            smem((levels,), F32),
            smem(mixing.shape, F32),
            vmem((links, blocks), jnp.int32),
            smem(send_idx.shape, jnp.int32),
            vmem((1, nodes), F32),
            vmem((levels + 1, *field), F32),
            vmem((2, *field), F32),
            vmem((blocks, nodes), F32),
            vmem(field, F32),
            vmem(field, F32),
            vmem(field, F32),
            vmem((slots, nodes, nodes), BF16),
            vmem((nodes, slots * nodes), BF16),
            vmem((levels, nodes), F32),
            vmem((levels, nodes), F32),
            vmem((ghosts, blocks), F32),
            vmem((blocks, ghosts), BF16),
            vmem((links * blocks, blocks), BF16),
            vmem((links * blocks, 2 * blocks), BF16),
            vmem((blocks, links * ghosts), BF16),
            vmem((links * ghosts, 2 * blocks), BF16),
            vmem((ghosts, links * ghosts), BF16),
            vmem((links * ghosts, 2 * ghosts), BF16),
            vmem((ghosts, 3 * blocks), BF16),
            vmem((3 * blocks, wide), BF16),
            vmem((ghosts, wide), F32),
            vmem((ghosts, nodes), F32),
            vmem((ghosts, wide), F32),
            vmem((2 * ghosts, wide), BF16),
            vmem((comps * ghosts, nodes), F32),
            vmem((blocks, wide), BF16),
            vmem((links * blocks, wide), BF16),
            vmem((slots, comps * blocks, nodes), F32),
            vmem(field, F32),
            vmem(field, F32),
            vmem((comps * ghosts, links * nodes), F32),
            vmem((links * ghosts, wide), BF16),
            vmem((2 * blocks, wide), BF16),
            vmem((links * blocks, wide), F32),
            vmem((links * ghosts, wide), F32),
            vmem((comps * blocks, slots * nodes), BF16),
            vmem((comps * ghosts, links * nodes), BF16),
            vmem((half, 4, halo, wide), BF16),
            vmem((half, 4, halo, wide), BF16),
            vmem((levels, 4, halo, wide), BF16),
            vmem((levels, 4, halo, wide), BF16),
            vmem((4, halo, wide), BF16),
            vmem((4, halo, wide), BF16),
            vmem((4, halo, wide), BF16),
            vmem((levels, nodes), F32),
            vmem((1, nodes), F32),
            vmem((plane, 1, nodes), F32),
            vmem((1, nodes), F32),
            vmem((2 * layers, 1, nodes), F32),
            dma((10,)),
            dma((2, 4)),
            dma((2, 4)),
            dma((2, 4)),
            dma((2, 4)),
            dma((4,)),
            dma((4,)),
            dma((2,)),
            dma((half,)),
            dma((half,)),
            dma,
            dma,
            dma,
            dma,
            dma((2,)),
            dma((2,)),
            pltpu.SemaphoreType.REGULAR((3,)),
        ]
        anywhere = pl.BlockSpec(memory_space=pl.ANY)
        results, sums = pl.pallas_call(
            functools.partial(sweep, n_space, plane),
            out_shape=(
                jax.ShapeDtypeStruct((1, *field), F32),
                jax.ShapeDtypeStruct((1, nodes), F32),
            ),
            in_specs=[pl.BlockSpec(memory_space=pltpu.HBM)] * 10,
            out_specs=(anywhere, anywhere),
            scratch_shapes=scratch,
            compiler_params=pltpu.CompilerParams(
                collective_id=0, has_side_effects=True, vmem_limit_bytes=67043328
            ),
            name="adjoint_window",
        )(checkpoints, sources, pitch, metric, obj_weight, adjoint_end, lift, mixing, faces.T, send_idx)
        return pl.pallas_call(
            deliver,
            out_shape=(
                jax.ShapeDtypeStruct((1, *field), F32),
                jax.ShapeDtypeStruct((levels,), F32),
            ),
            in_specs=[anywhere, anywhere],
            out_specs=(anywhere, anywhere),
            scratch_shapes=[
                vmem(field, F32),
                vmem((1, nodes), F32),
                vmem((levels,), F32),
                dma((2, comps + 1)),
            ],
            compiler_params=pltpu.CompilerParams(vmem_limit_bytes=67043328),
            name="deliver",
        )(results, sums)

    return jax.shard_map(
        shards,
        mesh=mesh,
        in_specs=(
            P("tm", None, "space", None),
            P(None, None, "space", None),
            P(),
            P("space", None),
            P(None, "space", None),
            P(None, "space", None),
            P(),
            P(),
            P("space", None),
            P("space", None, None),
        ),
        out_specs=(P("tm", None, "space", None), P()),
        check_vma=False,
    )
```

```python
import functools
import math

import jax
import jax.numpy as jnp
from jax import lax
from jax.experimental import pallas as pl
from jax.experimental.pallas import tpu as pltpu
from jax.sharding import PartitionSpec as P

OFFSETS = (1, -1, 2, -2)
FARTHEST_FIRST = (2, 3, 0, 1)
STEP_SIZE = 0.5
MESH = pl.DeviceIdType.MESH
F32, BF16 = jnp.float32, jnp.bfloat16
CHUNK = 32
FAR_HALF_FIRST = (32, 0)


def matmul(left, right):
    return jnp.dot(left, right, preferred_element_type=F32)


def parity(level):
    return level % 2 if isinstance(level, int) else lax.rem(level, 2)


def sweep(
    n_space,
    plane,
    checkpoint_in,
    sources_in,
    pitch_in,
    metric_in,
    weight_in,
    end_in,
    lift_in,
    mixing_in,
    faces_in,
    send_idx_in,
    bounds,
    grads,
    pitch,
    mixing,
    faces,
    send_idx,
    grads_row,
    states,
    sources,
    metric,
    weight,
    adjoint,
    kept,
    lift,
    lift_t,
    cosines,
    sines,
    pick,
    pick_t,
    near,
    near_t,
    far,
    far_t,
    far_pick,
    cross,
    pick_wide,
    thirds,
    picked,
    picked_scale,
    gain,
    back_split,
    ahead,
    squashed,
    gathered,
    lifted,
    base,
    slope,
    halo_lifted,
    halo_mixed,
    split,
    pulled,
    halo_pulled,
    mixed,
    far_mixed,
    fwd_out,
    fwd_in,
    rev_out,
    rev_in,
    bend_out,
    bend_in,
    bend_there,
    partial,
    plane_row,
    plane_parts,
    plane_sum,
    layer_parts,
    in_sem,
    fwd_send,
    fwd_recv,
    rev_send,
    rev_recv,
    bend_send,
    bend_recv,
    bend_sem,
    state_send,
    state_recv,
    plane_send,
    plane_recv,
    layer_send,
    layer_recv,
    end_sem,
    out_sem,
    hello,
):
    comps, blocks, nodes = states.shape[1:]
    slots = lift.shape[0]
    halo = fwd_in.shape[2]
    ghosts = 4 * halo
    levels = pitch.shape[0]
    half = levels // 2
    layers = n_space // plane
    t = lax.axis_index("tm")
    p = lax.axis_index("space")
    spot = lax.rem(p, plane)
    layer = p // plane
    first = t * half

    hot = jnp.where(lax.rem(p, 4) >= 2, 1, 0)
    toward = 2 * hot - 1
    aim = (-2 * toward, -toward, 2 * toward, toward)
    pull_way = (2 + hot, hot, 3 - hot, 1 - hot)
    back_way = (3 - hot, 1 - hot, 2 + hot, hot)

    def exists(q):
        return jnp.logical_and(q >= 0, q < n_space)

    def lane(c):
        return slice(c * nodes, (c + 1) * nodes)

    (
        load_first,
        load_idx,
        load_mixing,
        load_faces,
        load_pitch,
        load_lift,
        load_metric,
        load_sources,
        load_weight,
        load_end,
    ) = loads = [
        pltpu.make_async_copy(checkpoint_in.at[0], states.at[first], in_sem.at[0]),
        pltpu.make_async_copy(send_idx_in, send_idx, in_sem.at[6]),
        pltpu.make_async_copy(mixing_in, mixing, in_sem.at[7]),
        pltpu.make_async_copy(faces_in, faces, in_sem.at[8]),
        pltpu.make_async_copy(pitch_in, pitch, in_sem.at[9]),
        pltpu.make_async_copy(lift_in, lift, in_sem.at[1]),
        pltpu.make_async_copy(metric_in, metric, in_sem.at[2]),
        pltpu.make_async_copy(sources_in, sources, in_sem.at[3]),
        pltpu.make_async_copy(weight_in, weight, in_sem.at[4]),
        pltpu.make_async_copy(end_in, adjoint, in_sem.at[5]),
    ]
    barrier = pltpu.get_barrier_semaphore()

    def greet(device):
        pl.semaphore_signal(barrier, inc=1, device_id=device, device_id_type=MESH)

    for offset in OFFSETS:

        @pl.when(exists(p + offset))
        def _():
            greet((t, p + offset))

    greet((1 - t, p))

    def in_layer(r):
        return (1, lax.rem(layer + r + layers, layers) * plane + spot)

    @pl.when(t == 1)
    def _():
        greet(in_layer(1))
        greet(in_layer(-1))

    def call(which, distance):
        for r in (distance, -distance):
            pl.semaphore_signal(
                hello.at[which], inc=1, device_id=in_layer(r), device_id_type=MESH
            )

    for load in loads:
        load.start()

    load_idx.wait()
    lane_of = lax.broadcasted_iota(jnp.int32, (1, blocks), 1)
    for d in range(4):
        for s in range(halo):
            row = d * halo + s
            pick[pl.ds(row, 1), :] = jnp.where(lane_of == send_idx[0, pull_way[d], s], 1.0, 0.0)

    for d, offset in enumerate(OFFSETS):

        @pl.when(jnp.logical_not(exists(p - offset)))
        def _():
            bend_in[d] = jnp.zeros(bend_in.shape[1:], BF16)
            for i in range(half):
                fwd_in[i, d] = jnp.zeros(fwd_in.shape[2:], BF16)

        @pl.when(jnp.logical_not(exists(p + offset)))
        def _():
            for i in range(levels):
                rev_in[i, d] = jnp.zeros(rev_in.shape[2:], BF16)

    def fwd_copy(i, d, device, q=0):
        return pltpu.make_async_remote_copy(
            src_ref=fwd_out.at[i, q],
            dst_ref=fwd_in.at[i, d],
            send_sem=fwd_send.at[parity(i), q],
            recv_sem=fwd_recv.at[parity(i), d],
            device_id=(t, device),
            device_id_type=MESH,
        )

    def rev_copy(i, d, device, q=0):
        return pltpu.make_async_remote_copy(
            src_ref=rev_out.at[i, q],
            dst_ref=rev_in.at[i, d],
            send_sem=rev_send.at[parity(i), q],
            recv_sem=rev_recv.at[parity(i), d],
            device_id=(t, device),
            device_id_type=MESH,
        )

    def bend_copy(d, device, q=0):
        return pltpu.make_async_remote_copy(
            src_ref=bend_out.at[q],
            dst_ref=bend_in.at[d],
            send_sem=bend_send.at[q],
            recv_sem=bend_recv.at[d],
            device_id=(t, device),
            device_id_type=MESH,
        )

    def state_copy(i):
        return pltpu.make_async_remote_copy(
            src_ref=states.at[i],
            dst_ref=states.at[i],
            send_sem=state_send.at[i],
            recv_sem=state_recv.at[i],
            device_id=(1 - t, p),
            device_id_type=MESH,
        )

    def plane_copy(r):
        return pltpu.make_async_remote_copy(
            src_ref=plane_row,
            dst_ref=plane_parts.at[spot],
            send_sem=plane_send,
            recv_sem=plane_recv,
            device_id=(1, layer * plane + lax.rem(spot + r, plane)),
            device_id_type=MESH,
        )

    def layer_copy(r, core):
        return pltpu.make_async_remote_copy(
            src_ref=plane_sum,
            dst_ref=layer_parts.at[layer],
            send_sem=layer_send,
            recv_sem=layer_recv,
            device_id=(core, lax.rem(layer + r, layers) * plane + spot),
            device_id_type=MESH,
        )

    bend_pass = pltpu.make_async_remote_copy(
        src_ref=bend_in,
        dst_ref=bend_there,
        send_sem=bend_sem.at[0],
        recv_sem=bend_sem.at[1],
        device_id=(1 - t, p),
        device_id_type=MESH,
    )
    def all_parts(parts, count, send_sem, recv_sem):
        return pltpu.make_async_remote_copy(
            src_ref=parts.at[pl.ds(0, count)],
            dst_ref=parts.at[pl.ds(0, count)],
            send_sem=send_sem,
            recv_sem=recv_sem,
            device_id=(1 - t, p),
            device_id_type=MESH,
        )

    end_copy = pltpu.make_async_remote_copy(
        src_ref=adjoint,
        dst_ref=bounds.at[0],
        send_sem=end_sem.at[0],
        recv_sem=end_sem.at[1],
        device_id=(1 - t, p),
        device_id_type=MESH,
    )
    keep_copy = pltpu.make_async_copy(kept, bounds.at[0], out_sem.at[0])

    def fwd_sent(i):
        for q in range(4):

            @pl.when(exists(p + aim[q]))
            def _():
                fwd_copy(i, pull_way[q], p, q).wait_send()

    def rev_sent(j):
        for q in range(4):

            @pl.when(exists(p + aim[q]))
            def _():
                rev_copy(j, back_way[q], p, q).wait_send()

    def in_halves(value, where, columns):
        rows = value.shape[0]
        high = value.astype(BF16)
        where[:rows, columns] = high
        where[rows:, columns] = (value - high.astype(F32)).astype(BF16)

    def in_thirds(value, columns):
        for part in range(3):
            high = value.astype(BF16)
            thirds[part * blocks : (part + 1) * blocks, columns] = high
            value = value - high.astype(F32)

    def squash(state):
        for c in range(comps):
            squashed[:, lane(c)] = jnp.tanh(state(c)).astype(BF16)

    def send_forward(i):
        packets = matmul(pick[...].astype(BF16), squashed[...]).astype(BF16)
        for q in FARTHEST_FIRST:
            fwd_out[i, q] = packets[q * halo : (q + 1) * halo]

            @pl.when(exists(p + aim[q]))
            def _():
                fwd_copy(i, pull_way[q], p + aim[q], q).start()

    def forward_near(i):
        gathered[...] = matmul(near[...], squashed[...]).astype(BF16)
        for k in range(slots):
            rows = squashed if k == 0 else gathered.at[pl.ds((k - 1) * blocks, blocks)]
            left = jnp.concatenate([rows[:, lane(c)] for c in range(comps)], axis=0)
            lifted[k] = matmul(left, lift_t[:, lane(k)])
        cosine = cosines[pl.ds(first + i, 1), :]
        sine = sines[pl.ds(first + i, 1), :]
        for start in range(0, blocks, CHUNK):
            some = slice(start, start + CHUNK)
            totals = [None] * comps
            for k in range(slots):
                for c in range(comps):
                    term = lifted[k, c * blocks + start : c * blocks + start + CHUNK, :]
                    for e in range(comps):
                        more = mixing[k, e, c] * term
                        totals[e] = more if totals[e] is None else totals[e] + more
            for e in range(comps):
                forcing = cosine * sources[0, e, some, :] + sine * sources[1, e, some, :]
                change = forcing - metric[some, :] * totals[e]
                base[e, some, :] = states[first + i, e, some, :] + STEP_SIZE * change

    def forward_far(i):
        for d, offset in enumerate(OFFSETS):

            @pl.when(exists(p - offset))
            def _():
                fwd_copy(i, d, p).wait_recv()

        ghost = jnp.concatenate([fwd_in[i, d] for d in range(4)], axis=0)
        left = jnp.concatenate([ghost[:, lane(c)] for c in range(comps)], axis=0)
        halo_lifted[...] = matmul(left, lift_t[:, nodes:])
        for k in range(1, slots):
            for start in range(0, ghosts, CHUNK):
                totals = [None] * comps
                for c in range(comps):
                    term = halo_lifted[c * ghosts + start : c * ghosts + start + CHUNK, lane(k - 1)]
                    for e in range(comps):
                        more = mixing[k, e, c] * term
                        totals[e] = more if totals[e] is None else totals[e] + more
                row = (k - 1) * ghosts + start
                for e in range(comps):
                    halo_mixed[row : row + CHUNK, lane(e)] = totals[e].astype(BF16)

    def forward_ahead():
        for e in range(comps):
            in_thirds(base[e], lane(e))
        picked[...] = matmul(pick_wide[...], thirds[...])

    def send_picked(i):
        wide_scale = jnp.concatenate([picked_scale[...]] * comps, axis=1)
        for start in FAR_HALF_FIRST:
            some = slice(start, start + CHUNK)
            change = matmul(far_pick[some], halo_mixed[...])
            packets = jnp.tanh(picked[some] - wide_scale[some] * change).astype(BF16)
            for q in range(start // halo, (start + CHUNK) // halo):
                fwd_out[i, q] = packets[q * halo - start : (q + 1) * halo - start]

                @pl.when(exists(p + aim[q]))
                def _():
                    fwd_copy(i, pull_way[q], p + aim[q], q).start()

    def forward_end(i):
        scale = STEP_SIZE * metric[...]
        arrived = matmul(far[...], halo_mixed[...])
        for e in range(comps):
            states[first + i + 1, e] = base[e] - scale * arrived[:, lane(e)]

    def split_field(field):
        for e in range(comps):
            in_halves(metric[...] * field[e], split, lane(e))

    def far_product(start):
        for k in range(1, slots):
            row = (k - 1) * ghosts + start
            totals = [None] * comps
            for e in range(comps):
                term = halo_pulled[row : row + CHUNK, lane(e)]
                for c in range(comps):
                    more = mixing[k, e, c] * term
                    totals[c] = more if totals[c] is None else totals[c] + more
            for c in range(comps):
                far_mixed[c * ghosts + start : c * ghosts + start + CHUNK, lane(k - 1)] = totals[
                    c
                ].astype(BF16)
        left = jnp.concatenate(
            [far_mixed[c * ghosts + start : c * ghosts + start + CHUNK] for c in range(comps)], axis=0
        )
        right = jnp.concatenate([lift[k] for k in range(1, slots)], axis=0)
        return matmul(left, right)

    def ship_reverse(j, start, product):
        packets = product.astype(BF16)
        for q in range(start // halo, (start + CHUNK) // halo):
            for c in range(comps):
                row = c * CHUNK + q * halo - start
                rev_out[j, q, :, lane(c)] = packets[row : row + halo]

            @pl.when(exists(p + aim[q]))
            def _():
                rev_copy(j, back_way[q], p + aim[q], q).start()

    def send_reverse(j):
        halo_pulled[...] = matmul(far_t[...], split[...])
        for start in FAR_HALF_FIRST:
            ship_reverse(j, start, far_product(start))

    def reverse_ahead():
        split_field(slope)
        gain[...] = matmul(pick_wide[:, : 2 * blocks], split[...])
        split_field(base)
        halo_pulled[...] = matmul(far_t[...], split[...])
        for start in FAR_HALF_FIRST:
            product = far_product(start)
            for c in range(comps):
                row = c * ghosts + start
                ahead[row : row + CHUNK] = product[c * CHUNK : (c + 1) * CHUNK]

    def send_ahead(j):
        for c in range(comps):
            back = jnp.concatenate([rev_in[j - 1, d, :, lane(c)] for d in pull_way], axis=0)
            in_halves(gain[:, lane(c)] * back.astype(F32), back_split, lane(c))
        for start in FAR_HALF_FIRST:
            rows = [slice(k * ghosts + start, k * ghosts + start + CHUNK) for k in range(slots - 1)]
            left = jnp.concatenate([cross[some] for some in rows], axis=0)
            product = matmul(left, back_split[...])
            for k, some in enumerate(rows):
                halo_pulled[some] = product[k * CHUNK : (k + 1) * CHUNK]
            made = jnp.concatenate(
                [ahead[c * ghosts + start : c * ghosts + start + CHUNK] for c in range(comps)], axis=0
            )
            ship_reverse(j, start, made - far_product(start))

    def reverse_sum(n, field):
        by_cosine = jnp.zeros((8, nodes), F32)
        by_sine = jnp.zeros((8, nodes), F32)
        for e in range(comps):
            value = field[e]
            by_cosine += jnp.sum((value * sources[1, e]).reshape(blocks // 8, 8, nodes), axis=0)
            by_sine += jnp.sum((value * sources[0, e]).reshape(blocks // 8, 8, nodes), axis=0)
        both = cosines[pl.ds(n, 1), :] * by_cosine - sines[pl.ds(n, 1), :] * by_sine
        partial[pl.ds(n, 1), :] = jnp.sum(both, axis=0, keepdims=True)

    def reverse_near(n):
        pulled[...] = matmul(near_t[...], split[...])
        for k in range(slots):
            for start in range(0, blocks, CHUNK):
                some = slice(start, start + CHUNK)
                totals = [None] * comps
                for e in range(comps):
                    if k == 0:
                        term = metric[some, :] * adjoint[e, some, :]
                    else:
                        row = (k - 1) * blocks + start
                        term = pulled[row : row + CHUNK, lane(e)]
                    for c in range(comps):
                        more = mixing[k, e, c] * term
                        totals[c] = more if totals[c] is None else totals[c] + more
                for c in range(comps):
                    mixed[c * blocks + start : c * blocks + start + CHUNK, lane(k)] = totals[c].astype(
                        BF16
                    )
        right = jnp.concatenate([lift[k] for k in range(slots)], axis=0)
        pushed = matmul(mixed[...], right)
        inner = jnp.where(n > 0, 1.0, 0.0).astype(F32)
        for c in range(comps):
            state = states[n, c]
            bent = jnp.tanh(state)
            fall = STEP_SIZE * (1.0 - bent * bent)
            slope[c] = fall
            grown = adjoint[c] + inner * (weight[c] * state)
            base[c] = grown - fall * pushed[c * blocks : (c + 1) * blocks]

    def reverse_wait(j):
        for d, offset in enumerate(OFFSETS):

            @pl.when(exists(p + offset))
            def _():
                rev_copy(j, d, p).wait_recv()

    def reverse_far(j):
        ghost = jnp.concatenate([rev_in[j, d] for d in pull_way], axis=0)
        arrived = matmul(pick_t[...], ghost)
        for c in range(comps):
            adjoint[c] = base[c] - slope[c] * arrived[:, lane(c)]

    def send_bend():
        for e in range(comps):
            bent = jnp.tanh(states[1, e])
            turning = cosines[0:1, :] * sources[1, e] - sines[0:1, :] * sources[0, e]
            squashed[:, lane(e)] = (STEP_SIZE * (1.0 - bent * bent) * turning).astype(BF16)
        packets = matmul(pick[...].astype(BF16), squashed[...]).astype(BF16)
        for q in range(4):
            bend_out[q] = packets[q * halo : (q + 1) * halo]

            @pl.when(exists(p + aim[q]))
            def _():
                bend_copy(pull_way[q], p + aim[q], q).start()

        for d, offset in enumerate(OFFSETS):

            @pl.when(exists(p - offset))
            def _():
                bend_copy(d, p).wait_recv()

        bend_pass.start()

    def last_sum(j):
        reverse_sum(0, base)
        bend_pass.wait_recv()
        sent = jnp.zeros((halo, nodes), F32)
        for d in range(4):
            both = rev_out[j, d].astype(F32) * bend_there[back_way[d]].astype(F32)
            for c in range(comps):
                sent += both[:, lane(c)]
        partial[0:1, :] = partial[0:1, :] - jnp.sum(sent, axis=0, keepdims=True)

    norm = math.sqrt(comps * nodes * blocks * n_space)

    def in_row(tile):
        sums = jnp.sum(tile, axis=1, keepdims=True) * (STEP_SIZE / norm)
        lanes = lax.broadcasted_iota(jnp.int32, (levels, nodes), 1)
        diagonal = lanes == lax.broadcasted_iota(jnp.int32, (levels, nodes), 0)
        return jnp.sum(jnp.where(diagonal, sums, 0.0), axis=0, keepdims=True)

    load_first.wait()
    squash(lambda c: states[first, c])
    near_peers = sum(exists(p + offset).astype(jnp.int32) for offset in OFFSETS)
    pl.semaphore_wait(barrier, near_peers + 1 + 2 * t)
    send_forward(0)

    @pl.when(t == 0)
    def _():
        state_copy(0).start()

    @pl.when(t == 1)
    def _():
        call(0, 1)

    load_lift.wait()
    for k in range(slots):
        lift_t[:, lane(k)] = lift[k].astype(F32).T.astype(BF16)
    pick_t[...] = pick[...].T.astype(BF16)
    load_pitch.wait()
    load_faces.wait()
    load_mixing.wait()
    row_of = lax.broadcasted_iota(jnp.int32, (levels, nodes), 0)
    angles = jnp.zeros((levels, nodes), F32)
    for n in range(levels):
        angles = jnp.where(row_of == n, pitch[n], angles)
    cosines[...] = jnp.cos(angles)
    sines[...] = jnp.sin(angles)
    row_at = lax.broadcasted_iota(jnp.int32, (blocks, blocks), 0)
    for k in range(1, slots):
        chosen = jnp.where(faces[k - 1 : k, :] == row_at, 1.0, 0.0)
        near[(k - 1) * blocks : k * blocks, :] = chosen.T.astype(BF16)
        turned = chosen.astype(BF16)
        near_t[(k - 1) * blocks : k * blocks, :blocks] = turned
        near_t[(k - 1) * blocks : k * blocks, blocks:] = turned
    slot_at = lax.rem(row_at, ghosts)
    group = slot_at // halo
    way = jnp.where(group == 0, back_way[0], back_way[1])
    way = jnp.where(group == 2, back_way[2], way)
    way = jnp.where(group == 3, back_way[3], way)
    sent_at = way * halo + lax.rem(slot_at, halo)
    for pair in range(2):
        upper = faces[2 * pair : 2 * pair + 1, :] - blocks
        lower = faces[2 * pair + 1 : 2 * pair + 2, :] - blocks
        wanted = jnp.where(row_at < ghosts, upper, lower)
        chosen = jnp.where(wanted == slot_at, 1.0, 0.0)
        far[:, pair * blocks : (pair + 1) * blocks] = chosen.T.astype(BF16)
        turned = jnp.where(wanted == sent_at, 1.0, 0.0).astype(BF16)
        far_t[pair * blocks : (pair + 1) * blocks, :blocks] = turned
        far_t[pair * blocks : (pair + 1) * blocks, blocks:] = turned
    wide_pick = pick[...].astype(BF16)
    for part in range(3):
        pick_wide[:, part * blocks : (part + 1) * blocks] = wide_pick
    far_pick[...] = matmul(wide_pick, far[...]).astype(BF16)
    crossed = matmul(far_t[:, :blocks], pick_t[...]).astype(BF16)
    cross[...] = jnp.concatenate([crossed, crossed], axis=1)
    load_metric.wait()
    in_thirds(STEP_SIZE * metric[...], lane(0))
    picked_scale[...] = matmul(pick_wide[...], thirds[:, lane(0)])
    load_sources.wait()
    last = half - 2 + t

    def forward_level(i, carry):
        forward_near(i)
        forward_ahead()

        @pl.when(i > 0)
        def _():
            fwd_sent(i - 1)

        forward_far(i)

        @pl.when(i < last)
        def _():
            send_picked(i + 1)

        forward_end(i)

        @pl.when(i < last)
        def _():
            squash(lambda c: states[first + i + 1, c])

        @pl.when(t == 0)
        def _():
            state_copy(i + 1).start()

        return carry

    lax.fori_loop(0, half - 1 + t, forward_level, 0)

    load_weight.wait()
    load_end.wait()

    @pl.when(t == 0)
    def _():
        send_bend()

    @pl.when(t == 1)
    def _():
        pl.semaphore_wait(hello.at[0], 2)
        call(1, 2)
        for e in range(comps):
            adjoint[e] = adjoint[e] + weight[e] * states[levels, e]
        split_field(adjoint)
        send_reverse(0)

        def reverse_level(j, carry):
            n = levels - 1 - j

            @pl.when(n < half)
            def _():
                state_copy(n).wait_recv()

            reverse_sum(n, adjoint)
            reverse_near(n)
            reverse_ahead()

            @pl.when(j > 0)
            def _():
                rev_sent(j - 1)

            reverse_wait(j)
            send_ahead(j + 1)
            reverse_far(j)
            split_field(adjoint)

            @pl.when(n == half)
            def _():
                kept[...] = adjoint[...]
                keep_copy.start()

            return carry

        lax.fori_loop(0, levels - 2, reverse_level, 0)
        state_copy(1).wait_recv()
        reverse_sum(1, adjoint)
        reverse_near(1)
        pl.semaphore_wait(hello.at[1], 2)
        call(2, 2)
        last_sum(levels - 2)
        row = in_row(partial[...])
        plane_row[...] = row
        plane_parts[spot] = row
        for r in range(1, plane):
            plane_copy(r).start()
        reverse_ahead()
        rev_sent(levels - 3)
        reverse_wait(levels - 2)
        send_ahead(levels - 1)
        reverse_far(levels - 2)
        split_field(adjoint)
        pl.semaphore_wait(hello.at[2], 2)
        all_parts(plane_parts, plane - 1, plane_send, plane_recv).wait_recv()
        total = plane_parts[0]
        for s in range(1, plane):
            total = total + plane_parts[s]
        plane_sum[...] = total
        layer_parts[layer] = total
        for r in range(layers):
            layer_copy(r, 0).start()
            if r > 0:
                layer_copy(r, 1).start()
        state_copy(0).wait_recv()
        reverse_near(0)
        rev_sent(levels - 2)
        reverse_wait(levels - 1)
        reverse_far(levels - 1)
        end_copy.start()

    fwd_sent(last)

    @pl.when(t == 0)
    def _():
        for i in range(half):
            state_copy(i).wait_send()
        for q in range(4):

            @pl.when(exists(p + aim[q]))
            def _():
                bend_copy(pull_way[q], p, q).wait_send()

        bend_pass.wait_send()

    @pl.when(t == 1)
    def _():
        rev_sent(levels - 1)
        keep_copy.wait()
        all_parts(plane_parts, plane - 1, plane_send, plane_recv).wait_send()
        all_parts(layer_parts, 2 * layers - 1, layer_send, layer_recv).wait_send()

    @pl.when(t == 0)
    def _():
        all_parts(layer_parts, layers, layer_send, layer_recv).wait_recv()

    @pl.when(t == 1)
    def _():
        all_parts(layer_parts, layers - 1, layer_send, layer_recv).wait_recv()

    total = layer_parts[0]
    for s in range(1, layers):
        total = total + layer_parts[s]
    grads_row[...] = total
    give_sums = pltpu.make_async_copy(grads_row, grads, out_sem.at[1])
    give_sums.start()

    @pl.when(t == 0)
    def _():
        end_copy.wait_recv()

    @pl.when(t == 1)
    def _():
        end_copy.wait_send()

    give_sums.wait()


def deliver(found, row, bounds, grads, held, sums, sums_out, sem):
    into = [pltpu.make_async_copy(found.at[0], held, sem.at[0, 0])]
    outof = [pltpu.make_async_copy(held, bounds.at[0], sem.at[1, 0])]
    row_in = pltpu.make_async_copy(row, sums, sem.at[0, 1])
    row_out = pltpu.make_async_copy(sums_out, grads, sem.at[1, 1])
    row_in.start()
    for copy in into:
        copy.start()
    row_in.wait()
    sums_out[...] = sums[0, : sums_out.shape[0]]
    row_out.start()
    for arrive, leave in zip(into, outof):
        arrive.wait()
        leave.start()
    row_out.wait()
    for leave in outof:
        leave.wait()


def solution(mesh):
    n_space = mesh.shape["space"]
    plane = 16 if n_space % 16 == 0 else 4

    def shards(
        checkpoints, sources, pitch, metric, obj_weight, adjoint_end, lift, mixing, faces, send_idx
    ):
        comps, blocks, nodes = obj_weight.shape
        slots = lift.shape[0]
        levels = pitch.shape[0]
        half = levels // 2
        halo = send_idx.shape[2]
        ghosts = 4 * halo
        wide = comps * nodes
        links = slots - 1
        layers = n_space // plane
        vmem = pltpu.VMEM
        dma = pltpu.SemaphoreType.DMA
        field = (comps, blocks, nodes)
        smem = pltpu.SMEM
        scratch = [
            smem((levels,), F32),
            smem(mixing.shape, F32),
            vmem((links, blocks), jnp.int32),
            smem(send_idx.shape, jnp.int32),
            vmem((1, nodes), F32),
            vmem((levels + 1, *field), F32),
            vmem((2, *field), F32),
            vmem((blocks, nodes), F32),
            vmem(field, F32),
            vmem(field, F32),
            vmem(field, F32),
            vmem((slots, nodes, nodes), BF16),
            vmem((nodes, slots * nodes), BF16),
            vmem((levels, nodes), F32),
            vmem((levels, nodes), F32),
            vmem((ghosts, blocks), F32),
            vmem((blocks, ghosts), BF16),
            vmem((links * blocks, blocks), BF16),
            vmem((links * blocks, 2 * blocks), BF16),
            vmem((blocks, links * ghosts), BF16),
            vmem((links * ghosts, 2 * blocks), BF16),
            vmem((ghosts, links * ghosts), BF16),
            vmem((links * ghosts, 2 * ghosts), BF16),
            vmem((ghosts, 3 * blocks), BF16),
            vmem((3 * blocks, wide), BF16),
            vmem((ghosts, wide), F32),
            vmem((ghosts, nodes), F32),
            vmem((ghosts, wide), F32),
            vmem((2 * ghosts, wide), BF16),
            vmem((comps * ghosts, nodes), F32),
            vmem((blocks, wide), BF16),
            vmem((links * blocks, wide), BF16),
            vmem((slots, comps * blocks, nodes), F32),
            vmem(field, F32),
            vmem(field, F32),
            vmem((comps * ghosts, links * nodes), F32),
            vmem((links * ghosts, wide), BF16),
            vmem((2 * blocks, wide), BF16),
            vmem((links * blocks, wide), F32),
            vmem((links * ghosts, wide), F32),
            vmem((comps * blocks, slots * nodes), BF16),
            vmem((comps * ghosts, links * nodes), BF16),
            vmem((half, 4, halo, wide), BF16),
            vmem((half, 4, halo, wide), BF16),
            vmem((levels, 4, halo, wide), BF16),
            vmem((levels, 4, halo, wide), BF16),
            vmem((4, halo, wide), BF16),
            vmem((4, halo, wide), BF16),
            vmem((4, halo, wide), BF16),
            vmem((levels, nodes), F32),
            vmem((1, nodes), F32),
            vmem((plane, 1, nodes), F32),
            vmem((1, nodes), F32),
            vmem((2 * layers, 1, nodes), F32),
            dma((10,)),
            dma((2, 4)),
            dma((2, 4)),
            dma((2, 4)),
            dma((2, 4)),
            dma((4,)),
            dma((4,)),
            dma((2,)),
            dma((half,)),
            dma((half,)),
            dma,
            dma,
            dma,
            dma,
            dma((2,)),
            dma((2,)),
            pltpu.SemaphoreType.REGULAR((3,)),
        ]
        anywhere = pl.BlockSpec(memory_space=pl.ANY)
        results, sums = pl.pallas_call(
            functools.partial(sweep, n_space, plane),
            out_shape=(
                jax.ShapeDtypeStruct((1, *field), F32),
                jax.ShapeDtypeStruct((1, nodes), F32),
            ),
            in_specs=[pl.BlockSpec(memory_space=pltpu.HBM)] * 10,
            out_specs=(anywhere, anywhere),
            scratch_shapes=scratch,
            compiler_params=pltpu.CompilerParams(
                collective_id=0, has_side_effects=True, vmem_limit_bytes=67043328
            ),
            name="adjoint_window",
        )(checkpoints, sources, pitch, metric, obj_weight, adjoint_end, lift, mixing, faces.T, send_idx)
        return pl.pallas_call(
            deliver,
            out_shape=(
                jax.ShapeDtypeStruct((1, *field), F32),
                jax.ShapeDtypeStruct((levels,), F32),
            ),
            in_specs=[anywhere, anywhere],
            out_specs=(anywhere, anywhere),
            scratch_shapes=[
                vmem(field, F32),
                vmem((1, nodes), F32),
                vmem((levels,), F32),
                dma((2, 2)),
            ],
            compiler_params=pltpu.CompilerParams(vmem_limit_bytes=67043328),
            name="deliver",
        )(results, sums)

    return jax.shard_map(
        shards,
        mesh=mesh,
        in_specs=(
            P("tm", None, "space", None),
            P(None, None, "space", None),
            P(),
            P("space", None),
            P(None, "space", None),
            P(None, "space", None),
            P(),
            P(),
            P("space", None),
            P("space", None, None),
        ),
        out_specs=(P("tm", None, "space", None), P()),
        check_vma=False,
    )
```
